32 devices in a mesh: dp: 8 (over y, x, core), tensor: 4 (over z).
Axes of the slice: x: 2, y: 2, z: 4, core: 2. Of those that a mesh axis runs over, the one named last changes fastest.
Arguments:
- block_input: bfloat16 [8192, 2048], P('dp'), may hold values from -6 to 6
- image_starts: int32 [8, 2], P('dp'), may hold values from 0 to 768, as said below
- norm_gain: bfloat16 [2048], replicated, may hold values from 0.5 to 1.5
- q_down: bfloat16 [2048, 1024], replicated, may hold values from -0.125 to 0.125
- q_gain: bfloat16 [1024], replicated, may hold values from 0.5 to 1.5
- q_up: bfloat16 [1024, 4096], P(None, 'tensor'), may hold values from -0.1875 to 0.1875
- k_proj: bfloat16 [2048, 256], replicated, may hold values from -0.25 to 0.25
- v_proj: bfloat16 [2048, 256], replicated, may hold values from -0.125 to 0.125
- out_proj: bfloat16 [4096, 2048], P('tensor'), may hold values from -0.75 to 0.75
- mlp_gain: bfloat16 [2048], replicated, may hold values from 0.5 to 1.5
- w_gate: bfloat16 [2048, 5632], P(None, 'tensor'), may hold values from -0.125 to 0.125
- w_up: bfloat16 [2048, 5632], P(None, 'tensor'), may hold values from -0.125 to 0.125
- w_down: bfloat16 [5632, 2048], P('tensor'), may hold values from -0.078125 to 0.078125
- d_output: bfloat16 [8192, 2048], P('dp'), may hold values from -6 to 6
Outputs:
- block_output: bfloat16 [8192, 2048], P('dp')
- grad_input: bfloat16 [8192, 2048], P('dp')
- grad_norm_gain: float32 [2048], P(('dp', 'tensor'))
- grad_q_down: float32 [2048, 1024], P(('dp', 'tensor'))
- grad_q_gain: float32 [1024], P(('dp', 'tensor'))
- grad_q_up: float32 [1024, 4096], P('dp', 'tensor')
- grad_k_proj: float32 [2048, 256], P(('dp', 'tensor'))
- grad_v_proj: float32 [2048, 256], P(('dp', 'tensor'))
- grad_out_proj: float32 [4096, 2048], P('tensor', 'dp')
- grad_mlp_gain: float32 [2048], P(('dp', 'tensor'))
- grad_w_gate: float32 [2048, 5632], P('dp', 'tensor')
- grad_w_up: float32 [2048, 5632], P('dp', 'tensor')
- grad_w_down: float32 [5632, 2048], P('tensor', 'dp')
The draws below stay inside these ranges and needn't reach their ends.
Inputs may be any that keep to these rules, and one draw needn't show every extreme that they name: `image_starts`: each row holds the ascending starts of 2 image pieces of 256 positions of one sequence; the pieces lie inside the sequence and never intersect.
All inputs are finite; a program needn't handle non-finite values.
Results may differ from the reference program's by a relative error of at most 0.017.
The reference program's roundings to bfloat16 on the way count: a program that leaves them out, or rounds other values in their place, can miss the bound.
Values sent between devices are 32-bit elements; how exact they have to be, the bound alone decides.
A program may use at most 256 MiB of HBM per device.

```python
import jax
import jax.numpy as jnp
from jax import lax

D = 2048
QR = 1024
H = 16
HD = 256
FF = 5632
PIECE = 256
PIECES = 2
SEQ_LEN = 1024
SEQS = 8
TOKENS = 8192


def draw_image_starts(key, part):
    free_room = SEQ_LEN - PIECES * PIECE
    raw_starts = jax.random.randint(key, (SEQS, PIECES), 0, free_room + 1)
    ordered = jnp.sort(raw_starts, axis=1)
    row_ids = jnp.arange(SEQS)[:, None]
    col_ids = jnp.arange(PIECES)[None, :]
    ordered = jnp.where((row_ids == 0) & (col_ids == 0), 0, ordered)
    ordered = jnp.where((row_ids == 0) & (col_ids == PIECES - 1), free_room, ordered)
    return (ordered + col_ids * PIECE).astype(jnp.int32)


def block_scale(stream_key, extent, shards, low, high):
    factor_of = 1.0
    for axis_at, parts in shards:
        steps = jax.random.uniform(jax.random.fold_in(jax.random.fold_in(stream_key, 6), axis_at), (parts,), jnp.float32, low / len(shards), high / len(shards))
        factor_of = factor_of * jnp.repeat(jnp.exp(steps), extent[axis_at] // parts).reshape((-1,) + (1,) * (len(extent) - 1 - axis_at))
    return factor_of


def normal_values(key, shape, spread, reach, pieces=(), held_as=jnp.bfloat16):
    drawn = spread * jax.random.normal(key, shape, jnp.float32)
    if pieces:
        drawn = drawn * block_scale(key, shape, pieces, -0.22, 0.18)
    return jnp.clip(drawn, -reach, reach).astype(held_as)


def setup_inputs(seed: int = 0) -> dict:
    seeds = jax.random.split(jax.random.key(seed), 15)
    return {
        "block_input": normal_values(seeds[0], (TOKENS, D), 1.0, 6.0, ((0, 8),)),
        "image_starts": draw_image_starts(jax.random.fold_in(seeds[14], 71), 0),
        "norm_gain": jnp.clip(1.0 + 0.1 * jax.random.normal(seeds[2], (D,), jnp.float32), 0.5, 1.5).astype(jnp.bfloat16),
        "q_down": normal_values(seeds[3], (D, QR), D ** -0.5, 0.125),
        "q_gain": jnp.clip(1.0 + 0.1 * jax.random.normal(seeds[4], (QR,), jnp.float32), 0.5, 1.5).astype(jnp.bfloat16),
        "q_up": normal_values(seeds[5], (QR, H * HD), QR ** -0.5, 0.1875, ((1, 4),)),
        "k_proj": normal_values(seeds[6], (D, HD), (D // 4) ** -0.5, 0.25),
        "v_proj": normal_values(seeds[7], (D, HD), D ** -0.5, 0.125),
        "out_proj": normal_values(seeds[8], (H * HD, D), (H * HD // 64) ** -0.5, 0.75, ((0, 4),)),
        "mlp_gain": jnp.clip(1.0 + 0.1 * jax.random.normal(seeds[9], (D,), jnp.float32), 0.5, 1.5).astype(jnp.bfloat16),
        "w_gate": normal_values(seeds[10], (D, FF), D ** -0.5, 0.125, ((1, 4),)),
        "w_up": normal_values(seeds[11], (D, FF), D ** -0.5, 0.125, ((1, 4),)),
        "w_down": normal_values(seeds[12], (FF, D), FF ** -0.5, 0.078125, ((0, 4),)),
        "d_output": normal_values(seeds[13], (TOKENS, D), 1.0, 6.0, ((0, 8),)),
    }


epsilon = 1e-06
masked_score = -1e+30
highest = lax.Precision.HIGHEST

@jax.custom_vjp
def low(v):
    return lax.optimization_barrier(v.astype(jnp.bfloat16)).astype(jnp.float32)

@jax.custom_vjp
def low_back(v):
    return v

def low_keep(v):
    return (low(v), None)

def low_pass(kept, grad):
    return (grad,)

def back_keep(v):
    return (v, None)

def back_low(kept, grad):
    return (low(grad),)
low.defvjp(low_keep, low_pass)
low_back.defvjp(back_keep, back_low)

def exact_dot(left, right):
    return jnp.dot(left, right, precision=highest)

def rms_norm(values, gain):
    return values * lax.rsqrt(lax.optimization_barrier(jnp.mean(values * values, axis=-1, keepdims=True)) + epsilon) * gain

def rotate(values, cos_tab, sin_tab):
    half = values.shape[-1] // 2
    first_half = values[..., :half]
    second_half = values[..., half:]
    return jnp.concatenate([first_half * cos_tab - second_half * sin_tab, second_half * cos_tab + first_half * sin_tab], axis=-1)

def tables():
    positions = jnp.arange(SEQ_LEN).astype(jnp.float32)
    inv_freq = 10000.0 ** (-(jnp.arange(HD // 2).astype(jnp.float32) * 2.0) / HD)
    angles = positions[:, None] * inv_freq[None, :]
    return (jnp.cos(angles), jnp.sin(angles))

def allowed_mask(starts):
    positions = jnp.arange(SEQ_LEN, dtype=jnp.int32)
    inside = (positions[:, None] >= starts[None, :]) & (positions[:, None] < starts[None, :] + PIECE)
    labels = jnp.arange(1, PIECES + 1, dtype=jnp.int32)
    piece_ids = lax.optimization_barrier(jnp.sum(jnp.where(inside, labels[None, :], 0), axis=1)).astype(jnp.int32)
    causal = positions[None, :] <= positions[:, None]
    same_piece = (piece_ids[:, None] == piece_ids[None, :]) & (piece_ids[:, None] > 0)
    return causal | same_piece

def block_layer(weights, seq_input, cos_tab, sin_tab, allowed):
    norm_gain, q_down, q_gain, q_up, k_proj, v_proj, out_proj, mlp_gain, w_gate, w_up, w_down = weights
    normed_in = low(rms_norm(seq_input, norm_gain))
    q_latent = low_back(exact_dot(normed_in, q_down))
    q_normed = low(rms_norm(q_latent, q_gain))
    q_raw = low_back(exact_dot(q_normed, q_up)).reshape(SEQ_LEN, H, HD)
    queries = low(rotate(q_raw, cos_tab[:, None, :], sin_tab[:, None, :]))
    key_rot = low(rotate(low_back(exact_dot(normed_in, k_proj)), cos_tab, sin_tab))
    val_rows = low(low_back(exact_dot(normed_in, v_proj)))
    scores = low_back(jnp.einsum('qhd,kd->hqk', queries, key_rot, precision=highest) * HD ** (-0.5))
    scores = jnp.where(allowed[None], scores, masked_score)
    attn_probs = jax.nn.softmax(scores, axis=-1)
    mixed_heads = jnp.einsum('hqk,kd->qhd', low(attn_probs), val_rows, precision=highest).reshape(SEQ_LEN, H * HD)
    mixed_heads = low(low_back(mixed_heads))
    hidden_in = seq_input + low_back(exact_dot(mixed_heads, out_proj))
    normed_mid = low(rms_norm(hidden_in, mlp_gain))
    gate_pre = low_back(exact_dot(normed_mid, w_gate))
    up_pre = low_back(exact_dot(normed_mid, w_up))
    hidden_act = low(jax.nn.silu(gate_pre) * up_pre)
    return hidden_in + low_back(exact_dot(hidden_act, w_down))

def reference(block_input, image_starts, norm_gain, q_down, q_gain, q_up, k_proj, v_proj, out_proj, mlp_gain, w_gate, w_up, w_down, d_output):
    weights = tuple((item.astype(jnp.float32) for item in (norm_gain, q_down, q_gain, q_up, k_proj, v_proj, out_proj, mlp_gain, w_gate, w_up, w_down)))
    cos_tab, sin_tab = tables()
    seq_inputs = block_input.astype(jnp.float32).reshape(SEQS, SEQ_LEN, D)
    seq_cotans = d_output.astype(jnp.float32).reshape(SEQS, SEQ_LEN, D)

    def seq_step(totals, seq_item):
        seq_input, seq_cotan, starts = seq_item
        allowed = allowed_mask(starts)

        def apply_layer(layer_weights, layer_input):
            return block_layer(layer_weights, layer_input, cos_tab, sin_tab, allowed)
        layer_out, pull_back = jax.vjp(apply_layer, weights, seq_input)
        grad_weights, grad_in = pull_back(seq_cotan)
        return (jax.tree.map(jnp.add, totals, grad_weights), (layer_out, grad_in))
    zero_grads = jax.tree.map(jnp.zeros_like, weights)
    totals, (layer_outs, grad_ins) = lax.scan(seq_step, zero_grads, (seq_inputs, seq_cotans, image_starts))
    return (layer_outs.reshape(TOKENS, D).astype(jnp.bfloat16), grad_ins.reshape(TOKENS, D).astype(jnp.bfloat16), totals[0], totals[1], totals[2], totals[3], totals[4], totals[5], totals[6], totals[7], totals[8], totals[9], totals[10])
```

```python
import functools

import jax
import jax.numpy as jnp
from jax import lax
from jax.experimental import pallas as pl
from jax.experimental.pallas import tpu as pltpu
from jax.sharding import PartitionSpec as P


MESH = pl.DeviceIdType.MESH

PIECE = 256


epsilon = 1e-06
masked_score = -1e30


def normalize(values):
    scale_rows = lax.rsqrt(jnp.mean(values * values, axis=-1, keepdims=True) + epsilon)
    return (values * scale_rows, scale_rows)


def norm_back(grad_normed, normed, scale_rows):
    return scale_rows * (
        grad_normed - normed * jnp.mean(grad_normed * normed, axis=-1, keepdims=True)
    )


def left_dot(left, right):
    return lax.dot_general(
        left, right, (((0,), (0,)), ((), ())), preferred_element_type=jnp.float32
    )


def right_dot(left, right):
    return lax.dot_general(
        left, right, (((1,), (1,)), ((), ())), preferred_element_type=jnp.float32
    )


def rotate(values, cos_tab, sin_tab):
    half = values.shape[-1] // 2
    first_half = values[..., :half]
    second_half = values[..., half:]
    return jnp.concatenate(
        [
            first_half * cos_tab - second_half * sin_tab,
            second_half * cos_tab + first_half * sin_tab,
        ],
        axis=-1,
    )


def unrotate(grads, cos_tab, sin_tab):
    half = grads.shape[-1] // 2
    first_half = grads[..., :half]
    second_half = grads[..., half:]
    return jnp.concatenate(
        [
            first_half * cos_tab + second_half * sin_tab,
            second_half * cos_tab - first_half * sin_tab,
        ],
        axis=-1,
    )


def line_kernel(axis, n, chunks, K, x_ref, o_ref, red, s_red, r_red, s_fin, r_fin):
    me = lax.axis_index(axis)
    rows = x_ref.shape[0] // (2 * chunks)
    barrier = pltpu.get_barrier_semaphore()

    @pl.when(me > 0)
    def _():
        pl.semaphore_signal(barrier, inc=1, device_id={axis: me - 1}, device_id_type=MESH)

    @pl.when(me < n - 1)
    def _():
        pl.semaphore_signal(barrier, inc=1, device_id={axis: me + 1}, device_id_type=MESH)

    @pl.when((me == 0) | (me == n - 1))
    def _():
        pl.semaphore_wait(barrier, 1)

    @pl.when((me > 0) & (me < n - 1))
    def _():
        pl.semaphore_wait(barrier, 2)

    def at(half, c):
        return pl.ds(pl.multiple_of((half * chunks + c) * rows, rows), rows)

    def down(half):
        return me - 1 if half == 0 else me + 1

    def up(half):
        return me + 1 if half == 0 else me - 1

    def sum_copy(src, half, c):
        return pltpu.make_async_remote_copy(
            src_ref=src.at[at(half, c)], dst_ref=red.at[at(half, c)],
            send_sem=s_red.at[half, c], recv_sem=r_red.at[half, c],
            device_id={axis: down(half)}, device_id_type=MESH)

    def fin_copy(half, c):
        return pltpu.make_async_remote_copy(
            src_ref=o_ref.at[at(half, c)], dst_ref=o_ref.at[at(half, c)],
            send_sem=s_fin.at[half, c], recv_sem=r_fin.at[half, c],
            device_id={axis: up(half)}, device_id_type=MESH)

    def step(s, carry):
        for half in (0, 1):
            hop = (n - 1 - me) if half == 0 else me
            c = s - K * hop
            ok = (c >= 0) & (c < chunks)

            @pl.when(ok & (hop == 0))
            def _():
                sum_copy(x_ref, half, c).start()

            @pl.when(ok & (hop > 0) & (hop < n - 1))
            def _():
                sum_copy(x_ref, half, c).wait_recv()
                red[at(half, c)] = red[at(half, c)] + x_ref[at(half, c)]
                sum_copy(red, half, c).start()

            @pl.when(ok & (hop == n - 1))
            def _():
                sum_copy(x_ref, half, c).wait_recv()
                o_ref[at(half, c)] = red[at(half, c)] + x_ref[at(half, c)]
                fin_copy(half, c).start()
        for half in (0, 1):
            back = me if half == 0 else (n - 1 - me)
            c = s - K * (n - 1) - K * back
            ok = (c >= 0) & (c < chunks)

            @pl.when(ok & (back > 0))
            def _():
                fin_copy(half, c).wait_recv()

            @pl.when(ok & (back > 0) & (back < n - 1))
            def _():
                fin_copy(half, c).start()
        return carry

    lax.fori_loop(0, chunks + 2 * K * (n - 1), step, 0)

    def drain(c, carry):
        for half in (0, 1):
            hop = (n - 1 - me) if half == 0 else me

            @pl.when(hop < n - 1)
            def _():
                sum_copy(x_ref, half, c).wait_send()

            @pl.when(hop > 0)
            def _():
                fin_copy(half, c).wait_send()
        return carry

    lax.fori_loop(0, chunks, drain, 0)


def line_sum(x, axis, n, chunks, cid, K=1):
    return pl.pallas_call(
        functools.partial(line_kernel, axis, n, chunks, K),
        out_shape=jax.ShapeDtypeStruct(x.shape, x.dtype),
        in_specs=[pl.BlockSpec(memory_space=pltpu.VMEM)],
        out_specs=pl.BlockSpec(memory_space=pltpu.VMEM),
        scratch_shapes=[pltpu.VMEM(x.shape, x.dtype)] + [pltpu.SemaphoreType.DMA((2, chunks))] * 4,
        compiler_params=pltpu.CompilerParams(collective_id=cid, has_side_effects=True, vmem_limit_bytes=48 << 20),
        name="line_sum",
    )(x)


def shards(
    block_input,
    image_starts,
    norm_gain,
    q_down,
    q_gain,
    q_up,
    k_proj,
    v_proj,
    out_proj,
    mlp_gain,
    w_gate,
    w_up,
    w_down,
    d_output,
):
    row_count, model_width = block_input.shape
    dp_count = lax.axis_size("dp")
    tp_count = lax.axis_size("tensor")
    tp_index = lax.axis_index("tensor")

    def sum_parts(part):
        chunks = row_count // 32
        while row_count % (16 * chunks):
            chunks -= 1
        return line_sum(part, "tensor", tp_count, chunks, 1 if part.shape[1] == model_width else 2, 2)

    def own_part(values, axis):
        split = values.shape[axis] // (dp_count * tp_count)
        shape = values.shape[:axis] + (dp_count, tp_count, split) + values.shape[axis + 1 :]
        picked = lax.dynamic_index_in_dim(values.reshape(shape), tp_index, axis + 1, keepdims=False)
        return picked

    seq_count = image_starts.shape[0]
    seq_len = row_count // seq_count
    head_dim = k_proj.shape[1]
    head_count = q_up.shape[1] // head_dim
    block_rows = min(512, seq_len)
    block_count = seq_len // block_rows
    score_scale = head_dim ** (-0.5)
    positions = jnp.arange(seq_len, dtype=jnp.float32)
    inv_freq = 10000.0 ** (-(jnp.arange(head_dim // 2, dtype=jnp.float32) * 2.0) / head_dim)
    angles = positions[:, None] * inv_freq[None, :]
    cos_all = jnp.tile(jnp.cos(angles), (seq_count, 1))
    sin_all = jnp.tile(jnp.sin(angles), (seq_count, 1))
    pos_int = jnp.arange(seq_len, dtype=jnp.int32)
    inside = (pos_int[None, :, None] >= image_starts[:, None, :]) & (
        pos_int[None, :, None] < image_starts[:, None, :] + PIECE
    )
    labels = jnp.arange(1, image_starts.shape[1] + 1, dtype=jnp.int32)
    piece_ids = jnp.sum(jnp.where(inside, labels, 0), axis=2)

    def block_scores(q_block, key_rows, seq_ids, row_start):
        raw = (
            jnp.einsum("qhd,kd->hqk", q_block, key_rows, preferred_element_type=jnp.float32)
            * score_scale
        )
        query_pos = row_start + jnp.arange(block_rows, dtype=jnp.int32)
        query_ids = lax.dynamic_slice_in_dim(seq_ids, row_start, block_rows)
        visible = (pos_int[None, :] <= query_pos[:, None]) | (
            query_ids[:, None] == seq_ids[None, :]
        ) & (query_ids[:, None] > 0)
        return jnp.where(visible[None], raw, masked_score)

    input_f32 = block_input.astype(jnp.float32)
    gain_attn = norm_gain.astype(jnp.float32)
    gain_query = q_gain.astype(jnp.float32)
    gain_mlp = mlp_gain.astype(jnp.float32)
    cotan_f32 = d_output.astype(jnp.float32)
    normed_one, scale_one = normalize(input_f32)
    normed_in = (normed_one * gain_attn).astype(jnp.bfloat16)
    q_latent = jnp.dot(normed_in, q_down, preferred_element_type=jnp.float32)
    q_unit, q_scale = normalize(q_latent)
    q_normed = (q_unit * gain_query).astype(jnp.bfloat16)
    q_raw = jnp.dot(q_normed, q_up, preferred_element_type=jnp.float32).reshape(
        row_count, head_count, head_dim
    )
    queries = rotate(q_raw, cos_all[:, None, :], sin_all[:, None, :]).astype(jnp.bfloat16)
    key_rows = rotate(
        jnp.dot(normed_in, k_proj, preferred_element_type=jnp.float32), cos_all, sin_all
    ).astype(jnp.bfloat16)
    val_rows = jnp.dot(normed_in, v_proj, preferred_element_type=jnp.float32).astype(jnp.bfloat16)
    query_seq = queries.reshape(seq_count, block_count, block_rows, head_count, head_dim)
    key_seq = key_rows.reshape(seq_count, seq_len, head_dim)
    val_seq = val_rows.reshape(seq_count, seq_len, head_dim)
    block_ids = jnp.arange(block_count, dtype=jnp.int32)

    def forward_seq(seq_item):
        q_all, seq_keys, seq_vals, seq_ids = seq_item

        def forward_block(block_item):
            q_block, blk_index = block_item
            scores = block_scores(q_block, seq_keys, seq_ids, blk_index * block_rows)
            row_max = jnp.max(scores, axis=-1, keepdims=True)
            exp_terms = jnp.exp(scores - row_max)
            row_sum = jnp.sum(exp_terms, axis=-1, keepdims=True)
            attn_probs = (exp_terms / row_sum).astype(jnp.bfloat16)
            mixed_block = jnp.einsum(
                "hqk,kd->qhd", attn_probs, seq_vals, preferred_element_type=jnp.float32
            )
            return (mixed_block.astype(jnp.bfloat16), (row_max + jnp.log(row_sum))[..., 0])

        return lax.map(forward_block, (q_all, block_ids))

    mixed_seq, log_norm = lax.map(forward_seq, (query_seq, key_seq, val_seq, piece_ids))
    mixed_heads = mixed_seq.reshape(row_count, head_count * head_dim)
    attn_out = sum_parts(jnp.dot(mixed_heads, out_proj, preferred_element_type=jnp.float32))
    hidden_in = input_f32 + attn_out
    normed_two, scale_two = normalize(hidden_in)
    normed_mid = (normed_two * gain_mlp).astype(jnp.bfloat16)
    gate_pre = jnp.dot(normed_mid, w_gate, preferred_element_type=jnp.float32)
    up_pre = jnp.dot(normed_mid, w_up, preferred_element_type=jnp.float32)
    gate_sig = jax.nn.sigmoid(gate_pre)
    hidden_act = (gate_pre * gate_sig * up_pre).astype(jnp.bfloat16)
    mlp_part = jnp.dot(hidden_act, w_down, preferred_element_type=jnp.float32)
    grad_down = left_dot(hidden_act, d_output)
    d_act = right_dot(d_output, w_down)
    d_gate = (d_act * up_pre * gate_sig * (1.0 + gate_pre * (1.0 - gate_sig))).astype(jnp.bfloat16)
    d_up = (d_act * gate_pre * gate_sig).astype(jnp.bfloat16)
    grad_gate = left_dot(normed_mid, d_gate)
    grad_up = left_dot(normed_mid, d_up)
    d_mid_part = right_dot(d_gate, w_gate) + right_dot(d_up, w_up)
    d_mid_part, grad_down, grad_gate, grad_up = lax.optimization_barrier(
        (d_mid_part, grad_down, grad_gate, grad_up)
    )
    grad_gate = lax.psum_scatter(grad_gate, "dp", scatter_dimension=0, tiled=True)
    grad_up = lax.psum_scatter(grad_up, "dp", scatter_dimension=0, tiled=True)
    grad_down = lax.psum_scatter(grad_down, "dp", scatter_dimension=1, tiled=True)
    d_mid = sum_parts(d_mid_part)
    grad_gain_mlp = jnp.sum(d_mid * normed_two, axis=0)
    d_hidden = cotan_f32 + norm_back(d_mid * gain_mlp, normed_two, scale_two)
    d_hidden_low = d_hidden.astype(jnp.bfloat16)
    grad_out = left_dot(mixed_heads, d_hidden_low)
    d_mixed = right_dot(d_hidden_low, out_proj).astype(jnp.bfloat16)
    d_mixed_seq = d_mixed.reshape(seq_count, block_count, block_rows, head_count, head_dim)

    def backward_seq(seq_item):
        q_all, dm_all, norm_all, seq_keys, seq_vals, seq_ids = seq_item

        def backward_block(sums_pair, block_item):
            key_sum, val_sum = sums_pair
            q_block, dm_block, norm_block, blk_index = block_item
            scores = block_scores(q_block, seq_keys, seq_ids, blk_index * block_rows)
            attn_probs = jnp.exp(scores - norm_block[..., None])
            d_probs = jnp.einsum(
                "qhd,kd->hqk", dm_block, seq_vals, preferred_element_type=jnp.float32
            )
            d_scores = (
                attn_probs * (d_probs - jnp.sum(attn_probs * d_probs, axis=-1, keepdims=True))
            ).astype(jnp.bfloat16)
            d_query = (
                jnp.einsum("hqk,kd->qhd", d_scores, seq_keys, preferred_element_type=jnp.float32)
                * score_scale
            )
            key_sum = (
                key_sum
                + jnp.einsum("hqk,qhd->kd", d_scores, q_block, preferred_element_type=jnp.float32)
                * score_scale
            )
            val_sum = val_sum + jnp.einsum(
                "hqk,qhd->kd",
                attn_probs.astype(jnp.bfloat16),
                dm_block,
                preferred_element_type=jnp.float32,
            )
            return ((key_sum, val_sum), d_query)

        zero_rows = jnp.zeros((seq_len, head_dim), jnp.float32)
        (key_sum, val_sum), d_query = lax.scan(
            backward_block, (zero_rows, zero_rows), (q_all, dm_all, norm_all, block_ids)
        )
        return (key_sum, val_sum, d_query)

    key_grad, val_grad, query_grad = lax.map(
        backward_seq, (query_seq, d_mixed_seq, log_norm, key_seq, val_seq, piece_ids)
    )
    d_q_raw = unrotate(
        query_grad.reshape(row_count, head_count, head_dim),
        cos_all[:, None, :],
        sin_all[:, None, :],
    )
    d_q_raw = d_q_raw.reshape(row_count, head_count * head_dim).astype(jnp.bfloat16)
    key_val_part = jnp.concatenate(
        [key_grad.reshape(row_count, head_dim), val_grad.reshape(row_count, head_dim)], axis=1
    )
    grad_query_up = left_dot(q_normed, d_q_raw)
    d_bq_part = right_dot(d_q_raw, q_up)
    mlp_part, d_bq_part = lax.optimization_barrier((mlp_part, d_bq_part))
    mlp_out = sum_parts(mlp_part)
    block_output = (hidden_in + mlp_out).astype(jnp.bfloat16)
    query_key_val = sum_parts(jnp.concatenate([d_bq_part, key_val_part], axis=1))
    d_q_normed = query_key_val[:, : q_gain.shape[0]]
    key_val_full = query_key_val[:, q_gain.shape[0] :]
    d_key_low = unrotate(key_val_full[:, :head_dim], cos_all, sin_all).astype(jnp.bfloat16)
    d_val_low = key_val_full[:, head_dim:].astype(jnp.bfloat16)
    grad_gain_query = jnp.sum(d_q_normed * q_unit, axis=0)
    d_latent = norm_back(d_q_normed * gain_query, q_unit, q_scale).astype(jnp.bfloat16)
    d_normed_in = (
        right_dot(d_latent, q_down) + right_dot(d_key_low, k_proj) + right_dot(d_val_low, v_proj)
    )
    grad_gain_attn = jnp.sum(d_normed_in * normed_one, axis=0)
    grad_input = (d_hidden + norm_back(d_normed_in * gain_attn, normed_one, scale_one)).astype(
        jnp.bfloat16
    )
    grad_query_up = lax.psum_scatter(grad_query_up, "dp", scatter_dimension=0, tiled=True)
    grad_out = lax.psum_scatter(grad_out, "dp", scatter_dimension=1, tiled=True)
    own_in = own_part(normed_in, 1).reshape(row_count, -1)
    own_grads = left_dot(own_in, jnp.concatenate([d_latent, d_key_low, d_val_low], axis=1))
    own_rows = own_grads.shape[0]
    gain_one = own_part(grad_gain_attn, 0).reshape(own_rows, 1)
    gain_two = own_part(grad_gain_mlp, 0).reshape(own_rows, 1)
    gain_mid = own_part(grad_gain_query, 0)
    own_mid = gain_mid.shape[1]
    gain_mid = jnp.pad(gain_mid, ((0, 0), (0, own_rows // dp_count - own_mid))).reshape(own_rows, 1)
    gain_cols = jnp.concatenate([gain_one, gain_two, gain_mid], axis=1)
    own_grads = jnp.concatenate([own_grads, jnp.pad(gain_cols, ((0, 0), (0, 125)))], axis=1)
    own_sum = lax.psum_scatter(own_grads, "dp", scatter_dimension=0, tiled=True)
    rank = q_down.shape[1]
    grad_qd = own_sum[:, :rank]
    grad_key = own_sum[:, rank : rank + head_dim]
    grad_val = own_sum[:, rank + head_dim : rank + 2 * head_dim]
    gain_at = rank + 2 * head_dim
    grad_g1 = own_sum[:, gain_at]
    grad_g2 = own_sum[:, gain_at + 1]
    grad_gq = own_sum[:own_mid, gain_at + 2]
    return (
        block_output,
        grad_input,
        grad_g1,
        grad_qd,
        grad_gq,
        grad_query_up,
        grad_key,
        grad_val,
        grad_out,
        grad_g2,
        grad_gate,
        grad_up,
        grad_down,
    )


def solution(mesh):
    placed = (
        P("dp", None),
        P("dp", None),
        P(),
        P(),
        P(),
        P(None, "tensor"),
        P(),
        P(),
        P("tensor", None),
        P(),
        P(None, "tensor"),
        P(None, "tensor"),
        P("tensor", None),
        P("dp", None),
    )

    return jax.shard_map(
        shards,
        mesh=mesh,
        in_specs=placed,
        out_specs=(
            P("dp", None),
            P("dp", None),
            P(("dp", "tensor")),
            P(("dp", "tensor"), None),
            P(("dp", "tensor")),
            P("dp", "tensor"),
            P(("dp", "tensor"), None),
            P(("dp", "tensor"), None),
            P("tensor", "dp"),
            P(("dp", "tensor")),
            P("dp", "tensor"),
            P("dp", "tensor"),
            P("tensor", "dp"),
        ),
        check_vma=False,
    )
```

```python
import functools

import jax
import jax.numpy as jnp
from jax import lax
from jax.experimental import pallas as pl
from jax.experimental.pallas import tpu as pltpu
from jax.sharding import PartitionSpec as P


MESH = pl.DeviceIdType.MESH

PIECE = 256


epsilon = 1e-06
masked_score = -1e30


def normalize(values):
    scale_rows = lax.rsqrt(jnp.mean(values * values, axis=-1, keepdims=True) + epsilon)
    return (values * scale_rows, scale_rows)


def norm_back(grad_normed, normed, scale_rows):
    return scale_rows * (
        grad_normed - normed * jnp.mean(grad_normed * normed, axis=-1, keepdims=True)
    )


def left_dot(left, right):
    return lax.dot_general(
        left, right, (((0,), (0,)), ((), ())), preferred_element_type=jnp.float32
    )


def right_dot(left, right):
    return lax.dot_general(
        left, right, (((1,), (1,)), ((), ())), preferred_element_type=jnp.float32
    )


def rotate(values, cos_tab, sin_tab):
    half = values.shape[-1] // 2
    first_half = values[..., :half]
    second_half = values[..., half:]
    return jnp.concatenate(
        [
            first_half * cos_tab - second_half * sin_tab,
            second_half * cos_tab + first_half * sin_tab,
        ],
        axis=-1,
    )


def unrotate(grads, cos_tab, sin_tab):
    half = grads.shape[-1] // 2
    first_half = grads[..., :half]
    second_half = grads[..., half:]
    return jnp.concatenate(
        [
            first_half * cos_tab + second_half * sin_tab,
            second_half * cos_tab - first_half * sin_tab,
        ],
        axis=-1,
    )


def line_steps(axis, n, chunks, lag, x_ref, held, red, sems, finish, job, job_count):
    me = lax.axis_index(axis)
    rows = x_ref.shape[0] // (2 * chunks)
    s_red, r_red, s_fin, r_fin = sems
    barrier = pltpu.get_barrier_semaphore()

    @pl.when(me > 0)
    def _():
        pl.semaphore_signal(barrier, inc=1, device_id={axis: me - 1}, device_id_type=MESH)

    @pl.when(me < n - 1)
    def _():
        pl.semaphore_signal(barrier, inc=1, device_id={axis: me + 1}, device_id_type=MESH)

    @pl.when((me == 0) | (me == n - 1))
    def _():
        pl.semaphore_wait(barrier, 1)

    @pl.when((me > 0) & (me < n - 1))
    def _():
        pl.semaphore_wait(barrier, 2)

    def at(half, c):
        return pl.ds(pl.multiple_of((half * chunks + c) * rows, rows), rows)

    def sum_copy(src, half, c):
        return pltpu.make_async_remote_copy(
            src_ref=src.at[at(half, c)],
            dst_ref=red.at[at(half, c)],
            send_sem=s_red.at[half, c],
            recv_sem=r_red.at[half, c],
            device_id={axis: me - 1 if half == 0 else me + 1},
            device_id_type=MESH,
        )

    def fin_copy(half, c):
        return pltpu.make_async_remote_copy(
            src_ref=held.at[at(half, c)],
            dst_ref=held.at[at(half, c)],
            send_sem=s_fin.at[half, c],
            recv_sem=r_fin.at[half, c],
            device_id={axis: me + 1 if half == 0 else me - 1},
            device_id_type=MESH,
        )

    steps = chunks + 2 * lag * (n - 1)

    def step(s, carry):
        for half in (0, 1):
            hop = (n - 1 - me) if half == 0 else me
            c = s - lag * hop
            ok = (c >= 0) & (c < chunks)

            @pl.when(ok & (hop == 0))
            def _():
                sum_copy(x_ref, half, c).start()

            @pl.when(ok & (hop > 0) & (hop < n - 1))
            def _():
                sum_copy(x_ref, half, c).wait_recv()
                red[at(half, c)] = red[at(half, c)] + x_ref[at(half, c)]
                sum_copy(red, half, c).start()

            @pl.when(ok & (hop == n - 1))
            def _():
                sum_copy(x_ref, half, c).wait_recv()
                held[at(half, c)] = red[at(half, c)] + x_ref[at(half, c)]
                fin_copy(half, c).start()
                finish(at(half, c))

        for half in (0, 1):
            back = me if half == 0 else (n - 1 - me)
            c = s - lag * (n - 1) - lag * back
            ok = (c >= 0) & (c < chunks)

            @pl.when(ok & (back > 0))
            def _():
                fin_copy(half, c).wait_recv()

            @pl.when(ok & (back > 0) & (back < n - 1))
            def _():
                fin_copy(half, c).start()

            @pl.when(ok & (back > 0))
            def _():
                finish(at(half, c))

        if job_count:
            lax.fori_loop(s * job_count // steps, (s + 1) * job_count // steps, job, 0)
        return carry

    lax.fori_loop(0, steps, step, 0)

    def drain(c, carry):
        for half in (0, 1):
            hop = (n - 1 - me) if half == 0 else me

            @pl.when(hop < n - 1)
            def _():
                sum_copy(x_ref, half, c).wait_send()

            @pl.when(hop > 0)
            def _():
                fin_copy(half, c).wait_send()

        return carry

    lax.fori_loop(0, chunks, drain, 0)


def line_kernel(axis, n, chunks, lag, x_ref, o_ref, red, *sems):
    line_steps(axis, n, chunks, lag, x_ref, o_ref, red, sems, lambda at: None, None, 0)


def line_low_kernel(axis, n, chunks, lag, x_ref, o_ref, red, held, *sems):
    def finish(at):
        o_ref[at] = held[at].astype(o_ref.dtype)

    line_steps(axis, n, chunks, lag, x_ref, held, red, sems, finish, None, 0)


def chunk_count(rows, most, tile):
    chunks = most
    while rows % (2 * chunks * tile):
        chunks -= 1
    return chunks


def line_params(cid):
    return pltpu.CompilerParams(
        collective_id=cid, has_side_effects=True, vmem_limit_bytes=56 << 20
    )


def line_sum(x, axis, n, cid, low=False):
    chunks = chunk_count(x.shape[0], 32, 16 if low else 8)
    held = [pltpu.VMEM(x.shape, x.dtype)] if low else []
    return pl.pallas_call(
        functools.partial(line_low_kernel if low else line_kernel, axis, n, chunks, 2),
        out_shape=jax.ShapeDtypeStruct(x.shape, jnp.bfloat16 if low else x.dtype),
        in_specs=[pl.BlockSpec(memory_space=pltpu.VMEM)],
        out_specs=pl.BlockSpec(memory_space=pltpu.VMEM),
        scratch_shapes=[pltpu.VMEM(x.shape, x.dtype)]
        + held
        + [pltpu.SemaphoreType.DMA((2, chunks))] * 4,
        compiler_params=line_params(cid),
        name="line_sum",
    )(x)


def attend_back_kernel(
    axis,
    n,
    chunks,
    lag,
    seq_len,
    block,
    x_ref,
    q_ref,
    dm_ref,
    k_ref,
    v_ref,
    norm_ref,
    own_ref,
    all_ref,
    cos_ref,
    sin_ref,
    o_ref,
    dq_ref,
    dkv_ref,
    red,
    held,
    *sems,
):
    rows, head_dim = k_ref.shape
    heads = q_ref.shape[1] // head_dim
    half_dim = head_dim // 2
    blocks = seq_len // block
    scale = head_dim ** (-0.5)
    dkv_ref[...] = jnp.zeros_like(dkv_ref)

    def finish(at):
        o_ref[at] = held[at].astype(o_ref.dtype)

    def job(j, carry):
        head = lax.rem(j, heads)
        row_block = lax.div(j, heads)
        seq = lax.div(row_block, blocks)
        block_at = lax.rem(row_block, blocks)
        own = pl.ds(pl.multiple_of(row_block * block, block), block)
        cols = pl.ds(pl.multiple_of(head * head_dim, head_dim), head_dim)
        low_cols = pl.ds(pl.multiple_of(head * head_dim, half_dim), half_dim)
        high_cols = pl.ds(pl.multiple_of(head * head_dim + half_dim, half_dim), half_dim)

        def run(reach):
            keys = pl.ds(pl.multiple_of(seq * seq_len, seq_len), reach)
            q = q_ref[own, cols]
            dm = dm_ref[own, cols]
            k = k_ref[keys, :]
            v = v_ref[keys, :]
            scores = right_dot(q, k) * scale
            q_pos = block_at * block + lax.broadcasted_iota(jnp.int32, scores.shape, 0)
            k_pos = lax.broadcasted_iota(jnp.int32, scores.shape, 1)
            same = own_ref[own, :] == all_ref[:, keys]
            probs = jnp.where(
                (k_pos <= q_pos) | same, jnp.exp(scores - norm_ref[head, own, :]), 0.0
            )
            d_probs = right_dot(dm, v)
            row_sum = jnp.sum(probs * d_probs, axis=1, keepdims=True)
            d_scores = (probs * (d_probs - row_sum)).astype(jnp.bfloat16)
            dkv_ref[keys, 0:head_dim] += left_dot(d_scores, q) * scale
            dkv_ref[keys, head_dim : 2 * head_dim] += left_dot(probs.astype(jnp.bfloat16), dm)
            dq = jnp.dot(d_scores, k, preferred_element_type=jnp.float32) * scale
            first = dq[:, :half_dim]
            second = dq[:, half_dim:]
            cos_tab = cos_ref[own, :]
            sin_tab = sin_ref[own, :]
            dq_ref[own, low_cols] = (first * cos_tab + second * sin_tab).astype(dq_ref.dtype)
            dq_ref[own, high_cols] = (second * cos_tab - first * sin_tab).astype(dq_ref.dtype)

        reaches = [min(seq_len, (b + 1) * block + PIECE) for b in range(blocks)]
        for reach in sorted(set(reaches)):
            first = reaches.index(reach)
            last = first + reaches.count(reach) - 1

            @pl.when((block_at >= first) & (block_at <= last))
            def _():
                run(reach)

        return carry

    job_count = heads * (rows // block)
    line_steps(axis, n, chunks, lag, x_ref, held, red, sems, finish, job, job_count)


def attend_back(x, q, dm, k, v, norm, own_ids, all_ids, cos_tab, sin_tab, axis, n, seq_len, cid):
    chunks = chunk_count(x.shape[0], 32, 16)
    block = min(256, seq_len)
    vmem = pl.BlockSpec(memory_space=pltpu.VMEM)
    return pl.pallas_call(
        functools.partial(attend_back_kernel, axis, n, chunks, 2, seq_len, block),
        out_shape=(
            jax.ShapeDtypeStruct(x.shape, jnp.bfloat16),
            jax.ShapeDtypeStruct(q.shape, jnp.bfloat16),
            jax.ShapeDtypeStruct((k.shape[0], 2 * k.shape[1]), jnp.float32),
        ),
        in_specs=[vmem] * 10,
        out_specs=(vmem, vmem, vmem),
        scratch_shapes=[pltpu.VMEM(x.shape, x.dtype)] * 2
        + [pltpu.SemaphoreType.DMA((2, chunks))] * 4,
        compiler_params=line_params(cid),
        name="attend_back",
    )(x, q, dm, k, v, norm, own_ids, all_ids, cos_tab, sin_tab)


def shards(
    block_input,
    image_starts,
    norm_gain,
    q_down,
    q_gain,
    q_up,
    k_proj,
    v_proj,
    out_proj,
    mlp_gain,
    w_gate,
    w_up,
    w_down,
    d_output,
):
    row_count, _ = block_input.shape
    dp_count = lax.axis_size("dp")
    tp_count = lax.axis_size("tensor")
    tp_index = lax.axis_index("tensor")

    def own_part(values, axis):
        split = values.shape[axis] // (dp_count * tp_count)
        shape = values.shape[:axis] + (dp_count, tp_count, split) + values.shape[axis + 1 :]
        picked = lax.dynamic_index_in_dim(values.reshape(shape), tp_index, axis + 1, keepdims=False)
        return picked

    seq_count = image_starts.shape[0]
    seq_len = row_count // seq_count
    head_dim = k_proj.shape[1]
    head_count = q_up.shape[1] // head_dim
    block_rows = min(512, seq_len)
    block_count = seq_len // block_rows
    score_scale = head_dim ** (-0.5)
    positions = jnp.arange(seq_len, dtype=jnp.float32)
    inv_freq = 10000.0 ** (-(jnp.arange(head_dim // 2, dtype=jnp.float32) * 2.0) / head_dim)
    angles = positions[:, None] * inv_freq[None, :]
    cos_all = jnp.tile(jnp.cos(angles), (seq_count, 1))
    sin_all = jnp.tile(jnp.sin(angles), (seq_count, 1))
    pos_int = jnp.arange(seq_len, dtype=jnp.int32)
    inside = (pos_int[None, :, None] >= image_starts[:, None, :]) & (
        pos_int[None, :, None] < image_starts[:, None, :] + PIECE
    )
    labels = jnp.arange(1, image_starts.shape[1] + 1, dtype=jnp.int32)
    piece_ids = jnp.sum(jnp.where(inside, labels, 0), axis=2)

    def block_scores(q_block, key_rows, seq_ids, row_start):
        raw = (
            jnp.einsum("qhd,kd->hqk", q_block, key_rows, preferred_element_type=jnp.float32)
            * score_scale
        )
        query_pos = row_start + jnp.arange(block_rows, dtype=jnp.int32)
        query_ids = lax.dynamic_slice_in_dim(seq_ids, row_start, block_rows)
        visible = (pos_int[None, :] <= query_pos[:, None]) | (
            query_ids[:, None] == seq_ids[None, :]
        ) & (query_ids[:, None] > 0)
        return jnp.where(visible[None], raw, masked_score)

    input_f32 = block_input.astype(jnp.float32)
    gain_attn = norm_gain.astype(jnp.float32)
    gain_query = q_gain.astype(jnp.float32)
    gain_mlp = mlp_gain.astype(jnp.float32)
    cotan_f32 = d_output.astype(jnp.float32)
    normed_one, scale_one = normalize(input_f32)
    normed_in = (normed_one * gain_attn).astype(jnp.bfloat16)
    q_latent = jnp.dot(normed_in, q_down, preferred_element_type=jnp.float32)
    q_unit, q_scale = normalize(q_latent)
    q_normed = (q_unit * gain_query).astype(jnp.bfloat16)
    q_raw = jnp.dot(q_normed, q_up, preferred_element_type=jnp.float32).reshape(
        row_count, head_count, head_dim
    )
    queries = rotate(q_raw, cos_all[:, None, :], sin_all[:, None, :]).astype(jnp.bfloat16)
    key_rows = rotate(
        jnp.dot(normed_in, k_proj, preferred_element_type=jnp.float32), cos_all, sin_all
    ).astype(jnp.bfloat16)
    val_rows = jnp.dot(normed_in, v_proj, preferred_element_type=jnp.float32).astype(jnp.bfloat16)
    query_seq = queries.reshape(seq_count, block_count, block_rows, head_count, head_dim)
    key_seq = key_rows.reshape(seq_count, seq_len, head_dim)
    val_seq = val_rows.reshape(seq_count, seq_len, head_dim)
    block_ids = jnp.arange(block_count, dtype=jnp.int32)

    def forward_seq(seq_item):
        q_all, seq_keys, seq_vals, seq_ids = seq_item

        def forward_block(block_item):
            q_block, blk_index = block_item
            scores = block_scores(q_block, seq_keys, seq_ids, blk_index * block_rows)
            row_max = jnp.max(scores, axis=-1, keepdims=True)
            exp_terms = jnp.exp(scores - row_max)
            row_sum = jnp.sum(exp_terms, axis=-1, keepdims=True)
            attn_probs = (exp_terms / row_sum).astype(jnp.bfloat16)
            mixed_block = jnp.einsum(
                "hqk,kd->qhd", attn_probs, seq_vals, preferred_element_type=jnp.float32
            )
            return (mixed_block.astype(jnp.bfloat16), (row_max + jnp.log(row_sum))[..., 0])

        return lax.map(forward_block, (q_all, block_ids))

    mixed_seq, log_norm = lax.map(forward_seq, (query_seq, key_seq, val_seq, piece_ids))
    mixed_heads = mixed_seq.reshape(row_count, head_count * head_dim)
    first_here = (tp_index == 0).astype(jnp.float32)
    hidden_part = (
        jnp.dot(mixed_heads, out_proj, preferred_element_type=jnp.float32) + first_here * input_f32
    )
    hidden_in = line_sum(hidden_part, "tensor", tp_count, 1)
    normed_two, scale_two = normalize(hidden_in)
    normed_mid = (normed_two * gain_mlp).astype(jnp.bfloat16)
    gate_pre = jnp.dot(normed_mid, w_gate, preferred_element_type=jnp.float32)
    up_pre = jnp.dot(normed_mid, w_up, preferred_element_type=jnp.float32)
    gate_sig = jax.nn.sigmoid(gate_pre)
    hidden_act = (gate_pre * gate_sig * up_pre).astype(jnp.bfloat16)
    half_rows = row_count // 2
    out_part_one, out_part_two = (
        jnp.dot(hidden_act[at], w_down, preferred_element_type=jnp.float32)
        + first_here * hidden_in[at]
        for at in (slice(0, half_rows), slice(half_rows, row_count))
    )
    grad_down = left_dot(hidden_act, d_output)
    d_act = right_dot(d_output, w_down)
    d_gate = (d_act * up_pre * gate_sig * (1.0 + gate_pre * (1.0 - gate_sig))).astype(jnp.bfloat16)
    d_up = (d_act * gate_pre * gate_sig).astype(jnp.bfloat16)
    grad_gate = left_dot(normed_mid, d_gate)
    grad_up = left_dot(normed_mid, d_up)
    d_mid_part = right_dot(d_gate, w_gate) + right_dot(d_up, w_up)
    d_mid_part, grad_down, grad_gate, grad_up = lax.optimization_barrier(
        (d_mid_part, grad_down, grad_gate, grad_up)
    )
    grad_gate = lax.psum_scatter(grad_gate, "dp", scatter_dimension=0, tiled=True)
    grad_up = lax.psum_scatter(grad_up, "dp", scatter_dimension=0, tiled=True)
    grad_down = lax.psum_scatter(grad_down, "dp", scatter_dimension=1, tiled=True)
    d_mid = line_sum(d_mid_part, "tensor", tp_count, 1)
    grad_gain_mlp = jnp.sum(d_mid * normed_two, axis=0)
    d_hidden = cotan_f32 + norm_back(d_mid * gain_mlp, normed_two, scale_two)
    d_hidden_low = d_hidden.astype(jnp.bfloat16)
    grad_out = left_dot(mixed_heads, d_hidden_low)
    d_mixed = right_dot(d_hidden_low, out_proj).astype(jnp.bfloat16)
    log_cols = jnp.transpose(log_norm, (2, 0, 1, 3)).reshape(head_count, row_count, 1)
    out_part_one, grad_out = lax.optimization_barrier((out_part_one, grad_out))
    grad_out = lax.psum_scatter(grad_out, "dp", scatter_dimension=1, tiled=True)
    output_one, d_q_raw, key_val_part = attend_back(
        out_part_one,
        queries.reshape(row_count, head_count * head_dim),
        d_mixed,
        key_rows,
        val_rows,
        log_cols,
        jnp.where(piece_ids > 0, piece_ids, -1).reshape(row_count, 1),
        piece_ids.reshape(1, row_count),
        cos_all,
        sin_all,
        "tensor",
        tp_count,
        seq_len,
        3,
    )
    grad_query_up = left_dot(q_normed, d_q_raw)
    d_bq_part = right_dot(d_q_raw, q_up)
    d_bq_part, grad_query_up = lax.optimization_barrier((d_bq_part, grad_query_up))
    grad_query_up = lax.psum_scatter(grad_query_up, "dp", scatter_dimension=0, tiled=True)
    query_key_val = line_sum(
        jnp.concatenate([d_bq_part, key_val_part], axis=1), "tensor", tp_count, 2
    )
    d_q_normed = query_key_val[:, : q_gain.shape[0]]
    key_val_full = query_key_val[:, q_gain.shape[0] :]
    d_key_low = unrotate(key_val_full[:, :head_dim], cos_all, sin_all).astype(jnp.bfloat16)
    d_val_low = key_val_full[:, head_dim:].astype(jnp.bfloat16)
    grad_gain_query = jnp.sum(d_q_normed * q_unit, axis=0)
    d_latent = norm_back(d_q_normed * gain_query, q_unit, q_scale).astype(jnp.bfloat16)
    d_normed_in = (
        right_dot(d_latent, q_down) + right_dot(d_key_low, k_proj) + right_dot(d_val_low, v_proj)
    )
    grad_gain_attn = jnp.sum(d_normed_in * normed_one, axis=0)
    grad_input = (d_hidden + norm_back(d_normed_in * gain_attn, normed_one, scale_one)).astype(
        jnp.bfloat16
    )
    own_in = own_part(normed_in, 1).reshape(row_count, -1)
    own_grads = left_dot(own_in, jnp.concatenate([d_latent, d_key_low, d_val_low], axis=1))
    own_rows = own_grads.shape[0]
    gain_one = own_part(grad_gain_attn, 0).reshape(own_rows, 1)
    gain_two = own_part(grad_gain_mlp, 0).reshape(own_rows, 1)
    gain_mid = own_part(grad_gain_query, 0)
    own_mid = gain_mid.shape[1]
    gain_mid = jnp.pad(gain_mid, ((0, 0), (0, own_rows // dp_count - own_mid))).reshape(own_rows, 1)
    gain_cols = jnp.concatenate([gain_one, gain_two, gain_mid], axis=1)
    own_grads = jnp.concatenate([own_grads, jnp.pad(gain_cols, ((0, 0), (0, 125)))], axis=1)
    own_sum = lax.psum_scatter(own_grads, "dp", scatter_dimension=0, tiled=True)
    output_two = line_sum(out_part_two, "tensor", tp_count, 4, low=True)
    block_output = jnp.concatenate([output_one, output_two], axis=0)
    rank = q_down.shape[1]
    grad_qd = own_sum[:, :rank]
    grad_key = own_sum[:, rank : rank + head_dim]
    grad_val = own_sum[:, rank + head_dim : rank + 2 * head_dim]
    gain_at = rank + 2 * head_dim
    grad_g1 = own_sum[:, gain_at]
    grad_g2 = own_sum[:, gain_at + 1]
    grad_gq = own_sum[:own_mid, gain_at + 2]
    return (
        block_output,
        grad_input,
        grad_g1,
        grad_qd,
        grad_gq,
        grad_query_up,
        grad_key,
        grad_val,
        grad_out,
        grad_g2,
        grad_gate,
        grad_up,
        grad_down,
    )


def solution(mesh):
    placed = (
        P("dp", None),
        P("dp", None),
        P(),
        P(),
        P(),
        P(None, "tensor"),
        P(),
        P(),
        P("tensor", None),
        P(),
        P(None, "tensor"),
        P(None, "tensor"),
        P("tensor", None),
        P("dp", None),
    )

    return jax.shard_map(
        shards,
        mesh=mesh,
        in_specs=placed,
        out_specs=(
            P("dp", None),
            P("dp", None),
            P(("dp", "tensor")),
            P(("dp", "tensor"), None),
            P(("dp", "tensor")),
            P("dp", "tensor"),
            P(("dp", "tensor"), None),
            P(("dp", "tensor"), None),
            P("tensor", "dp"),
            P(("dp", "tensor")),
            P("dp", "tensor"),
            P("dp", "tensor"),
            P("tensor", "dp"),
        ),
        check_vma=False,
    )
```

```python
import functools

import jax
import jax.numpy as jnp
from jax import lax
from jax.experimental import pallas as pl
from jax.experimental.pallas import tpu as pltpu
from jax.sharding import PartitionSpec as P


MESH = pl.DeviceIdType.MESH

PIECE = 256


epsilon = 1e-06
masked_score = -1e30


def normalize(values):
    scale_rows = lax.rsqrt(jnp.mean(values * values, axis=-1, keepdims=True) + epsilon)
    return (values * scale_rows, scale_rows)


def norm_back(grad_normed, normed, scale_rows):
    return scale_rows * (
        grad_normed - normed * jnp.mean(grad_normed * normed, axis=-1, keepdims=True)
    )


def left_dot(left, right):
    return lax.dot_general(
        left, right, (((0,), (0,)), ((), ())), preferred_element_type=jnp.float32
    )


def right_dot(left, right):
    return lax.dot_general(
        left, right, (((1,), (1,)), ((), ())), preferred_element_type=jnp.float32
    )


def rotate(values, cos_tab, sin_tab):
    half = values.shape[-1] // 2
    first_half = values[..., :half]
    second_half = values[..., half:]
    return jnp.concatenate(
        [
            first_half * cos_tab - second_half * sin_tab,
            second_half * cos_tab + first_half * sin_tab,
        ],
        axis=-1,
    )


def unrotate(grads, cos_tab, sin_tab):
    half = grads.shape[-1] // 2
    first_half = grads[..., :half]
    second_half = grads[..., half:]
    return jnp.concatenate(
        [
            first_half * cos_tab + second_half * sin_tab,
            second_half * cos_tab - first_half * sin_tab,
        ],
        axis=-1,
    )


def line_steps(axis, n, chunks, lag, x_ref, held, red, sems, finish, job, job_range):
    me = lax.axis_index(axis)
    rows = x_ref.shape[0] // (2 * chunks)
    s_red, r_red, s_fin, r_fin = sems
    barrier = pltpu.get_barrier_semaphore()

    @pl.when(me > 0)
    def _():
        pl.semaphore_signal(barrier, inc=1, device_id={axis: me - 1}, device_id_type=MESH)

    @pl.when(me < n - 1)
    def _():
        pl.semaphore_signal(barrier, inc=1, device_id={axis: me + 1}, device_id_type=MESH)

    @pl.when((me == 0) | (me == n - 1))
    def _():
        pl.semaphore_wait(barrier, 1)

    @pl.when((me > 0) & (me < n - 1))
    def _():
        pl.semaphore_wait(barrier, 2)

    def at(half, c):
        return pl.ds(pl.multiple_of((half * chunks + c) * rows, rows), rows)

    def sum_copy(src, half, c):
        return pltpu.make_async_remote_copy(
            src_ref=src.at[at(half, c)],
            dst_ref=red.at[at(half, c)],
            send_sem=s_red.at[half, c],
            recv_sem=r_red.at[half, c],
            device_id={axis: me - 1 if half == 0 else me + 1},
            device_id_type=MESH,
        )

    def fin_copy(half, c):
        return pltpu.make_async_remote_copy(
            src_ref=held.at[at(half, c)],
            dst_ref=held.at[at(half, c)],
            send_sem=s_fin.at[half, c],
            recv_sem=r_fin.at[half, c],
            device_id={axis: me + 1 if half == 0 else me - 1},
            device_id_type=MESH,
        )

    steps = chunks + 2 * lag * (n - 1)

    def step(s, carry):
        for half in (0, 1):
            hop = (n - 1 - me) if half == 0 else me
            c = s - lag * hop
            ok = (c >= 0) & (c < chunks)

            @pl.when(ok & (hop == 0))
            def _():
                sum_copy(x_ref, half, c).start()

            @pl.when(ok & (hop > 0) & (hop < n - 1))
            def _():
                sum_copy(x_ref, half, c).wait_recv()
                red[at(half, c)] = red[at(half, c)] + x_ref[at(half, c)]
                sum_copy(red, half, c).start()

            @pl.when(ok & (hop == n - 1))
            def _():
                sum_copy(x_ref, half, c).wait_recv()
                held[at(half, c)] = red[at(half, c)] + x_ref[at(half, c)]
                fin_copy(half, c).start()
                finish(at(half, c))

        for half in (0, 1):
            back = me if half == 0 else (n - 1 - me)
            c = s - lag * (n - 1) - lag * back
            ok = (c >= 0) & (c < chunks)

            @pl.when(ok & (back > 0))
            def _():
                fin_copy(half, c).wait_recv()

            @pl.when(ok & (back > 0) & (back < n - 1))
            def _():
                fin_copy(half, c).start()

            @pl.when(ok & (back > 0))
            def _():
                finish(at(half, c))

        if job is not None:
            lax.fori_loop(*job_range(s, steps), job, 0)
        return carry

    lax.fori_loop(0, steps, step, 0)

    def drain(c, carry):
        for half in (0, 1):
            hop = (n - 1 - me) if half == 0 else me

            @pl.when(hop < n - 1)
            def _():
                sum_copy(x_ref, half, c).wait_send()

            @pl.when(hop > 0)
            def _():
                fin_copy(half, c).wait_send()

        return carry

    lax.fori_loop(0, chunks, drain, 0)


def line_kernel(axis, n, chunks, lag, x_ref, o_ref, red, *sems):
    line_steps(axis, n, chunks, lag, x_ref, o_ref, red, sems, lambda at: None, None, None)


def line_low_kernel(axis, n, chunks, lag, x_ref, o_ref, red, held, *sems):
    def finish(at):
        o_ref[at] = held[at].astype(o_ref.dtype)

    line_steps(axis, n, chunks, lag, x_ref, held, red, sems, finish, None, None)


def chunk_count(rows, most, tile):
    chunks = most
    while rows % (2 * chunks * tile):
        chunks -= 1
    return chunks


def line_params(cid):
    return pltpu.CompilerParams(
        collective_id=cid, has_side_effects=True, vmem_limit_bytes=56 << 20
    )


def line_sum(x, axis, n, cid, low=False):
    chunks = chunk_count(x.shape[0], 32, 16 if low else 8)
    held = [pltpu.VMEM(x.shape, x.dtype)] if low else []
    return pl.pallas_call(
        functools.partial(line_low_kernel if low else line_kernel, axis, n, chunks, 2),
        out_shape=jax.ShapeDtypeStruct(x.shape, jnp.bfloat16 if low else x.dtype),
        in_specs=[pl.BlockSpec(memory_space=pltpu.VMEM)],
        out_specs=pl.BlockSpec(memory_space=pltpu.VMEM),
        scratch_shapes=[pltpu.VMEM(x.shape, x.dtype)]
        + held
        + [pltpu.SemaphoreType.DMA((2, chunks))] * 4,
        compiler_params=line_params(cid),
        name="line_sum",
    )(x)


def attend_kernel(
    axis,
    n,
    chunks,
    lag,
    seq_len,
    block,
    raw_ref,
    k_ref,
    v_ref,
    own_ref,
    all_ref,
    cos_ref,
    sin_ref,
    out_ref,
    base_ref,
    o_ref,
    q_ref,
    mixed_ref,
    norm_ref,
    part,
    red,
    *sems,
):
    rows, head_dim = k_ref.shape
    heads = raw_ref.shape[1] // head_dim
    half_dim = head_dim // 2
    blocks = seq_len // block
    scale = head_dim ** (-0.5)
    pairs = rows // (2 * block)
    turns = heads + 1
    pair_jobs = 2 * turns

    def job(j, carry):
        pair = lax.div(j, pair_jobs)
        side = lax.div(lax.rem(j, pair_jobs), turns)
        head = lax.rem(j, turns)
        row_block = side * pairs + pair
        seq = lax.div(row_block, blocks)
        block_at = lax.rem(row_block, blocks)
        own = pl.ds(pl.multiple_of(row_block * block, block), block)
        cols = pl.ds(pl.multiple_of(head * head_dim, head_dim), head_dim)
        low_cols = pl.ds(pl.multiple_of(head * head_dim, half_dim), half_dim)
        high_cols = pl.ds(pl.multiple_of(head * head_dim + half_dim, half_dim), half_dim)

        def run(reach):
            keys = pl.ds(pl.multiple_of(seq * seq_len, seq_len), reach)
            first = raw_ref[own, low_cols]
            second = raw_ref[own, high_cols]
            cos_tab = cos_ref[own, :]
            sin_tab = sin_ref[own, :]
            q_ref[own, low_cols] = (first * cos_tab - second * sin_tab).astype(q_ref.dtype)
            q_ref[own, high_cols] = (second * cos_tab + first * sin_tab).astype(q_ref.dtype)
            scores = right_dot(q_ref[own, cols], k_ref[keys, :]) * scale
            q_pos = block_at * block + lax.broadcasted_iota(jnp.int32, scores.shape, 0)
            k_pos = lax.broadcasted_iota(jnp.int32, scores.shape, 1)
            same = own_ref[own, :] == all_ref[:, keys]
            scores = jnp.where((k_pos <= q_pos) | same, scores, masked_score)
            row_max = jnp.max(scores, axis=1, keepdims=True)
            exp_terms = jnp.exp(scores - row_max)
            row_sum = jnp.sum(exp_terms, axis=1, keepdims=True)
            probs = (exp_terms * (1.0 / row_sum)).astype(jnp.bfloat16)
            mixed = jnp.dot(probs, v_ref[keys, :], preferred_element_type=jnp.float32)
            mixed_ref[own, cols] = mixed.astype(mixed_ref.dtype)
            norm_ref[head, own, :] = row_max + jnp.log(row_sum)

        reaches = reach_list(seq_len, block)
        for reach in sorted(set(reaches)):
            first = reaches.index(reach)
            last = first + reaches.count(reach) - 1

            @pl.when((head < heads) & (block_at >= first) & (block_at <= last))
            def _():
                run(reach)

        @pl.when(head == heads)
        def _():
            part[own, :] = jnp.dot(
                mixed_ref[own, :], out_ref[...], preferred_element_type=jnp.float32
            )

        @pl.when((head == heads) & (lax.axis_index(axis) == 0))
        def _():
            part[own, :] += base_ref[own, :].astype(jnp.float32)

        return carry

    lax.fori_loop(0, pair_jobs, job, 0)
    pair_steps = chunks // pairs

    def job_range(s, steps):
        return tuple(
            jnp.minimum((pair_steps + at) * pair_jobs // pair_steps, pairs * pair_jobs)
            for at in (s, s + 1)
        )

    line_steps(axis, n, chunks, lag, part, o_ref, red, sems, lambda at: None, job, job_range)


def reach_list(seq_len, block):
    step = max(256, block)
    ends = [(b + 1) * block + PIECE for b in range(seq_len // block)]
    return [min(seq_len, -(-end // step) * step) for end in ends]


def attend(raw, k, v, own_ids, all_ids, cos_tab, sin_tab, out_proj, base, axis, n, seq_len, cid):
    rows, width = base.shape
    block = min(128, seq_len)
    chunks = chunk_count(rows, 32, 8)
    vmem = pl.BlockSpec(memory_space=pltpu.VMEM)
    return pl.pallas_call(
        functools.partial(attend_kernel, axis, n, chunks, 2, seq_len, block),
        out_shape=(
            jax.ShapeDtypeStruct((rows, width), jnp.float32),
            jax.ShapeDtypeStruct(raw.shape, jnp.bfloat16),
            jax.ShapeDtypeStruct(raw.shape, jnp.bfloat16),
            jax.ShapeDtypeStruct((raw.shape[1] // k.shape[1], rows, 1), jnp.float32),
        ),
        in_specs=[vmem] * 9,
        out_specs=(vmem,) * 4,
        scratch_shapes=[pltpu.VMEM((rows, width), jnp.float32)] * 2
        + [pltpu.SemaphoreType.DMA((2, chunks))] * 4,
        compiler_params=pltpu.CompilerParams(
            collective_id=cid, has_side_effects=True, vmem_limit_bytes=60 << 20
        ),
        name="attend",
    )(raw, k, v, own_ids, all_ids, cos_tab, sin_tab, out_proj, base)


def attend_back_kernel(
    axis,
    n,
    chunks,
    lag,
    seq_len,
    block,
    x_ref,
    q_ref,
    dm_ref,
    k_ref,
    v_ref,
    norm_ref,
    own_ref,
    all_ref,
    cos_ref,
    sin_ref,
    up_ref,
    o_ref,
    dq_ref,
    sums_ref,
    red,
    held,
    *sems,
):
    rows, head_dim = k_ref.shape
    heads = q_ref.shape[1] // head_dim
    half_dim = head_dim // 2
    blocks = seq_len // block
    scale = head_dim ** (-0.5)
    rank = up_ref.shape[0]
    key_cols = slice(rank, rank + head_dim)
    val_cols = slice(rank + head_dim, rank + 2 * head_dim)
    sums_ref[:, rank:] = jnp.zeros((rows, 2 * head_dim), jnp.float32)

    def finish(at):
        o_ref[at] = held[at].astype(o_ref.dtype)

    def job(j, carry):
        head = lax.rem(j, heads)
        row_block = lax.div(j, heads)
        seq = lax.div(row_block, blocks)
        block_at = lax.rem(row_block, blocks)
        own = pl.ds(pl.multiple_of(row_block * block, block), block)
        cols = pl.ds(pl.multiple_of(head * head_dim, head_dim), head_dim)
        low_cols = pl.ds(pl.multiple_of(head * head_dim, half_dim), half_dim)
        high_cols = pl.ds(pl.multiple_of(head * head_dim + half_dim, half_dim), half_dim)

        def run(reach):
            keys = pl.ds(pl.multiple_of(seq * seq_len, seq_len), reach)
            q = q_ref[own, cols]
            dm = dm_ref[own, cols]
            k = k_ref[keys, :]
            v = v_ref[keys, :]
            scores = right_dot(q, k) * scale
            q_pos = block_at * block + lax.broadcasted_iota(jnp.int32, scores.shape, 0)
            k_pos = lax.broadcasted_iota(jnp.int32, scores.shape, 1)
            same = own_ref[own, :] == all_ref[:, keys]
            probs = jnp.where(
                (k_pos <= q_pos) | same, jnp.exp(scores - norm_ref[head, own, :]), 0.0
            )
            d_probs = right_dot(dm, v)
            row_sum = jnp.sum(probs * d_probs, axis=1, keepdims=True)
            d_scores = (probs * (d_probs - row_sum)).astype(jnp.bfloat16)
            sums_ref[keys, key_cols] += left_dot(d_scores, q) * scale
            sums_ref[keys, val_cols] += left_dot(probs.astype(jnp.bfloat16), dm)
            dq = jnp.dot(d_scores, k, preferred_element_type=jnp.float32) * scale
            first = dq[:, :half_dim]
            second = dq[:, half_dim:]
            cos_tab = cos_ref[own, :]
            sin_tab = sin_ref[own, :]
            dq_ref[own, low_cols] = (first * cos_tab + second * sin_tab).astype(dq_ref.dtype)
            dq_ref[own, high_cols] = (second * cos_tab - first * sin_tab).astype(dq_ref.dtype)

        reaches = reach_list(seq_len, block)
        for reach in sorted(set(reaches)):
            first = reaches.index(reach)
            last = first + reaches.count(reach) - 1

            @pl.when((block_at >= first) & (block_at <= last))
            def _():
                run(reach)

        @pl.when(head == heads - 1)
        def _():
            sums_ref[own, 0:rank] = right_dot(dq_ref[own, :], up_ref[...])

        return carry

    job_count = heads * (rows // block)

    def job_range(s, steps):
        return s * job_count // steps, (s + 1) * job_count // steps

    line_steps(axis, n, chunks, lag, x_ref, held, red, sems, finish, job, job_range)


def attend_back(
    x, q, dm, k, v, norm, own_ids, all_ids, cos_tab, sin_tab, q_up, axis, n, seq_len, cid
):
    chunks = chunk_count(x.shape[0], 32, 16)
    block = min(256, seq_len)
    vmem = pl.BlockSpec(memory_space=pltpu.VMEM)
    return pl.pallas_call(
        functools.partial(attend_back_kernel, axis, n, chunks, 2, seq_len, block),
        out_shape=(
            jax.ShapeDtypeStruct(x.shape, jnp.bfloat16),
            jax.ShapeDtypeStruct(q.shape, jnp.bfloat16),
            jax.ShapeDtypeStruct((k.shape[0], q_up.shape[0] + 2 * k.shape[1]), jnp.float32),
        ),
        in_specs=[vmem] * 11,
        out_specs=(vmem, vmem, vmem),
        scratch_shapes=[pltpu.VMEM(x.shape, x.dtype)] * 2
        + [pltpu.SemaphoreType.DMA((2, chunks))] * 4,
        compiler_params=line_params(cid),
        name="attend_back",
    )(x, q, dm, k, v, norm, own_ids, all_ids, cos_tab, sin_tab, q_up)


def shards(
    block_input,
    image_starts,
    norm_gain,
    q_down,
    q_gain,
    q_up,
    k_proj,
    v_proj,
    out_proj,
    mlp_gain,
    w_gate,
    w_up,
    w_down,
    d_output,
):
    row_count, _ = block_input.shape
    dp_count = lax.axis_size("dp")
    tp_count = lax.axis_size("tensor")
    tp_index = lax.axis_index("tensor")

    def own_part(values, axis):
        split = values.shape[axis] // (dp_count * tp_count)
        shape = values.shape[:axis] + (dp_count, tp_count, split) + values.shape[axis + 1 :]
        picked = lax.dynamic_index_in_dim(values.reshape(shape), tp_index, axis + 1, keepdims=False)
        return picked

    seq_count = image_starts.shape[0]
    seq_len = row_count // seq_count
    head_dim = k_proj.shape[1]
    positions = jnp.arange(seq_len, dtype=jnp.float32)
    inv_freq = 10000.0 ** (-(jnp.arange(head_dim // 2, dtype=jnp.float32) * 2.0) / head_dim)
    angles = positions[:, None] * inv_freq[None, :]
    cos_all = jnp.tile(jnp.cos(angles), (seq_count, 1))
    sin_all = jnp.tile(jnp.sin(angles), (seq_count, 1))
    pos_int = jnp.arange(seq_len, dtype=jnp.int32)
    inside = (pos_int[None, :, None] >= image_starts[:, None, :]) & (
        pos_int[None, :, None] < image_starts[:, None, :] + PIECE
    )
    labels = jnp.arange(1, image_starts.shape[1] + 1, dtype=jnp.int32)
    piece_ids = jnp.sum(jnp.where(inside, labels, 0), axis=2)

    own_ids = jnp.where(piece_ids > 0, piece_ids, -1).reshape(row_count, 1)
    all_ids = piece_ids.reshape(1, row_count)
    input_f32 = block_input.astype(jnp.float32)
    gain_attn = norm_gain.astype(jnp.float32)
    gain_query = q_gain.astype(jnp.float32)
    gain_mlp = mlp_gain.astype(jnp.float32)
    cotan_f32 = d_output.astype(jnp.float32)
    normed_one, scale_one = normalize(input_f32)
    normed_in = (normed_one * gain_attn).astype(jnp.bfloat16)
    q_latent = jnp.dot(normed_in, q_down, preferred_element_type=jnp.float32)
    q_unit, q_scale = normalize(q_latent)
    q_normed = (q_unit * gain_query).astype(jnp.bfloat16)
    q_raw = jnp.dot(q_normed, q_up, preferred_element_type=jnp.float32)
    key_rows = rotate(
        jnp.dot(normed_in, k_proj, preferred_element_type=jnp.float32), cos_all, sin_all
    ).astype(jnp.bfloat16)
    val_rows = jnp.dot(normed_in, v_proj, preferred_element_type=jnp.float32).astype(jnp.bfloat16)
    first_here = (tp_index == 0).astype(jnp.float32)
    hidden_in, queries, mixed_heads, log_norm = attend(
        q_raw,
        key_rows,
        val_rows,
        own_ids,
        all_ids,
        cos_all,
        sin_all,
        out_proj,
        block_input,
        "tensor",
        tp_count,
        seq_len,
        5,
    )
    normed_two, scale_two = normalize(hidden_in)
    normed_mid = (normed_two * gain_mlp).astype(jnp.bfloat16)
    gate_pre = jnp.dot(normed_mid, w_gate, preferred_element_type=jnp.float32)
    up_pre = jnp.dot(normed_mid, w_up, preferred_element_type=jnp.float32)
    gate_sig = jax.nn.sigmoid(gate_pre)
    hidden_act = (gate_pre * gate_sig * up_pre).astype(jnp.bfloat16)
    half_rows = row_count // 2
    out_part_one, out_part_two = (
        jnp.dot(hidden_act[at], w_down, preferred_element_type=jnp.float32)
        + first_here * hidden_in[at]
        for at in (slice(0, half_rows), slice(half_rows, row_count))
    )
    grad_down = left_dot(hidden_act, d_output)
    d_act = right_dot(d_output, w_down)
    d_gate = (d_act * up_pre * gate_sig * (1.0 + gate_pre * (1.0 - gate_sig))).astype(jnp.bfloat16)
    d_up = (d_act * gate_pre * gate_sig).astype(jnp.bfloat16)
    grad_gate = left_dot(normed_mid, d_gate)
    grad_up = left_dot(normed_mid, d_up)
    d_mid_part = right_dot(d_gate, w_gate) + right_dot(d_up, w_up)
    d_mid_part, grad_down, grad_gate, grad_up = lax.optimization_barrier(
        (d_mid_part, grad_down, grad_gate, grad_up)
    )
    grad_gate = lax.psum_scatter(grad_gate, "dp", scatter_dimension=0, tiled=True)
    grad_up = lax.psum_scatter(grad_up, "dp", scatter_dimension=0, tiled=True)
    grad_down = lax.psum_scatter(grad_down, "dp", scatter_dimension=1, tiled=True)
    d_mid = line_sum(d_mid_part, "tensor", tp_count, 1)
    grad_gain_mlp = jnp.sum(d_mid * normed_two, axis=0)
    d_hidden = cotan_f32 + norm_back(d_mid * gain_mlp, normed_two, scale_two)
    d_hidden_low = d_hidden.astype(jnp.bfloat16)
    grad_out = left_dot(mixed_heads, d_hidden_low)
    d_mixed = right_dot(d_hidden_low, out_proj).astype(jnp.bfloat16)
    out_part_one, grad_out = lax.optimization_barrier((out_part_one, grad_out))
    grad_out = lax.psum_scatter(grad_out, "dp", scatter_dimension=1, tiled=True)
    output_one, d_q_raw, query_key_val = attend_back(
        out_part_one,
        queries,
        d_mixed,
        key_rows,
        val_rows,
        log_norm,
        own_ids,
        all_ids,
        cos_all,
        sin_all,
        q_up,
        "tensor",
        tp_count,
        seq_len,
        3,
    )
    grad_query_up = left_dot(q_normed, d_q_raw)
    query_key_val, grad_query_up = lax.optimization_barrier((query_key_val, grad_query_up))
    grad_query_up = lax.psum_scatter(grad_query_up, "dp", scatter_dimension=0, tiled=True)
    query_key_val = line_sum(query_key_val, "tensor", tp_count, 2)
    d_q_normed = query_key_val[:, : q_gain.shape[0]]
    key_val_full = query_key_val[:, q_gain.shape[0] :]
    d_key_low = unrotate(key_val_full[:, :head_dim], cos_all, sin_all).astype(jnp.bfloat16)
    d_val_low = key_val_full[:, head_dim:].astype(jnp.bfloat16)
    grad_gain_query = jnp.sum(d_q_normed * q_unit, axis=0)
    d_latent = norm_back(d_q_normed * gain_query, q_unit, q_scale).astype(jnp.bfloat16)
    d_normed_in = (
        right_dot(d_latent, q_down) + right_dot(d_key_low, k_proj) + right_dot(d_val_low, v_proj)
    )
    grad_gain_attn = jnp.sum(d_normed_in * normed_one, axis=0)
    grad_input = (d_hidden + norm_back(d_normed_in * gain_attn, normed_one, scale_one)).astype(
        jnp.bfloat16
    )
    own_in = own_part(normed_in, 1).reshape(row_count, -1)
    own_grads = left_dot(own_in, jnp.concatenate([d_latent, d_key_low, d_val_low], axis=1))
    own_rows = own_grads.shape[0]
    gain_one = own_part(grad_gain_attn, 0).reshape(own_rows, 1)
    gain_two = own_part(grad_gain_mlp, 0).reshape(own_rows, 1)
    gain_mid = own_part(grad_gain_query, 0)
    own_mid = gain_mid.shape[1]
    gain_mid = jnp.pad(gain_mid, ((0, 0), (0, own_rows // dp_count - own_mid))).reshape(own_rows, 1)
    gain_cols = jnp.concatenate([gain_one, gain_two, gain_mid], axis=1)
    own_grads = jnp.concatenate([own_grads, jnp.pad(gain_cols, ((0, 0), (0, 125)))], axis=1)
    own_sum = lax.psum_scatter(own_grads, "dp", scatter_dimension=0, tiled=True)
    output_two = line_sum(out_part_two, "tensor", tp_count, 4, low=True)
    block_output = jnp.concatenate([output_one, output_two], axis=0)
    rank = q_down.shape[1]
    grad_qd = own_sum[:, :rank]
    grad_key = own_sum[:, rank : rank + head_dim]
    grad_val = own_sum[:, rank + head_dim : rank + 2 * head_dim]
    gain_at = rank + 2 * head_dim
    grad_g1 = own_sum[:, gain_at]
    grad_g2 = own_sum[:, gain_at + 1]
    grad_gq = own_sum[:own_mid, gain_at + 2]
    return (
        block_output,
        grad_input,
        grad_g1,
        grad_qd,
        grad_gq,
        grad_query_up,
        grad_key,
        grad_val,
        grad_out,
        grad_g2,
        grad_gate,
        grad_up,
        grad_down,
    )


def solution(mesh):
    placed = (
        P("dp", None),
        P("dp", None),
        P(),
        P(),
        P(),
        P(None, "tensor"),
        P(),
        P(),
        P("tensor", None),
        P(),
        P(None, "tensor"),
        P(None, "tensor"),
        P("tensor", None),
        P("dp", None),
    )

    return jax.shard_map(
        shards,
        mesh=mesh,
        in_specs=placed,
        out_specs=(
            P("dp", None),
            P("dp", None),
            P(("dp", "tensor")),
            P(("dp", "tensor"), None),
            P(("dp", "tensor")),
            P("dp", "tensor"),
            P(("dp", "tensor"), None),
            P(("dp", "tensor"), None),
            P("tensor", "dp"),
            P(("dp", "tensor")),
            P("dp", "tensor"),
            P("dp", "tensor"),
            P("tensor", "dp"),
        ),
        check_vma=False,
    )
```

```python
import functools

import jax
import jax.numpy as jnp
from jax import lax
from jax.experimental import pallas as pl
from jax.experimental.pallas import tpu as pltpu
from jax.sharding import PartitionSpec as P


MESH = pl.DeviceIdType.MESH

PIECE = 256


epsilon = 1e-06
masked_score = -1e30


def normalize(values):
    scale_rows = lax.rsqrt(jnp.mean(values * values, axis=-1, keepdims=True) + epsilon)
    return (values * scale_rows, scale_rows)


def norm_back(grad_normed, normed, scale_rows):
    return scale_rows * (
        grad_normed - normed * jnp.mean(grad_normed * normed, axis=-1, keepdims=True)
    )


def left_dot(left, right):
    return lax.dot_general(
        left, right, (((0,), (0,)), ((), ())), preferred_element_type=jnp.float32
    )


def right_dot(left, right):
    return lax.dot_general(
        left, right, (((1,), (1,)), ((), ())), preferred_element_type=jnp.float32
    )


def rotate(values, cos_tab, sin_tab):
    half = values.shape[-1] // 2
    first_half = values[..., :half]
    second_half = values[..., half:]
    return jnp.concatenate(
        [
            first_half * cos_tab - second_half * sin_tab,
            second_half * cos_tab + first_half * sin_tab,
        ],
        axis=-1,
    )


def unrotate(grads, cos_tab, sin_tab):
    half = grads.shape[-1] // 2
    first_half = grads[..., :half]
    second_half = grads[..., half:]
    return jnp.concatenate(
        [
            first_half * cos_tab + second_half * sin_tab,
            second_half * cos_tab - first_half * sin_tab,
        ],
        axis=-1,
    )


def line_steps(axis, n, chunks, lag, x_ref, held, red, sems, finish, job, job_range):
    me = lax.axis_index(axis)
    rows = x_ref.shape[0] // (2 * chunks)
    s_red, r_red, s_fin, r_fin = sems
    barrier = pltpu.get_barrier_semaphore()

    @pl.when(me > 0)
    def _():
        pl.semaphore_signal(barrier, inc=1, device_id={axis: me - 1}, device_id_type=MESH)

    @pl.when(me < n - 1)
    def _():
        pl.semaphore_signal(barrier, inc=1, device_id={axis: me + 1}, device_id_type=MESH)

    @pl.when((me == 0) | (me == n - 1))
    def _():
        pl.semaphore_wait(barrier, 1)

    @pl.when((me > 0) & (me < n - 1))
    def _():
        pl.semaphore_wait(barrier, 2)

    def at(half, c):
        return pl.ds(pl.multiple_of((half * chunks + c) * rows, rows), rows)

    def sum_copy(src, half, c):
        return pltpu.make_async_remote_copy(
            src_ref=src.at[at(half, c)],
            dst_ref=red.at[at(half, c)],
            send_sem=s_red.at[half, c],
            recv_sem=r_red.at[half, c],
            device_id={axis: me - 1 if half == 0 else me + 1},
            device_id_type=MESH,
        )

    def fin_copy(half, c):
        return pltpu.make_async_remote_copy(
            src_ref=held.at[at(half, c)],
            dst_ref=held.at[at(half, c)],
            send_sem=s_fin.at[half, c],
            recv_sem=r_fin.at[half, c],
            device_id={axis: me + 1 if half == 0 else me - 1},
            device_id_type=MESH,
        )

    steps = chunks + 2 * lag * (n - 1)

    def step(s, carry):
        for half in (0, 1):
            hop = (n - 1 - me) if half == 0 else me
            c = s - lag * hop
            ok = (c >= 0) & (c < chunks)

            @pl.when(ok & (hop == 0))
            def _():
                sum_copy(x_ref, half, c).start()

            @pl.when(ok & (hop > 0) & (hop < n - 1))
            def _():
                sum_copy(x_ref, half, c).wait_recv()
                red[at(half, c)] = red[at(half, c)] + x_ref[at(half, c)]
                sum_copy(red, half, c).start()

            @pl.when(ok & (hop == n - 1))
            def _():
                sum_copy(x_ref, half, c).wait_recv()
                held[at(half, c)] = red[at(half, c)] + x_ref[at(half, c)]
                fin_copy(half, c).start()
                finish(at(half, c))

        for half in (0, 1):
            back = me if half == 0 else (n - 1 - me)
            c = s - lag * (n - 1) - lag * back
            ok = (c >= 0) & (c < chunks)

            @pl.when(ok & (back > 0))
            def _():
                fin_copy(half, c).wait_recv()

            @pl.when(ok & (back > 0) & (back < n - 1))
            def _():
                fin_copy(half, c).start()

            @pl.when(ok & (back > 0))
            def _():
                finish(at(half, c))

        if job is not None:
            lax.fori_loop(*job_range(s, steps), job, 0)
        return carry

    lax.fori_loop(0, steps, step, 0)

    def drain(c, carry):
        for half in (0, 1):
            hop = (n - 1 - me) if half == 0 else me

            @pl.when(hop < n - 1)
            def _():
                sum_copy(x_ref, half, c).wait_send()

            @pl.when(hop > 0)
            def _():
                fin_copy(half, c).wait_send()

        return carry

    lax.fori_loop(0, chunks, drain, 0)


def line_kernel(axis, n, chunks, lag, x_ref, o_ref, red, *sems):
    line_steps(axis, n, chunks, lag, x_ref, o_ref, red, sems, lambda at: None, None, None)


def line_low_kernel(axis, n, chunks, lag, x_ref, base_ref, o_ref, red, held, *sems):
    def finish(at):
        o_ref[at] = (base_ref[at] + held[at]).astype(o_ref.dtype)

    line_steps(axis, n, chunks, lag, x_ref, held, red, sems, finish, None, None)


def chunk_count(rows, most, tile):
    chunks = most
    while rows % (2 * chunks * tile):
        chunks -= 1
    return chunks


def line_params(cid):
    return pltpu.CompilerParams(
        collective_id=cid, has_side_effects=True, vmem_limit_bytes=56 << 20
    )


def line_sum(x, axis, n, cid, base=None):
    low = base is not None
    chunks = chunk_count(x.shape[0], 32, 16 if low else 8)
    held = [pltpu.VMEM(x.shape, x.dtype)] if low else []
    operands = (x, base) if low else (x,)
    return pl.pallas_call(
        functools.partial(line_low_kernel if low else line_kernel, axis, n, chunks, 2),
        out_shape=jax.ShapeDtypeStruct(x.shape, jnp.bfloat16 if low else x.dtype),
        in_specs=[pl.BlockSpec(memory_space=pltpu.VMEM)] * len(operands),
        out_specs=pl.BlockSpec(memory_space=pltpu.VMEM),
        scratch_shapes=[pltpu.VMEM(x.shape, x.dtype)]
        + held
        + [pltpu.SemaphoreType.DMA((2, chunks))] * 4,
        compiler_params=line_params(cid),
        name="line_sum",
    )(*operands)


def mid_kernel(
    axis,
    n,
    chunks,
    lag,
    x_ref,
    mid_hbm,
    act_hbm,
    gate_hbm,
    up_hbm,
    cot_hbm,
    down_hbm,
    o_ref,
    grad_gate_ref,
    grad_up_ref,
    grad_down_ref,
    one_ref,
    two_ref,
    red,
    mid_ref,
    act_ref,
    gate_ref,
    up_ref,
    cot_ref,
    down_ref,
    wide_tile,
    row_tile,
    load_sem,
    wide_sem,
    row_sem,
    *sems,
):
    rows, width = cot_ref.shape
    units = act_ref.shape[1]
    tile = wide_tile.shape[0]
    wide_count = width // tile
    by_units = units % 128 == 0 and units >= tile
    tall_count = -(-units // tile) if by_units else wide_count
    row_blocks = rows // tile
    loads = [
        pltpu.make_async_copy(src, dst, load_sem.at[i])
        for i, (src, dst) in enumerate(
            (
                (mid_hbm, mid_ref),
                (gate_hbm, gate_ref),
                (up_hbm, up_ref),
                (act_hbm, act_ref),
                (cot_hbm, cot_ref),
                (down_hbm, down_ref),
            )
        )
    ]
    for load in loads:
        load.start()

    def block(t):
        return pl.ds(pl.multiple_of(t * tile, tile), tile)

    def wide_copy(dst, t):
        return pltpu.make_async_copy(wide_tile, dst.at[block(t)], wide_sem.at[0])

    def tall_at(t):
        return pl.ds(pl.multiple_of(jnp.minimum(t * tile, units - tile), 128), tile)

    def tall_copy(t):
        if by_units:
            return pltpu.make_async_copy(
                row_tile.at[0:tile], grad_down_ref.at[tall_at(t)], row_sem.at[0]
            )
        return pltpu.make_async_copy(
            row_tile.at[0:units, 0:tile], grad_down_ref.at[:, block(t)], row_sem.at[0]
        )

    def out_copy(dst, t):
        return pltpu.make_async_copy(row_tile.at[0:tile], dst.at[block(t)], row_sem.at[0])

    half_blocks = row_blocks // 2
    tall_from = 2 * wide_count
    out_from = tall_from + tall_count
    job_count = out_from + row_blocks

    def job(j, carry):
        @pl.when(j == 0)
        def _():
            for load in loads:
                load.wait()

        for src, dst, start, before in (
            (gate_ref, grad_gate_ref, 0, None),
            (up_ref, grad_up_ref, wide_count, grad_gate_ref),
        ):
            t = j - start

            @pl.when((t >= 0) & (t < wide_count))
            def _():
                value = left_dot(mid_ref[:, block(t)], src[...])

                @pl.when(t > 0)
                def _():
                    wide_copy(dst, t - 1).wait()

                if before is not None:

                    @pl.when(t == 0)
                    def _():
                        wide_copy(before, wide_count - 1).wait()

                wide_tile[...] = value
                wide_copy(dst, t).start()

        @pl.when((j >= tall_from) & (j < out_from))
        def _():
            t = j - tall_from

            @pl.when(t > 0)
            def _():
                tall_copy(t - 1).wait()

            if by_units:
                row_tile[...] = left_dot(act_ref[:, tall_at(t)], cot_ref[...])
            else:
                row_tile[0:units, 0:tile] = left_dot(act_ref[...], cot_ref[:, block(t)])
            tall_copy(t).start()

        for side, dst in enumerate((one_ref, two_ref)):
            t = j - out_from - side * half_blocks

            @pl.when((t >= 0) & (t < half_blocks))
            def _():
                @pl.when(t > 0)
                def _():
                    out_copy(dst, t - 1).wait()

                @pl.when(t == 0)
                def _():
                    if side == 0:
                        tall_copy(tall_count - 1).wait()
                    else:
                        out_copy(one_ref, half_blocks - 1).wait()

                row_tile[0:tile, :] = jnp.dot(
                    act_ref[block(t + side * half_blocks), :],
                    down_ref[...],
                    preferred_element_type=jnp.float32,
                )
                out_copy(dst, t).start()

        return carry

    def bounds(s, steps):
        late = steps - 4
        return tuple(jnp.clip(at - 2, 0, late) * job_count // late for at in (s, s + 1))

    line_steps(axis, n, chunks, lag, x_ref, o_ref, red, sems, lambda at: None, job, bounds)
    wide_copy(grad_up_ref, wide_count - 1).wait()
    out_copy(two_ref, half_blocks - 1).wait()


def mid_sum(x, mid, act, d_gate, d_up, cot, w_down, axis, n, cid):
    rows, width = x.shape
    units = act.shape[1]
    tile = min(256, rows // 2)
    chunks = chunk_count(rows, 32, 8)
    vmem = pl.BlockSpec(memory_space=pltpu.VMEM)
    anywhere = pl.BlockSpec(memory_space=pl.ANY)
    loaded = (mid, act, d_gate, d_up, cot, w_down)
    tall = tile if units % 128 == 0 and units >= tile else max(tile, units)
    return pl.pallas_call(
        functools.partial(mid_kernel, axis, n, chunks, 2),
        out_shape=(
            jax.ShapeDtypeStruct(x.shape, jnp.float32),
            jax.ShapeDtypeStruct((width, units), jnp.float32),
            jax.ShapeDtypeStruct((width, units), jnp.float32),
            jax.ShapeDtypeStruct((units, width), jnp.float32),
            jax.ShapeDtypeStruct((rows // 2, width), jnp.float32),
            jax.ShapeDtypeStruct((rows // 2, width), jnp.float32),
        ),
        in_specs=[vmem] + [anywhere] * 6,
        out_specs=(vmem,) + (anywhere,) * 5,
        scratch_shapes=[pltpu.VMEM(x.shape, jnp.float32)]
        + [pltpu.VMEM(item.shape, item.dtype) for item in loaded]
        + [pltpu.VMEM((tile, units), jnp.float32), pltpu.VMEM((tall, width), jnp.float32)]
        + [pltpu.SemaphoreType.DMA((len(loaded),))]
        + [pltpu.SemaphoreType.DMA((1,))] * 2
        + [pltpu.SemaphoreType.DMA((2, chunks))] * 4,
        compiler_params=pltpu.CompilerParams(
            collective_id=cid, has_side_effects=True, vmem_limit_bytes=62 << 20
        ),
        name="mid_sum",
    )(x, *loaded)


def attend_kernel(
    axis,
    n,
    chunks,
    lag,
    seq_len,
    block,
    raw_ref,
    k_ref,
    v_ref,
    own_ref,
    all_ref,
    cos_ref,
    sin_ref,
    out_ref,
    base_ref,
    o_ref,
    q_ref,
    mixed_ref,
    norm_ref,
    part,
    red,
    *sems,
):
    rows, head_dim = k_ref.shape
    heads = raw_ref.shape[1] // head_dim
    half_dim = head_dim // 2
    blocks = seq_len // block
    scale = head_dim ** (-0.5)
    pairs = rows // (2 * block)
    turns = heads + 1
    pair_jobs = 2 * turns

    def job(j, carry):
        pair = lax.div(j, pair_jobs)
        side = lax.div(lax.rem(j, pair_jobs), turns)
        head = lax.rem(j, turns)
        row_block = side * pairs + pair
        seq = lax.div(row_block, blocks)
        block_at = lax.rem(row_block, blocks)
        own = pl.ds(pl.multiple_of(row_block * block, block), block)
        cols = pl.ds(pl.multiple_of(head * head_dim, head_dim), head_dim)
        low_cols = pl.ds(pl.multiple_of(head * head_dim, half_dim), half_dim)
        high_cols = pl.ds(pl.multiple_of(head * head_dim + half_dim, half_dim), half_dim)

        def run(reach):
            keys = pl.ds(pl.multiple_of(seq * seq_len, seq_len), reach)
            first = raw_ref[own, low_cols]
            second = raw_ref[own, high_cols]
            cos_tab = cos_ref[own, :]
            sin_tab = sin_ref[own, :]
            q_ref[own, low_cols] = (first * cos_tab - second * sin_tab).astype(q_ref.dtype)
            q_ref[own, high_cols] = (second * cos_tab + first * sin_tab).astype(q_ref.dtype)
            scores = right_dot(q_ref[own, cols], k_ref[keys, :]) * scale
            q_pos = block_at * block + lax.broadcasted_iota(jnp.int32, scores.shape, 0)
            k_pos = lax.broadcasted_iota(jnp.int32, scores.shape, 1)
            same = own_ref[own, :] == all_ref[:, keys]
            scores = jnp.where((k_pos <= q_pos) | same, scores, masked_score)
            row_max = jnp.max(scores, axis=1, keepdims=True)
            exp_terms = jnp.exp(scores - row_max)
            row_sum = jnp.sum(exp_terms, axis=1, keepdims=True)
            probs = (exp_terms * (1.0 / row_sum)).astype(jnp.bfloat16)
            mixed = jnp.dot(probs, v_ref[keys, :], preferred_element_type=jnp.float32)
            mixed_ref[own, cols] = mixed.astype(mixed_ref.dtype)
            norm_ref[head, own, :] = row_max + jnp.log(row_sum)

        reaches = reach_list(seq_len, block)
        for reach in sorted(set(reaches)):
            first = reaches.index(reach)
            last = first + reaches.count(reach) - 1

            @pl.when((head < heads) & (block_at >= first) & (block_at <= last))
            def _():
                run(reach)

        @pl.when(head == heads)
        def _():
            part[own, :] = jnp.dot(
                mixed_ref[own, :], out_ref[...], preferred_element_type=jnp.float32
            )

        @pl.when((head == heads) & (lax.axis_index(axis) == 0))
        def _():
            part[own, :] += base_ref[own, :].astype(jnp.float32)

        return carry

    lax.fori_loop(0, pair_jobs, job, 0)
    pair_steps = chunks // pairs

    def job_range(s, steps):
        return tuple(
            jnp.minimum((pair_steps + at) * pair_jobs // pair_steps, pairs * pair_jobs)
            for at in (s, s + 1)
        )

    line_steps(axis, n, chunks, lag, part, o_ref, red, sems, lambda at: None, job, job_range)


def reach_list(seq_len, block):
    step = max(256, block)
    ends = [(b + 1) * block + PIECE for b in range(seq_len // block)]
    return [min(seq_len, -(-end // step) * step) for end in ends]


def attend(raw, k, v, own_ids, all_ids, cos_tab, sin_tab, out_proj, base, axis, n, seq_len, cid):
    rows, width = base.shape
    block = min(128, seq_len)
    chunks = chunk_count(rows, 32, 8)
    vmem = pl.BlockSpec(memory_space=pltpu.VMEM)
    return pl.pallas_call(
        functools.partial(attend_kernel, axis, n, chunks, 2, seq_len, block),
        out_shape=(
            jax.ShapeDtypeStruct((rows, width), jnp.float32),
            jax.ShapeDtypeStruct(raw.shape, jnp.bfloat16),
            jax.ShapeDtypeStruct(raw.shape, jnp.bfloat16),
            jax.ShapeDtypeStruct((raw.shape[1] // k.shape[1], rows, 1), jnp.float32),
        ),
        in_specs=[vmem] * 9,
        out_specs=(vmem,) * 4,
        scratch_shapes=[pltpu.VMEM((rows, width), jnp.float32)] * 2
        + [pltpu.SemaphoreType.DMA((2, chunks))] * 4,
        compiler_params=pltpu.CompilerParams(
            collective_id=cid, has_side_effects=True, vmem_limit_bytes=60 << 20
        ),
        name="attend",
    )(raw, k, v, own_ids, all_ids, cos_tab, sin_tab, out_proj, base)


def attend_back_kernel(
    axis,
    n,
    chunks,
    lag,
    seq_len,
    block,
    x_ref,
    base_ref,
    q_ref,
    dm_ref,
    k_ref,
    v_ref,
    norm_ref,
    own_ref,
    all_ref,
    cos_ref,
    sin_ref,
    up_ref,
    o_ref,
    dq_ref,
    sums_ref,
    red,
    held,
    *sems,
):
    rows, head_dim = k_ref.shape
    heads = q_ref.shape[1] // head_dim
    half_dim = head_dim // 2
    blocks = seq_len // block
    scale = head_dim ** (-0.5)
    rank = up_ref.shape[0]
    key_cols = slice(rank, rank + head_dim)
    val_cols = slice(rank + head_dim, rank + 2 * head_dim)
    sums_ref[:, rank:] = jnp.zeros((rows, 2 * head_dim), jnp.float32)

    def finish(at):
        o_ref[at] = (base_ref[at] + held[at]).astype(o_ref.dtype)

    def job(j, carry):
        head = lax.rem(j, heads)
        row_block = lax.div(j, heads)
        seq = lax.div(row_block, blocks)
        block_at = lax.rem(row_block, blocks)
        own = pl.ds(pl.multiple_of(row_block * block, block), block)
        cols = pl.ds(pl.multiple_of(head * head_dim, head_dim), head_dim)
        low_cols = pl.ds(pl.multiple_of(head * head_dim, half_dim), half_dim)
        high_cols = pl.ds(pl.multiple_of(head * head_dim + half_dim, half_dim), half_dim)

        def run(reach):
            keys = pl.ds(pl.multiple_of(seq * seq_len, seq_len), reach)
            q = q_ref[own, cols]
            dm = dm_ref[own, cols]
            k = k_ref[keys, :]
            v = v_ref[keys, :]
            scores = right_dot(q, k) * scale
            q_pos = block_at * block + lax.broadcasted_iota(jnp.int32, scores.shape, 0)
            k_pos = lax.broadcasted_iota(jnp.int32, scores.shape, 1)
            same = own_ref[own, :] == all_ref[:, keys]
            probs = jnp.where(
                (k_pos <= q_pos) | same, jnp.exp(scores - norm_ref[head, own, :]), 0.0
            )
            d_probs = right_dot(dm, v)
            row_sum = jnp.sum(probs * d_probs, axis=1, keepdims=True)
            d_scores = (probs * (d_probs - row_sum)).astype(jnp.bfloat16)
            sums_ref[keys, key_cols] += left_dot(d_scores, q) * scale
            sums_ref[keys, val_cols] += left_dot(probs.astype(jnp.bfloat16), dm)
            dq = jnp.dot(d_scores, k, preferred_element_type=jnp.float32) * scale
            first = dq[:, :half_dim]
            second = dq[:, half_dim:]
            cos_tab = cos_ref[own, :]
            sin_tab = sin_ref[own, :]
            dq_ref[own, low_cols] = (first * cos_tab + second * sin_tab).astype(dq_ref.dtype)
            dq_ref[own, high_cols] = (second * cos_tab - first * sin_tab).astype(dq_ref.dtype)

        reaches = reach_list(seq_len, block)
        for reach in sorted(set(reaches)):
            first = reaches.index(reach)
            last = first + reaches.count(reach) - 1

            @pl.when((block_at >= first) & (block_at <= last))
            def _():
                run(reach)

        @pl.when(head == heads - 1)
        def _():
            sums_ref[own, 0:rank] = right_dot(dq_ref[own, :], up_ref[...])

        return carry

    job_count = heads * (rows // block)

    def job_range(s, steps):
        return s * job_count // steps, (s + 1) * job_count // steps

    line_steps(axis, n, chunks, lag, x_ref, held, red, sems, finish, job, job_range)


def attend_back(
    x, base, q, dm, k, v, norm, own_ids, all_ids, cos_tab, sin_tab, q_up, axis, n, seq_len, cid
):
    chunks = chunk_count(x.shape[0], 32, 16)
    block = min(256, seq_len)
    vmem = pl.BlockSpec(memory_space=pltpu.VMEM)
    return pl.pallas_call(
        functools.partial(attend_back_kernel, axis, n, chunks, 2, seq_len, block),
        out_shape=(
            jax.ShapeDtypeStruct(x.shape, jnp.bfloat16),
            jax.ShapeDtypeStruct(q.shape, jnp.bfloat16),
            jax.ShapeDtypeStruct((k.shape[0], q_up.shape[0] + 2 * k.shape[1]), jnp.float32),
        ),
        in_specs=[vmem] * 12,
        out_specs=(vmem, vmem, vmem),
        scratch_shapes=[pltpu.VMEM(x.shape, x.dtype)] * 2
        + [pltpu.SemaphoreType.DMA((2, chunks))] * 4,
        compiler_params=line_params(cid),
        name="attend_back",
    )(x, base, q, dm, k, v, norm, own_ids, all_ids, cos_tab, sin_tab, q_up)


def shards(
    block_input,
    image_starts,
    norm_gain,
    q_down,
    q_gain,
    q_up,
    k_proj,
    v_proj,
    out_proj,
    mlp_gain,
    w_gate,
    w_up,
    w_down,
    d_output,
):
    row_count, model_width = block_input.shape
    dp_count = lax.axis_size("dp")
    tp_count = lax.axis_size("tensor")
    tp_index = lax.axis_index("tensor")

    def own_part(values, axis):
        split = values.shape[axis] // (dp_count * tp_count)
        shape = values.shape[:axis] + (dp_count, tp_count, split) + values.shape[axis + 1 :]
        picked = lax.dynamic_index_in_dim(values.reshape(shape), tp_index, axis + 1, keepdims=False)
        return picked

    seq_count = image_starts.shape[0]
    seq_len = row_count // seq_count
    head_dim = k_proj.shape[1]
    positions = jnp.arange(seq_len, dtype=jnp.float32)
    inv_freq = 10000.0 ** (-(jnp.arange(head_dim // 2, dtype=jnp.float32) * 2.0) / head_dim)
    angles = positions[:, None] * inv_freq[None, :]
    cos_all = jnp.tile(jnp.cos(angles), (seq_count, 1))
    sin_all = jnp.tile(jnp.sin(angles), (seq_count, 1))
    pos_int = jnp.arange(seq_len, dtype=jnp.int32)
    inside = (pos_int[None, :, None] >= image_starts[:, None, :]) & (
        pos_int[None, :, None] < image_starts[:, None, :] + PIECE
    )
    labels = jnp.arange(1, image_starts.shape[1] + 1, dtype=jnp.int32)
    piece_ids = jnp.sum(jnp.where(inside, labels, 0), axis=2)

    own_ids = jnp.where(piece_ids > 0, piece_ids, -1).reshape(row_count, 1)
    all_ids = piece_ids.reshape(1, row_count)
    input_f32 = block_input.astype(jnp.float32)
    gain_attn = norm_gain.astype(jnp.float32)
    gain_query = q_gain.astype(jnp.float32)
    gain_mlp = mlp_gain.astype(jnp.float32)
    cotan_f32 = d_output.astype(jnp.float32)
    normed_one, scale_one = normalize(input_f32)
    normed_in = (normed_one * gain_attn).astype(jnp.bfloat16)
    q_latent = jnp.dot(normed_in, q_down, preferred_element_type=jnp.float32)
    q_latent = lax.optimization_barrier(q_latent)
    q_unit, q_scale = normalize(q_latent)
    q_normed = (q_unit * gain_query).astype(jnp.bfloat16)
    q_raw = jnp.dot(q_normed, q_up, preferred_element_type=jnp.float32)
    key_rows = rotate(
        jnp.dot(normed_in, k_proj, preferred_element_type=jnp.float32), cos_all, sin_all
    ).astype(jnp.bfloat16)
    val_rows = jnp.dot(normed_in, v_proj, preferred_element_type=jnp.float32).astype(jnp.bfloat16)
    hidden_in, queries, mixed_heads, log_norm = attend(
        q_raw,
        key_rows,
        val_rows,
        own_ids,
        all_ids,
        cos_all,
        sin_all,
        out_proj,
        block_input,
        "tensor",
        tp_count,
        seq_len,
        5,
    )
    normed_two, scale_two = normalize(hidden_in)
    normed_mid = (normed_two * gain_mlp).astype(jnp.bfloat16)
    gate_pre = jnp.dot(normed_mid, w_gate, preferred_element_type=jnp.float32)
    up_pre = jnp.dot(normed_mid, w_up, preferred_element_type=jnp.float32)
    gate_sig = jax.nn.sigmoid(gate_pre)
    hidden_act = (gate_pre * gate_sig * up_pre).astype(jnp.bfloat16)
    d_act = right_dot(d_output, w_down)
    d_gate = (d_act * up_pre * gate_sig * (1.0 + gate_pre * (1.0 - gate_sig))).astype(jnp.bfloat16)
    d_up = (d_act * gate_pre * gate_sig).astype(jnp.bfloat16)
    d_mid_part = right_dot(d_gate, w_gate) + right_dot(d_up, w_up)
    d_mid, grad_gate, grad_up, grad_down, out_part_one, out_part_two = mid_sum(
        d_mid_part,
        normed_mid,
        hidden_act,
        d_gate,
        d_up,
        d_output,
        w_down,
        "tensor",
        tp_count,
        1,
    )
    grad_gate = lax.psum_scatter(grad_gate, "dp", scatter_dimension=0, tiled=True)
    grad_up = lax.psum_scatter(grad_up, "dp", scatter_dimension=0, tiled=True)
    grad_down = lax.psum_scatter(grad_down, "dp", scatter_dimension=1, tiled=True)
    grad_gain_mlp = jnp.sum(d_mid * normed_two, axis=0)
    d_hidden = cotan_f32 + norm_back(d_mid * gain_mlp, normed_two, scale_two)
    d_hidden_low = d_hidden.astype(jnp.bfloat16)
    grad_out = left_dot(mixed_heads, d_hidden_low)
    d_mixed = right_dot(d_hidden_low, out_proj).astype(jnp.bfloat16)
    half_rows = row_count // 2
    out_part_one, grad_out = lax.optimization_barrier((out_part_one, grad_out))
    grad_out = lax.psum_scatter(grad_out, "dp", scatter_dimension=1, tiled=True)
    output_one, d_q_raw, query_key_val = attend_back(
        out_part_one,
        hidden_in[:half_rows],
        queries,
        d_mixed,
        key_rows,
        val_rows,
        log_norm,
        own_ids,
        all_ids,
        cos_all,
        sin_all,
        q_up,
        "tensor",
        tp_count,
        seq_len,
        3,
    )
    grad_query_up = left_dot(q_normed, d_q_raw)
    query_key_val, grad_query_up = lax.optimization_barrier((query_key_val, grad_query_up))
    grad_query_up = lax.psum_scatter(grad_query_up, "dp", scatter_dimension=0, tiled=True)
    query_key_val = line_sum(query_key_val, "tensor", tp_count, 2)
    d_q_normed = query_key_val[:, : q_gain.shape[0]]
    key_val_full = query_key_val[:, q_gain.shape[0] :]
    d_key_low = unrotate(key_val_full[:, :head_dim], cos_all, sin_all).astype(jnp.bfloat16)
    d_val_low = key_val_full[:, head_dim:].astype(jnp.bfloat16)
    grad_gain_query = jnp.sum(d_q_normed * q_unit, axis=0)
    d_latent = norm_back(d_q_normed * gain_query, q_unit, q_scale).astype(jnp.bfloat16)
    d_normed_in = (
        right_dot(d_latent, q_down) + right_dot(d_key_low, k_proj) + right_dot(d_val_low, v_proj)
    )
    grad_gain_attn = jnp.sum(d_normed_in * normed_one, axis=0)
    grad_input = (d_hidden + norm_back(d_normed_in * gain_attn, normed_one, scale_one)).astype(
        jnp.bfloat16
    )
    own_width = model_width // (dp_count * tp_count)
    own_at = jnp.arange(model_width // tp_count)
    own_at = (own_at // own_width * tp_count + tp_index) * own_width + own_at % own_width
    pick = (jnp.arange(model_width)[:, None] == own_at[None, :]).astype(jnp.bfloat16)
    own_in = jnp.dot(normed_in, pick, preferred_element_type=jnp.float32).astype(jnp.bfloat16)
    own_grads = left_dot(own_in, jnp.concatenate([d_latent, d_key_low, d_val_low], axis=1))
    own_rows = own_grads.shape[0]
    gain_one = own_part(grad_gain_attn, 0).reshape(own_rows, 1)
    gain_two = own_part(grad_gain_mlp, 0).reshape(own_rows, 1)
    gain_mid = own_part(grad_gain_query, 0)
    own_mid = gain_mid.shape[1]
    gain_mid = jnp.pad(gain_mid, ((0, 0), (0, own_rows // dp_count - own_mid))).reshape(own_rows, 1)
    gain_cols = jnp.concatenate([gain_one, gain_two, gain_mid], axis=1)
    own_grads = jnp.concatenate([own_grads, jnp.pad(gain_cols, ((0, 0), (0, 125)))], axis=1)
    own_sum = lax.psum_scatter(own_grads, "dp", scatter_dimension=0, tiled=True)
    output_two = line_sum(out_part_two, "tensor", tp_count, 4, base=hidden_in[half_rows:])
    block_output = jnp.concatenate([output_one, output_two], axis=0)
    rank = q_down.shape[1]
    grad_qd = own_sum[:, :rank]
    grad_key = own_sum[:, rank : rank + head_dim]
    grad_val = own_sum[:, rank + head_dim : rank + 2 * head_dim]
    gain_at = rank + 2 * head_dim
    grad_g1 = own_sum[:, gain_at]
    grad_g2 = own_sum[:, gain_at + 1]
    grad_gq = own_sum[:own_mid, gain_at + 2]
    return (
        block_output,
        grad_input,
        grad_g1,
        grad_qd,
        grad_gq,
        grad_query_up,
        grad_key,
        grad_val,
        grad_out,
        grad_g2,
        grad_gate,
        grad_up,
        grad_down,
    )


def solution(mesh):
    placed = (
        P("dp", None),
        P("dp", None),
        P(),
        P(),
        P(),
        P(None, "tensor"),
        P(),
        P(),
        P("tensor", None),
        P(),
        P(None, "tensor"),
        P(None, "tensor"),
        P("tensor", None),
        P("dp", None),
    )

    return jax.shard_map(
        shards,
        mesh=mesh,
        in_specs=placed,
        out_specs=(
            P("dp", None),
            P("dp", None),
            P(("dp", "tensor")),
            P(("dp", "tensor"), None),
            P(("dp", "tensor")),
            P("dp", "tensor"),
            P(("dp", "tensor"), None),
            P(("dp", "tensor"), None),
            P("tensor", "dp"),
            P(("dp", "tensor")),
            P("dp", "tensor"),
            P("dp", "tensor"),
            P("tensor", "dp"),
        ),
        check_vma=False,
    )
```

```python
import functools

import jax
import jax.numpy as jnp
from jax import lax
from jax.experimental import pallas as pl
from jax.experimental.pallas import tpu as pltpu
from jax.sharding import PartitionSpec as P


MESH = pl.DeviceIdType.MESH

PIECE = 256


epsilon = 1e-06
masked_score = -1e30


def normalize(values):
    scale_rows = lax.rsqrt(jnp.mean(values * values, axis=-1, keepdims=True) + epsilon)
    return (values * scale_rows, scale_rows)


def norm_back(grad_normed, normed, scale_rows):
    return scale_rows * (
        grad_normed - normed * jnp.mean(grad_normed * normed, axis=-1, keepdims=True)
    )


def left_dot(left, right):
    return lax.dot_general(
        left, right, (((0,), (0,)), ((), ())), preferred_element_type=jnp.float32
    )


def right_dot(left, right):
    return lax.dot_general(
        left, right, (((1,), (1,)), ((), ())), preferred_element_type=jnp.float32
    )


def rotate(values, cos_tab, sin_tab):
    half = values.shape[-1] // 2
    first_half = values[..., :half]
    second_half = values[..., half:]
    return jnp.concatenate(
        [
            first_half * cos_tab - second_half * sin_tab,
            second_half * cos_tab + first_half * sin_tab,
        ],
        axis=-1,
    )


def line_steps(axis, n, chunks, lag, x_ref, held, red, sems, finish, after_step):
    me = lax.axis_index(axis)
    rows = x_ref.shape[0] // (2 * chunks)
    s_red, r_red, s_fin, r_fin = sems
    barrier = pltpu.get_barrier_semaphore()

    @pl.when(me > 0)
    def _():
        pl.semaphore_signal(barrier, inc=1, device_id={axis: me - 1}, device_id_type=MESH)

    @pl.when(me < n - 1)
    def _():
        pl.semaphore_signal(barrier, inc=1, device_id={axis: me + 1}, device_id_type=MESH)

    @pl.when((me == 0) | (me == n - 1))
    def _():
        pl.semaphore_wait(barrier, 1)

    @pl.when((me > 0) & (me < n - 1))
    def _():
        pl.semaphore_wait(barrier, 2)

    def at(half, c):
        return pl.ds(pl.multiple_of((half * chunks + c) * rows, rows), rows)

    def sum_copy(src, half, c):
        return pltpu.make_async_remote_copy(
            src_ref=src.at[at(half, c)],
            dst_ref=red.at[at(half, c)],
            send_sem=s_red.at[half, c],
            recv_sem=r_red.at[half, c],
            device_id={axis: me - 1 if half == 0 else me + 1},
            device_id_type=MESH,
        )

    def fin_copy(half, c):
        return pltpu.make_async_remote_copy(
            src_ref=held.at[at(half, c)],
            dst_ref=held.at[at(half, c)],
            send_sem=s_fin.at[half, c],
            recv_sem=r_fin.at[half, c],
            device_id={axis: me + 1 if half == 0 else me - 1},
            device_id_type=MESH,
        )

    steps = chunks + 2 * lag * (n - 1)

    def step(s, carry):
        for half in (0, 1):
            hop = (n - 1 - me) if half == 0 else me
            c = s - lag * hop
            ok = (c >= 0) & (c < chunks)

            @pl.when(ok & (hop == 0))
            def _():
                sum_copy(x_ref, half, c).start()

            @pl.when(ok & (hop > 0) & (hop < n - 1))
            def _():
                sum_copy(x_ref, half, c).wait_recv()
                red[at(half, c)] = red[at(half, c)] + x_ref[at(half, c)]
                sum_copy(red, half, c).start()

            @pl.when(ok & (hop == n - 1))
            def _():
                sum_copy(x_ref, half, c).wait_recv()
                held[at(half, c)] = red[at(half, c)] + x_ref[at(half, c)]
                fin_copy(half, c).start()
                finish(at(half, c))

        for half in (0, 1):
            back = me if half == 0 else (n - 1 - me)
            c = s - lag * (n - 1) - lag * back
            ok = (c >= 0) & (c < chunks)

            @pl.when(ok & (back > 0))
            def _():
                fin_copy(half, c).wait_recv()

            @pl.when(ok & (back > 0) & (back < n - 1))
            def _():
                fin_copy(half, c).start()

            @pl.when(ok & (back > 0))
            def _():
                finish(at(half, c))

        if after_step is not None:
            after_step(s, steps)
        return carry

    lax.fori_loop(0, steps, step, 0)

    def drain(c, carry):
        for half in (0, 1):
            hop = (n - 1 - me) if half == 0 else me

            @pl.when(hop < n - 1)
            def _():
                sum_copy(x_ref, half, c).wait_send()

            @pl.when(hop > 0)
            def _():
                fin_copy(half, c).wait_send()

        return carry

    lax.fori_loop(0, chunks, drain, 0)


def line_kernel(axis, n, chunks, lag, x_ref, o_ref, red, *sems):
    line_steps(axis, n, chunks, lag, x_ref, o_ref, red, sems, lambda at: None, None)


def line_low_kernel(axis, n, chunks, lag, x_ref, base_ref, o_ref, red, held, *sems):
    def finish(at):
        o_ref[at] = (base_ref[at] + held[at]).astype(o_ref.dtype)

    line_steps(axis, n, chunks, lag, x_ref, held, red, sems, finish, None)


def chunk_count(rows, most, tile):
    chunks = most
    while rows % (2 * chunks * tile):
        chunks -= 1
    return chunks


def line_params(cid):
    return pltpu.CompilerParams(
        collective_id=cid, has_side_effects=True, vmem_limit_bytes=56 << 20
    )


def line_sum(x, axis, n, cid, base=None):
    low = base is not None
    chunks = chunk_count(x.shape[0], 32, 16 if low else 8)
    held = [pltpu.VMEM(x.shape, x.dtype)] if low else []
    operands = (x, base) if low else (x,)
    return pl.pallas_call(
        functools.partial(line_low_kernel if low else line_kernel, axis, n, chunks, 2),
        out_shape=jax.ShapeDtypeStruct(x.shape, jnp.bfloat16 if low else x.dtype),
        in_specs=[pl.BlockSpec(memory_space=pltpu.VMEM)] * len(operands),
        out_specs=pl.BlockSpec(memory_space=pltpu.VMEM),
        scratch_shapes=[pltpu.VMEM(x.shape, x.dtype)]
        + held
        + [pltpu.SemaphoreType.DMA((2, chunks))] * 4,
        compiler_params=line_params(cid),
        name="line_sum",
    )(*operands)


def mid_kernel(
    axis,
    n,
    chunks,
    lag,
    x_ref,
    mid_hbm,
    act_hbm,
    gate_hbm,
    up_hbm,
    cot_hbm,
    down_hbm,
    o_ref,
    grad_wide_ref,
    grad_down_ref,
    one_ref,
    two_ref,
    red,
    mid_ref,
    act_ref,
    gate_ref,
    up_ref,
    cot_ref,
    down_ref,
    wide_tile,
    row_tile,
    load_sem,
    wide_sem,
    row_sem,
    *sems,
):
    rows, width = cot_ref.shape
    units = act_ref.shape[1]
    wide = wide_tile.shape[0]
    wide_count = width // wide
    tile = min(256, rows // 2)
    by_units = units % 128 == 0 and units >= tile
    tall_count = -(-units // tile) if by_units else width // tile
    row_blocks = rows // tile
    loads = [
        pltpu.make_async_copy(src, dst, load_sem.at[i])
        for i, (src, dst) in enumerate(
            (
                (mid_hbm, mid_ref),
                (gate_hbm, gate_ref),
                (up_hbm, up_ref),
                (act_hbm, act_ref),
                (cot_hbm, cot_ref),
                (down_hbm, down_ref),
            )
        )
    ]
    for load in loads:
        load.start()

    def block(t):
        return pl.ds(pl.multiple_of(t * tile, tile), tile)

    def wide_copy(which, t):
        to = pl.ds(pl.multiple_of((2 * t + which) * wide, wide), wide)
        return pltpu.make_async_copy(wide_tile, grad_wide_ref.at[to], wide_sem.at[0])

    def tall_at(t):
        return pl.ds(pl.multiple_of(jnp.minimum(t * tile, units - tile), 128), tile)

    def tall_copy(t):
        if by_units:
            return pltpu.make_async_copy(
                row_tile.at[0:tile], grad_down_ref.at[tall_at(t)], row_sem.at[0]
            )
        return pltpu.make_async_copy(
            row_tile.at[0:units, 0:tile], grad_down_ref.at[:, block(t)], row_sem.at[0]
        )

    def out_copy(dst, t):
        return pltpu.make_async_copy(row_tile.at[0:tile], dst.at[block(t)], row_sem.at[0])

    half_blocks = row_blocks // 2
    tall_from = 2 * wide_count
    out_from = tall_from + tall_count
    job_count = out_from + row_blocks

    def job(j, carry):
        @pl.when(j == 0)
        def _():
            for load in loads:
                load.wait()

        for which, src in enumerate((gate_ref, up_ref)):
            t = lax.div(j, 2)

            @pl.when((j < tall_from) & (lax.rem(j, 2) == which))
            def _():
                cols = pl.ds(pl.multiple_of(t * wide, wide), wide)
                value = left_dot(mid_ref[:, cols], src[...])
                if which:
                    wide_copy(0, t).wait()
                else:

                    @pl.when(t > 0)
                    def _():
                        wide_copy(1, t - 1).wait()

                wide_tile[...] = value
                wide_copy(which, t).start()

        @pl.when((j >= tall_from) & (j < out_from))
        def _():
            t = j - tall_from

            @pl.when(t > 0)
            def _():
                tall_copy(t - 1).wait()

            if by_units:
                row_tile[...] = left_dot(act_ref[:, tall_at(t)], cot_ref[...])
            else:
                row_tile[0:units, 0:tile] = left_dot(act_ref[...], cot_ref[:, block(t)])
            tall_copy(t).start()

        for side, dst in enumerate((one_ref, two_ref)):
            t = j - out_from - side * half_blocks

            @pl.when((t >= 0) & (t < half_blocks))
            def _():
                @pl.when(t > 0)
                def _():
                    out_copy(dst, t - 1).wait()

                @pl.when(t == 0)
                def _():
                    if side == 0:
                        tall_copy(tall_count - 1).wait()
                    else:
                        out_copy(one_ref, half_blocks - 1).wait()

                row_tile[0:tile, :] = jnp.dot(
                    act_ref[block(t + side * half_blocks), :],
                    down_ref[...],
                    preferred_element_type=jnp.float32,
                )
                out_copy(dst, t).start()

        return carry

    def after_step(s, steps):
        late = steps - 4
        bounds = tuple(jnp.clip(at - 2, 0, late) * job_count // late for at in (s, s + 1))
        lax.fori_loop(*bounds, job, 0)

    line_steps(axis, n, chunks, lag, x_ref, o_ref, red, sems, lambda at: None, after_step)
    wide_copy(1, wide_count - 1).wait()
    out_copy(two_ref, half_blocks - 1).wait()


def mid_sum(x, mid, act, d_gate, d_up, cot, w_down, axis, n, parts, cid):
    rows, width = x.shape
    units = act.shape[1]
    tile = min(256, rows // 2)
    chunks = chunk_count(rows, 32, 8)
    vmem = pl.BlockSpec(memory_space=pltpu.VMEM)
    anywhere = pl.BlockSpec(memory_space=pl.ANY)
    loaded = (mid, act, d_gate, d_up, cot, w_down)
    tall = tile if units % 128 == 0 and units >= tile else max(tile, units)
    return pl.pallas_call(
        functools.partial(mid_kernel, axis, n, chunks, 2),
        out_shape=(
            jax.ShapeDtypeStruct(x.shape, jnp.float32),
            jax.ShapeDtypeStruct((2 * width, units), jnp.float32),
            jax.ShapeDtypeStruct((units, width), jnp.float32),
            jax.ShapeDtypeStruct((rows // 2, width), jnp.float32),
            jax.ShapeDtypeStruct((rows // 2, width), jnp.float32),
        ),
        in_specs=[vmem] + [anywhere] * 6,
        out_specs=(vmem,) + (anywhere,) * 4,
        scratch_shapes=[pltpu.VMEM(x.shape, jnp.float32)]
        + [pltpu.VMEM(item.shape, item.dtype) for item in loaded]
        + [pltpu.VMEM((width // parts, units), jnp.float32), pltpu.VMEM((tall, width), jnp.float32)]
        + [pltpu.SemaphoreType.DMA((len(loaded),))]
        + [pltpu.SemaphoreType.DMA((1,))] * 2
        + [pltpu.SemaphoreType.DMA((2, chunks))] * 4,
        compiler_params=pltpu.CompilerParams(
            collective_id=cid, has_side_effects=True, vmem_limit_bytes=62 << 20
        ),
        name="mid_sum",
    )(x, *loaded)


def tail_kernel(
    axis,
    n,
    chunks,
    lag,
    block,
    x_ref,
    scale_one_ref,
    scale_mid_ref,
    cos_ref,
    sin_ref,
    gain_one_ref,
    gain_mid_ref,
    unit_hbm,
    down_hbm,
    key_hbm,
    val_hbm,
    own_hbm,
    input_hbm,
    hidden_hbm,
    grad_hbm,
    own_ref,
    acc_one_ref,
    acc_mid_ref,
    held,
    red,
    unit_ref,
    down_ref,
    key_ref,
    val_ref,
    own_in_ref,
    input_ref,
    hidden_ref,
    grad_ref,
    low_ref,
    load_sem,
    block_sem,
    store_sem,
    *sems,
):
    me = lax.axis_index(axis)
    rows = x_ref.shape[0]
    rank = unit_ref.shape[1]
    head_dim = key_ref.shape[1]
    half_dim = head_dim // 2
    pairs = rows // (2 * block)
    per = chunks // pairs
    loads = [
        pltpu.make_async_copy(src, dst, load_sem.at[i])
        for i, (src, dst) in enumerate(
            (
                (unit_hbm, unit_ref),
                (down_hbm, down_ref),
                (key_hbm, key_ref),
                (val_hbm, val_ref),
                (own_hbm, own_in_ref),
            )
        )
    ]
    for load in loads:
        load.start()
    acc_one_ref[...] = jnp.zeros_like(acc_one_ref)
    acc_mid_ref[...] = jnp.zeros_like(acc_mid_ref)
    own_ref[...] = jnp.zeros_like(own_ref)

    def fold(values):
        return jnp.sum(values.reshape(values.shape[0] // 8, 8, values.shape[1]), axis=0)

    def store(own):
        return pltpu.make_async_copy(grad_ref, grad_hbm.at[own], store_sem.at[0])

    def consume(row_block):
        own = pl.ds(pl.multiple_of(row_block * block, block), block)
        take_input = pltpu.make_async_copy(input_hbm.at[own], input_ref, block_sem.at[0])
        take_hidden = pltpu.make_async_copy(hidden_hbm.at[own], hidden_ref, block_sem.at[1])
        take_input.start()
        take_hidden.start()
        d_bq = held[own, 0:rank]
        unit = unit_ref[own, :]
        acc_mid_ref[...] += fold(d_bq * unit)
        eq = d_bq * gain_mid_ref[...]
        mean_mid = jnp.mean(eq * unit, axis=1, keepdims=True)
        d_latent = (scale_mid_ref[own, :] * (eq - unit * mean_mid)).astype(jnp.bfloat16)
        first = held[own, rank : rank + half_dim]
        second = held[own, rank + half_dim : rank + head_dim]
        cos_tab = cos_ref[own, :]
        sin_tab = sin_ref[own, :]
        low_ref[own, 0:rank] = d_latent
        low_ref[own, rank : rank + half_dim] = (first * cos_tab + second * sin_tab).astype(
            jnp.bfloat16
        )
        low_ref[own, rank + half_dim : rank + head_dim] = (
            second * cos_tab - first * sin_tab
        ).astype(jnp.bfloat16)
        low_ref[own, rank + head_dim :] = held[own, rank + head_dim :].astype(jnp.bfloat16)
        d_in = (
            right_dot(d_latent, down_ref[...])
            + right_dot(low_ref[own, rank : rank + head_dim], key_ref[...])
            + right_dot(low_ref[own, rank + head_dim :], val_ref[...])
        )
        take_input.wait()
        take_hidden.wait()
        scale_one = scale_one_ref[own, :]
        normed = input_ref[...].astype(jnp.float32) * scale_one
        acc_one_ref[...] += fold(d_in * normed)
        e_in = d_in * gain_one_ref[...]
        mean_one = jnp.mean(e_in * normed, axis=1, keepdims=True)
        grad_ref[...] = (hidden_ref[...] + scale_one * (e_in - normed * mean_one)).astype(
            grad_ref.dtype
        )
        store(own).start()
        store(own).wait()

    def after_step(s, steps):
        @pl.when(s == lag)
        def _():
            for load in loads:
                load.wait()

        for half in (0, 1):
            back = me if half == 0 else (n - 1 - me)
            c = s - lag * (n - 1) - lag * back

            @pl.when((c >= 0) & (c < chunks) & (lax.rem(c + 1, per) == 0))
            def _():
                consume(half * pairs + lax.div(c, per))

    line_steps(axis, n, chunks, lag, x_ref, held, red, sems, lambda at: None, after_step)
    grads = left_dot(own_in_ref[...], low_ref[...])
    parts, _, _ = own_ref.shape
    kept = grads.shape[0] // parts
    for part in range(parts):
        own_ref[part, 0:kept, :] = grads[part * kept : (part + 1) * kept]


def tail_sum(
    x,
    scale_one,
    scale_mid,
    cos_tab,
    sin_tab,
    gain_one,
    gain_mid,
    unit,
    q_down,
    k_proj,
    v_proj,
    own_in,
    block_input,
    d_hidden,
    axis,
    n,
    parts,
    cid,
):
    rows, width = block_input.shape
    block = min(128, rows // 2)
    chunks = chunk_count(rows, 32, 8)
    kept = -(-(own_in.shape[1] // parts) // 8) * 8 + 8
    vmem = pl.BlockSpec(memory_space=pltpu.VMEM)
    anywhere = pl.BlockSpec(memory_space=pl.ANY)
    loaded = (unit, q_down, k_proj, v_proj, own_in)
    return pl.pallas_call(
        functools.partial(tail_kernel, axis, n, chunks, 2, block),
        out_shape=(
            jax.ShapeDtypeStruct((rows, width), jnp.bfloat16),
            jax.ShapeDtypeStruct((parts, kept, x.shape[1]), jnp.float32),
            jax.ShapeDtypeStruct((8, width), jnp.float32),
            jax.ShapeDtypeStruct((8, unit.shape[1]), jnp.float32),
        ),
        in_specs=[vmem] * 7 + [anywhere] * 7,
        out_specs=(anywhere, vmem, vmem, vmem),
        scratch_shapes=[pltpu.VMEM(x.shape, jnp.float32)] * 2
        + [pltpu.VMEM(item.shape, item.dtype) for item in loaded]
        + [
            pltpu.VMEM((block, width), jnp.bfloat16),
            pltpu.VMEM((block, width), jnp.float32),
            pltpu.VMEM((block, width), jnp.bfloat16),
            pltpu.VMEM(x.shape, jnp.bfloat16),
            pltpu.SemaphoreType.DMA((len(loaded),)),
            pltpu.SemaphoreType.DMA((2,)),
            pltpu.SemaphoreType.DMA((1,)),
        ]
        + [pltpu.SemaphoreType.DMA((2, chunks))] * 4,
        compiler_params=pltpu.CompilerParams(
            collective_id=cid, has_side_effects=True, vmem_limit_bytes=60 << 20
        ),
        name="tail_sum",
    )(x, scale_one, scale_mid, cos_tab, sin_tab, gain_one, gain_mid, *loaded, block_input, d_hidden)


def attend_kernel(
    axis,
    n,
    chunks,
    lag,
    seq_len,
    block,
    raw_ref,
    k_ref,
    v_ref,
    own_ref,
    all_ref,
    cos_ref,
    sin_ref,
    out_ref,
    base_ref,
    o_ref,
    q_ref,
    mixed_ref,
    norm_ref,
    part,
    red,
    *sems,
):
    rows, head_dim = k_ref.shape
    heads = raw_ref.shape[1] // head_dim
    half_dim = head_dim // 2
    blocks = seq_len // block
    scale = head_dim ** (-0.5)
    pairs = rows // (2 * block)
    turns = heads + 1
    pair_jobs = 2 * turns

    def job(j, carry):
        pair = lax.div(j, pair_jobs)
        side = lax.div(lax.rem(j, pair_jobs), turns)
        head = lax.rem(j, turns)
        row_block = side * pairs + pair
        seq = lax.div(row_block, blocks)
        block_at = lax.rem(row_block, blocks)
        own = pl.ds(pl.multiple_of(row_block * block, block), block)
        cols = pl.ds(pl.multiple_of(head * head_dim, head_dim), head_dim)
        low_cols = pl.ds(pl.multiple_of(head * head_dim, half_dim), half_dim)
        high_cols = pl.ds(pl.multiple_of(head * head_dim + half_dim, half_dim), half_dim)

        def run(reach):
            keys = pl.ds(pl.multiple_of(seq * seq_len, seq_len), reach)
            first = raw_ref[own, low_cols]
            second = raw_ref[own, high_cols]
            cos_tab = cos_ref[own, :]
            sin_tab = sin_ref[own, :]
            q_ref[own, low_cols] = (first * cos_tab - second * sin_tab).astype(q_ref.dtype)
            q_ref[own, high_cols] = (second * cos_tab + first * sin_tab).astype(q_ref.dtype)
            scores = right_dot(q_ref[own, cols], k_ref[keys, :]) * scale
            q_pos = block_at * block + lax.broadcasted_iota(jnp.int32, scores.shape, 0)
            k_pos = lax.broadcasted_iota(jnp.int32, scores.shape, 1)
            same = own_ref[own, :] == all_ref[:, keys]
            scores = jnp.where((k_pos <= q_pos) | same, scores, masked_score)
            row_max = jnp.max(scores, axis=1, keepdims=True)
            exp_terms = jnp.exp(scores - row_max)
            row_sum = jnp.sum(exp_terms, axis=1, keepdims=True)
            probs = (exp_terms * (1.0 / row_sum)).astype(jnp.bfloat16)
            mixed = jnp.dot(probs, v_ref[keys, :], preferred_element_type=jnp.float32)
            mixed_ref[own, cols] = mixed.astype(mixed_ref.dtype)
            norm_ref[head, own, :] = row_max + jnp.log(row_sum)

        reaches = reach_list(seq_len, block)
        for reach in sorted(set(reaches)):
            first = reaches.index(reach)
            last = first + reaches.count(reach) - 1

            @pl.when((head < heads) & (block_at >= first) & (block_at <= last))
            def _():
                run(reach)

        @pl.when(head == heads)
        def _():
            part[own, :] = jnp.dot(
                mixed_ref[own, :], out_ref[...], preferred_element_type=jnp.float32
            )

        @pl.when((head == heads) & (lax.axis_index(axis) == 0))
        def _():
            part[own, :] += base_ref[own, :].astype(jnp.float32)

        return carry

    lax.fori_loop(0, pair_jobs, job, 0)
    pair_steps = chunks // pairs

    def after_step(s, steps):
        bounds = tuple(
            jnp.minimum((pair_steps + at) * pair_jobs // pair_steps, pairs * pair_jobs)
            for at in (s, s + 1)
        )
        lax.fori_loop(*bounds, job, 0)

    line_steps(axis, n, chunks, lag, part, o_ref, red, sems, lambda at: None, after_step)


def reach_list(seq_len, block):
    step = max(256, block)
    ends = [(b + 1) * block + PIECE for b in range(seq_len // block)]
    return [min(seq_len, -(-end // step) * step) for end in ends]


def attend(raw, k, v, own_ids, all_ids, cos_tab, sin_tab, out_proj, base, axis, n, seq_len, cid):
    rows, width = base.shape
    block = min(128, seq_len)
    chunks = chunk_count(rows, 32, 8)
    vmem = pl.BlockSpec(memory_space=pltpu.VMEM)
    return pl.pallas_call(
        functools.partial(attend_kernel, axis, n, chunks, 2, seq_len, block),
        out_shape=(
            jax.ShapeDtypeStruct((rows, width), jnp.float32),
            jax.ShapeDtypeStruct(raw.shape, jnp.bfloat16),
            jax.ShapeDtypeStruct(raw.shape, jnp.bfloat16),
            jax.ShapeDtypeStruct((raw.shape[1] // k.shape[1], rows, 1), jnp.float32),
        ),
        in_specs=[vmem] * 9,
        out_specs=(vmem,) * 4,
        scratch_shapes=[pltpu.VMEM((rows, width), jnp.float32)] * 2
        + [pltpu.SemaphoreType.DMA((2, chunks))] * 4,
        compiler_params=pltpu.CompilerParams(
            collective_id=cid, has_side_effects=True, vmem_limit_bytes=60 << 20
        ),
        name="attend",
    )(raw, k, v, own_ids, all_ids, cos_tab, sin_tab, out_proj, base)


def attend_back_kernel(
    axis,
    n,
    chunks,
    lag,
    seq_len,
    block,
    x_ref,
    base_ref,
    q_ref,
    dm_ref,
    k_ref,
    v_ref,
    norm_ref,
    own_ref,
    all_ref,
    cos_ref,
    sin_ref,
    up_ref,
    o_ref,
    dq_ref,
    sums_ref,
    red,
    held,
    *sems,
):
    rows, head_dim = k_ref.shape
    heads = q_ref.shape[1] // head_dim
    half_dim = head_dim // 2
    blocks = seq_len // block
    scale = head_dim ** (-0.5)
    rank = up_ref.shape[0]
    key_cols = slice(rank, rank + head_dim)
    val_cols = slice(rank + head_dim, rank + 2 * head_dim)
    sums_ref[:, rank:] = jnp.zeros((rows, 2 * head_dim), jnp.float32)

    def finish(at):
        o_ref[at] = (base_ref[at] + held[at]).astype(o_ref.dtype)

    def job(j, carry):
        head = lax.rem(j, heads)
        row_block = lax.div(j, heads)
        seq = lax.div(row_block, blocks)
        block_at = lax.rem(row_block, blocks)
        own = pl.ds(pl.multiple_of(row_block * block, block), block)
        cols = pl.ds(pl.multiple_of(head * head_dim, head_dim), head_dim)
        low_cols = pl.ds(pl.multiple_of(head * head_dim, half_dim), half_dim)
        high_cols = pl.ds(pl.multiple_of(head * head_dim + half_dim, half_dim), half_dim)

        def run(reach):
            keys = pl.ds(pl.multiple_of(seq * seq_len, seq_len), reach)
            q = q_ref[own, cols]
            dm = dm_ref[own, cols]
            k = k_ref[keys, :]
            v = v_ref[keys, :]
            scores = right_dot(q, k) * scale
            q_pos = block_at * block + lax.broadcasted_iota(jnp.int32, scores.shape, 0)
            k_pos = lax.broadcasted_iota(jnp.int32, scores.shape, 1)
            same = own_ref[own, :] == all_ref[:, keys]
            probs = jnp.where(
                (k_pos <= q_pos) | same, jnp.exp(scores - norm_ref[head, own, :]), 0.0
            )
            d_probs = right_dot(dm, v)
            row_sum = jnp.sum(probs * d_probs, axis=1, keepdims=True)
            d_scores = (probs * (d_probs - row_sum)).astype(jnp.bfloat16)
            sums_ref[keys, key_cols] += left_dot(d_scores, q) * scale
            sums_ref[keys, val_cols] += left_dot(probs.astype(jnp.bfloat16), dm)
            dq = jnp.dot(d_scores, k, preferred_element_type=jnp.float32) * scale
            first = dq[:, :half_dim]
            second = dq[:, half_dim:]
            cos_tab = cos_ref[own, :]
            sin_tab = sin_ref[own, :]
            dq_ref[own, low_cols] = (first * cos_tab + second * sin_tab).astype(dq_ref.dtype)
            dq_ref[own, high_cols] = (second * cos_tab - first * sin_tab).astype(dq_ref.dtype)

        reaches = reach_list(seq_len, block)
        for reach in sorted(set(reaches)):
            first = reaches.index(reach)
            last = first + reaches.count(reach) - 1

            @pl.when((block_at >= first) & (block_at <= last))
            def _():
                run(reach)

        @pl.when(head == heads - 1)
        def _():
            sums_ref[own, 0:rank] = right_dot(dq_ref[own, :], up_ref[...])

        return carry

    job_count = heads * (rows // block)

    def after_step(s, steps):
        lax.fori_loop(s * job_count // steps, (s + 1) * job_count // steps, job, 0)

    line_steps(axis, n, chunks, lag, x_ref, held, red, sems, finish, after_step)


def attend_back(
    x, base, q, dm, k, v, norm, own_ids, all_ids, cos_tab, sin_tab, q_up, axis, n, seq_len, cid
):
    chunks = chunk_count(x.shape[0], 32, 16)
    block = min(256, seq_len)
    vmem = pl.BlockSpec(memory_space=pltpu.VMEM)
    return pl.pallas_call(
        functools.partial(attend_back_kernel, axis, n, chunks, 2, seq_len, block),
        out_shape=(
            jax.ShapeDtypeStruct(x.shape, jnp.bfloat16),
            jax.ShapeDtypeStruct(q.shape, jnp.bfloat16),
            jax.ShapeDtypeStruct((k.shape[0], q_up.shape[0] + 2 * k.shape[1]), jnp.float32),
        ),
        in_specs=[vmem] * 12,
        out_specs=(vmem, vmem, vmem),
        scratch_shapes=[pltpu.VMEM(x.shape, x.dtype)] * 2
        + [pltpu.SemaphoreType.DMA((2, chunks))] * 4,
        compiler_params=line_params(cid),
        name="attend_back",
    )(x, base, q, dm, k, v, norm, own_ids, all_ids, cos_tab, sin_tab, q_up)


def shards(
    block_input,
    image_starts,
    norm_gain,
    q_down,
    q_gain,
    q_up,
    k_proj,
    v_proj,
    out_proj,
    mlp_gain,
    w_gate,
    w_up,
    w_down,
    d_output,
):
    row_count, model_width = block_input.shape
    dp_count = lax.axis_size("dp")
    tp_count = lax.axis_size("tensor")
    tp_index = lax.axis_index("tensor")

    def own_part(values, axis):
        split = values.shape[axis] // (dp_count * tp_count)
        shape = values.shape[:axis] + (dp_count, tp_count, split) + values.shape[axis + 1 :]
        picked = lax.dynamic_index_in_dim(values.reshape(shape), tp_index, axis + 1, keepdims=False)
        return picked

    seq_count = image_starts.shape[0]
    seq_len = row_count // seq_count
    head_dim = k_proj.shape[1]
    positions = jnp.arange(seq_len, dtype=jnp.float32)
    inv_freq = 10000.0 ** (-(jnp.arange(head_dim // 2, dtype=jnp.float32) * 2.0) / head_dim)
    angles = positions[:, None] * inv_freq[None, :]
    cos_all = jnp.tile(jnp.cos(angles), (seq_count, 1))
    sin_all = jnp.tile(jnp.sin(angles), (seq_count, 1))
    pos_int = jnp.arange(seq_len, dtype=jnp.int32)
    inside = (pos_int[None, :, None] >= image_starts[:, None, :]) & (
        pos_int[None, :, None] < image_starts[:, None, :] + PIECE
    )
    labels = jnp.arange(1, image_starts.shape[1] + 1, dtype=jnp.int32)
    piece_ids = jnp.sum(jnp.where(inside, labels, 0), axis=2)

    own_ids = jnp.where(piece_ids > 0, piece_ids, -1).reshape(row_count, 1)
    all_ids = piece_ids.reshape(1, row_count)
    input_f32 = block_input.astype(jnp.float32)
    gain_attn = norm_gain.astype(jnp.float32)
    gain_query = q_gain.astype(jnp.float32)
    gain_mlp = mlp_gain.astype(jnp.float32)
    cotan_f32 = d_output.astype(jnp.float32)
    normed_one, scale_one = normalize(input_f32)
    normed_in = (normed_one * gain_attn).astype(jnp.bfloat16)
    q_latent = jnp.dot(normed_in, q_down, preferred_element_type=jnp.float32)
    q_latent = lax.optimization_barrier(q_latent)
    q_unit, q_scale = normalize(q_latent)
    q_normed = (q_unit * gain_query).astype(jnp.bfloat16)
    q_raw = jnp.dot(q_normed, q_up, preferred_element_type=jnp.float32)
    key_rows = rotate(
        jnp.dot(normed_in, k_proj, preferred_element_type=jnp.float32), cos_all, sin_all
    ).astype(jnp.bfloat16)
    val_rows = jnp.dot(normed_in, v_proj, preferred_element_type=jnp.float32).astype(jnp.bfloat16)
    hidden_in, queries, mixed_heads, log_norm = attend(
        q_raw,
        key_rows,
        val_rows,
        own_ids,
        all_ids,
        cos_all,
        sin_all,
        out_proj,
        block_input,
        "tensor",
        tp_count,
        seq_len,
        5,
    )
    normed_two, scale_two = normalize(hidden_in)
    normed_mid = (normed_two * gain_mlp).astype(jnp.bfloat16)
    gate_pre = jnp.dot(normed_mid, w_gate, preferred_element_type=jnp.float32)
    up_pre = jnp.dot(normed_mid, w_up, preferred_element_type=jnp.float32)
    gate_sig = jax.nn.sigmoid(gate_pre)
    hidden_act = (gate_pre * gate_sig * up_pre).astype(jnp.bfloat16)
    d_act = right_dot(d_output, w_down)
    d_gate = (d_act * up_pre * gate_sig * (1.0 + gate_pre * (1.0 - gate_sig))).astype(jnp.bfloat16)
    d_up = (d_act * gate_pre * gate_sig).astype(jnp.bfloat16)
    d_mid_part = right_dot(d_gate, w_gate) + right_dot(d_up, w_up)
    d_mid, grad_wide, grad_down, out_part_one, out_part_two = mid_sum(
        d_mid_part,
        normed_mid,
        hidden_act,
        d_gate,
        d_up,
        d_output,
        w_down,
        "tensor",
        tp_count,
        dp_count,
        1,
    )
    grad_wide = lax.psum_scatter(grad_wide, "dp", scatter_dimension=0, tiled=True)
    grad_gate = grad_wide[: grad_wide.shape[0] // 2]
    grad_up = grad_wide[grad_wide.shape[0] // 2 :]
    grad_down = lax.psum_scatter(grad_down, "dp", scatter_dimension=1, tiled=True)
    grad_gain_mlp = jnp.sum(d_mid * normed_two, axis=0)
    d_hidden = cotan_f32 + norm_back(d_mid * gain_mlp, normed_two, scale_two)
    d_hidden_low = d_hidden.astype(jnp.bfloat16)
    grad_out = left_dot(mixed_heads, d_hidden_low)
    d_mixed = right_dot(d_hidden_low, out_proj).astype(jnp.bfloat16)
    half_rows = row_count // 2
    out_part_one, grad_out = lax.optimization_barrier((out_part_one, grad_out))
    grad_out = lax.psum_scatter(grad_out, "dp", scatter_dimension=1, tiled=True)
    output_one, d_q_raw, query_key_val = attend_back(
        out_part_one,
        hidden_in[:half_rows],
        queries,
        d_mixed,
        key_rows,
        val_rows,
        log_norm,
        own_ids,
        all_ids,
        cos_all,
        sin_all,
        q_up,
        "tensor",
        tp_count,
        seq_len,
        3,
    )
    grad_query_up = left_dot(q_normed, d_q_raw)
    query_key_val, grad_query_up = lax.optimization_barrier((query_key_val, grad_query_up))
    grad_query_up = lax.psum_scatter(grad_query_up, "dp", scatter_dimension=0, tiled=True)
    own_width = model_width // (dp_count * tp_count)
    own_at = jnp.arange(model_width // tp_count)
    own_at = (own_at // own_width * tp_count + tp_index) * own_width + own_at % own_width
    pick = (jnp.arange(model_width)[:, None] == own_at[None, :]).astype(jnp.bfloat16)
    own_in = jnp.dot(normed_in, pick, preferred_element_type=jnp.float32).astype(jnp.bfloat16)
    grad_input, own_grads, acc_one, acc_mid = tail_sum(
        query_key_val,
        scale_one,
        q_scale,
        cos_all,
        sin_all,
        gain_attn.reshape(1, -1),
        gain_query.reshape(1, -1),
        q_unit,
        q_down,
        k_proj,
        v_proj,
        own_in,
        block_input,
        d_hidden,
        "tensor",
        tp_count,
        dp_count,
        2,
    )
    gains = jnp.concatenate(
        [
            own_part(jnp.sum(acc_one, axis=0), 0),
            own_part(grad_gain_mlp, 0),
            own_part(jnp.sum(acc_mid, axis=0), 0),
        ],
        axis=1,
    )
    kept = own_width
    gain_row = own_grads.shape[1] - 8
    own_grads = lax.dynamic_update_slice(own_grads, gains[:, None, :], (0, gain_row, 0))
    own_grads = own_grads.reshape(-1, own_grads.shape[2])
    own_sum = lax.psum_scatter(own_grads, "dp", scatter_dimension=0, tiled=True)
    rank = q_down.shape[1]
    own_mid = rank // (dp_count * tp_count)
    grad_qd = own_sum[:kept, :rank]
    grad_key = own_sum[:kept, rank : rank + head_dim]
    grad_val = own_sum[:kept, rank + head_dim :]
    grad_g1 = own_sum[gain_row, :kept]
    grad_g2 = own_sum[gain_row, kept : 2 * kept]
    grad_gq = own_sum[gain_row, 2 * kept : 2 * kept + own_mid]
    output_two = line_sum(out_part_two, "tensor", tp_count, 4, base=hidden_in[half_rows:])
    block_output = jnp.concatenate([output_one, output_two], axis=0)
    return (
        block_output,
        grad_input,
        grad_g1,
        grad_qd,
        grad_gq,
        grad_query_up,
        grad_key,
        grad_val,
        grad_out,
        grad_g2,
        grad_gate,
        grad_up,
        grad_down,
    )


def solution(mesh):
    placed = (
        P("dp", None),
        P("dp", None),
        P(),
        P(),
        P(),
        P(None, "tensor"),
        P(),
        P(),
        P("tensor", None),
        P(),
        P(None, "tensor"),
        P(None, "tensor"),
        P("tensor", None),
        P("dp", None),
    )

    return jax.shard_map(
        shards,
        mesh=mesh,
        in_specs=placed,
        out_specs=(
            P("dp", None),
            P("dp", None),
            P(("dp", "tensor")),
            P(("dp", "tensor"), None),
            P(("dp", "tensor")),
            P("dp", "tensor"),
            P(("dp", "tensor"), None),
            P(("dp", "tensor"), None),
            P("tensor", "dp"),
            P(("dp", "tensor")),
            P("dp", "tensor"),
            P("dp", "tensor"),
            P("tensor", "dp"),
        ),
        check_vma=False,
    )
```

```python
import functools

import jax
import jax.numpy as jnp
from jax import lax
from jax.experimental import pallas as pl
from jax.experimental.pallas import tpu as pltpu
from jax.sharding import PartitionSpec as P


MESH = pl.DeviceIdType.MESH

PIECE = 256


epsilon = 1e-06
masked_score = -1e30


def normalize(values):
    scale_rows = lax.rsqrt(jnp.mean(values * values, axis=-1, keepdims=True) + epsilon)
    return (values * scale_rows, scale_rows)


def left_dot(left, right):
    return lax.dot_general(
        left, right, (((0,), (0,)), ((), ())), preferred_element_type=jnp.float32
    )


def right_dot(left, right):
    return lax.dot_general(
        left, right, (((1,), (1,)), ((), ())), preferred_element_type=jnp.float32
    )


def rotate(values, cos_tab, sin_tab):
    half = values.shape[-1] // 2
    first_half = values[..., :half]
    second_half = values[..., half:]
    return jnp.concatenate(
        [
            first_half * cos_tab - second_half * sin_tab,
            second_half * cos_tab + first_half * sin_tab,
        ],
        axis=-1,
    )


def line_steps(axis, n, chunks, lag, x_ref, held, red, sems, finish, after_step):
    me = lax.axis_index(axis)
    rows = x_ref.shape[0] // (2 * chunks)
    s_red, r_red, s_fin, r_fin = sems
    barrier = pltpu.get_barrier_semaphore()

    @pl.when(me > 0)
    def _():
        pl.semaphore_signal(barrier, inc=1, device_id={axis: me - 1}, device_id_type=MESH)

    @pl.when(me < n - 1)
    def _():
        pl.semaphore_signal(barrier, inc=1, device_id={axis: me + 1}, device_id_type=MESH)

    @pl.when((me == 0) | (me == n - 1))
    def _():
        pl.semaphore_wait(barrier, 1)

    @pl.when((me > 0) & (me < n - 1))
    def _():
        pl.semaphore_wait(barrier, 2)

    def at(half, c):
        return pl.ds(pl.multiple_of((half * chunks + c) * rows, rows), rows)

    def sum_copy(src, half, c):
        return pltpu.make_async_remote_copy(
            src_ref=src.at[at(half, c)],
            dst_ref=red.at[at(half, c)],
            send_sem=s_red.at[half, c],
            recv_sem=r_red.at[half, c],
            device_id={axis: me - 1 if half == 0 else me + 1},
            device_id_type=MESH,
        )

    def fin_copy(half, c):
        return pltpu.make_async_remote_copy(
            src_ref=held.at[at(half, c)],
            dst_ref=held.at[at(half, c)],
            send_sem=s_fin.at[half, c],
            recv_sem=r_fin.at[half, c],
            device_id={axis: me + 1 if half == 0 else me - 1},
            device_id_type=MESH,
        )

    steps = chunks + 2 * lag * (n - 1)

    def step(s, carry):
        for half in (0, 1):
            hop = (n - 1 - me) if half == 0 else me
            c = s - lag * hop
            ok = (c >= 0) & (c < chunks)

            @pl.when(ok & (hop == 0))
            def _():
                sum_copy(x_ref, half, c).start()

            @pl.when(ok & (hop > 0) & (hop < n - 1))
            def _():
                sum_copy(x_ref, half, c).wait_recv()
                red[at(half, c)] = red[at(half, c)] + x_ref[at(half, c)]
                sum_copy(red, half, c).start()

            @pl.when(ok & (hop == n - 1))
            def _():
                sum_copy(x_ref, half, c).wait_recv()
                held[at(half, c)] = red[at(half, c)] + x_ref[at(half, c)]
                fin_copy(half, c).start()
                finish(at(half, c))

        for half in (0, 1):
            back = me if half == 0 else (n - 1 - me)
            c = s - lag * (n - 1) - lag * back
            ok = (c >= 0) & (c < chunks)

            @pl.when(ok & (back > 0))
            def _():
                fin_copy(half, c).wait_recv()

            @pl.when(ok & (back > 0) & (back < n - 1))
            def _():
                fin_copy(half, c).start()

            @pl.when(ok & (back > 0))
            def _():
                finish(at(half, c))

        if after_step is not None:
            after_step(s, steps)
        return carry

    lax.fori_loop(0, steps, step, 0)

    def drain(c, carry):
        for half in (0, 1):
            hop = (n - 1 - me) if half == 0 else me

            @pl.when(hop < n - 1)
            def _():
                sum_copy(x_ref, half, c).wait_send()

            @pl.when(hop > 0)
            def _():
                fin_copy(half, c).wait_send()

        return carry

    lax.fori_loop(0, chunks, drain, 0)


def line_low_kernel(axis, n, chunks, lag, x_ref, o_ref, red, held, *sems):
    def finish(at):
        o_ref[at] = held[at].astype(o_ref.dtype)

    line_steps(axis, n, chunks, lag, x_ref, held, red, sems, finish, None)


def chunk_count(rows, most, tile):
    chunks = most
    while rows % (2 * chunks * tile):
        chunks -= 1
    return chunks


def line_params(cid):
    return pltpu.CompilerParams(
        collective_id=cid, has_side_effects=True, vmem_limit_bytes=56 << 20
    )


def line_sum(x, axis, n, cid):
    chunks = chunk_count(x.shape[0], 32, 16)
    return pl.pallas_call(
        functools.partial(line_low_kernel, axis, n, chunks, 2),
        out_shape=jax.ShapeDtypeStruct(x.shape, jnp.bfloat16),
        in_specs=[pl.BlockSpec(memory_space=pltpu.VMEM)],
        out_specs=pl.BlockSpec(memory_space=pltpu.VMEM),
        scratch_shapes=[pltpu.VMEM(x.shape, x.dtype)] * 2
        + [pltpu.SemaphoreType.DMA((2, chunks))] * 4,
        compiler_params=line_params(cid),
        name="line_sum",
    )(x)


def fold_rows(values):
    return jnp.sum(values.reshape(values.shape[0] // 8, 8, values.shape[1]), axis=0)


def mid_kernel(
    axis,
    n,
    chunks,
    lag,
    x_ref,
    scale_ref,
    gain_ref,
    mid_hbm,
    act_hbm,
    gate_hbm,
    up_hbm,
    cot_hbm,
    down_hbm,
    hidden_hbm,
    d_hidden_ref,
    d_low_ref,
    acc_ref,
    grad_wide_ref,
    grad_down_ref,
    one_ref,
    two_ref,
    held,
    red,
    mid_ref,
    act_ref,
    gate_ref,
    up_ref,
    cot_ref,
    down_ref,
    wide_tile,
    row_tile,
    base_tile,
    hidden_tile,
    d_tile,
    low_tile,
    load_sem,
    wide_sem,
    row_sem,
    base_sem,
    hidden_sem,
    d_sem,
    low_sem,
    *sems,
):
    me = lax.axis_index(axis)
    rows, width = cot_ref.shape
    part_rows = rows // (2 * chunks)
    acc_ref[...] = jnp.zeros_like(acc_ref)
    units = act_ref.shape[1]
    wide = wide_tile.shape[0]
    wide_count = width // wide
    tile = min(256, rows // 2)
    by_units = units % 128 == 0 and units >= tile
    tall_count = -(-units // tile) if by_units else width // tile
    row_blocks = rows // tile
    loads = [
        pltpu.make_async_copy(src, dst, load_sem.at[i])
        for i, (src, dst) in enumerate(
            (
                (mid_hbm, mid_ref),
                (gate_hbm, gate_ref),
                (up_hbm, up_ref),
                (act_hbm, act_ref),
                (cot_hbm, cot_ref),
                (down_hbm, down_ref),
            )
        )
    ]
    for load in loads:
        load.start()

    def block(t):
        return pl.ds(pl.multiple_of(t * tile, tile), tile)

    def wide_copy(which, t):
        to = pl.ds(pl.multiple_of((2 * t + which) * wide, wide), wide)
        return pltpu.make_async_copy(wide_tile, grad_wide_ref.at[to], wide_sem.at[0])

    def tall_at(t):
        return pl.ds(pl.multiple_of(jnp.minimum(t * tile, units - tile), 128), tile)

    def tall_copy(t):
        if by_units:
            return pltpu.make_async_copy(
                row_tile.at[0:tile], grad_down_ref.at[tall_at(t)], row_sem.at[0]
            )
        return pltpu.make_async_copy(
            row_tile.at[0:units, 0:tile], grad_down_ref.at[:, block(t)], row_sem.at[0]
        )

    def out_copy(dst, t):
        return pltpu.make_async_copy(row_tile.at[0:tile], dst.at[block(t)], row_sem.at[0])

    half_blocks = row_blocks // 2
    tall_from = 2 * wide_count
    out_from = tall_from + tall_count
    job_count = out_from + row_blocks

    def job(j, carry):
        @pl.when(j == 0)
        def _():
            for load in loads:
                load.wait()

        for which, src in enumerate((gate_ref, up_ref)):
            t = lax.div(j, 2)

            @pl.when((j < tall_from) & (lax.rem(j, 2) == which))
            def _():
                cols = pl.ds(pl.multiple_of(t * wide, wide), wide)
                value = left_dot(mid_ref[:, cols], src[...])
                if which:
                    wide_copy(0, t).wait()
                else:

                    @pl.when(t > 0)
                    def _():
                        wide_copy(1, t - 1).wait()

                wide_tile[...] = value
                wide_copy(which, t).start()

        @pl.when((j >= tall_from) & (j < out_from))
        def _():
            t = j - tall_from

            @pl.when(t > 0)
            def _():
                tall_copy(t - 1).wait()

            if by_units:
                row_tile[...] = left_dot(act_ref[:, tall_at(t)], cot_ref[...])
            else:
                row_tile[0:units, 0:tile] = left_dot(act_ref[...], cot_ref[:, block(t)])
            tall_copy(t).start()

        for side, dst in enumerate((one_ref, two_ref)):
            t = j - out_from - side * half_blocks

            @pl.when((t >= 0) & (t < half_blocks))
            def _():
                @pl.when(t > 0)
                def _():
                    out_copy(dst, t - 1).wait()

                @pl.when(t == 0)
                def _():
                    if side == 0:
                        tall_copy(tall_count - 1).wait()
                    else:
                        out_copy(one_ref, half_blocks - 1).wait()

                base = pltpu.make_async_copy(
                    hidden_hbm.at[block(t + side * half_blocks)], base_tile, base_sem.at[0]
                )
                base.start()
                row_tile[0:tile, :] = jnp.dot(
                    act_ref[block(t + side * half_blocks), :],
                    down_ref[...],
                    preferred_element_type=jnp.float32,
                )
                base.wait()

                @pl.when(me == 0)
                def _():
                    row_tile[0:tile, :] += base_tile[...]

                out_copy(dst, t).start()

        return carry

    def after_step(s, steps):
        late = steps - 4
        bounds = tuple(jnp.clip(at - 2, 0, late) * job_count // late for at in (s, s + 1))
        lax.fori_loop(*bounds, job, 0)
        for half in (0, 1):
            back = me if half == 0 else (n - 1 - me)
            c = s - lag * (n - 1) - lag * back

            @pl.when((c + 1 >= 0) & (c + 1 < chunks))
            def _():
                take_hidden(half, c + 1).start()

            @pl.when((c >= 0) & (c < chunks))
            def _():
                close(half, c)

    def at_chunk(half, c):
        return pl.ds(pl.multiple_of((half * chunks + c) * part_rows, part_rows), part_rows)

    def take_hidden(half, c):
        slot = lax.rem(c, 2)
        return pltpu.make_async_copy(
            hidden_hbm.at[at_chunk(half, c)], hidden_tile.at[half, slot], hidden_sem.at[half, slot]
        )

    def put(tile_ref, dst, sem, half, c):
        slot = lax.rem(c, 2)
        return pltpu.make_async_copy(
            tile_ref.at[half, slot], dst.at[at_chunk(half, c)], sem.at[half, slot]
        )

    def puts(half, c):
        return (
            put(d_tile, d_hidden_ref, d_sem, half, c),
            put(low_tile, d_low_ref, low_sem, half, c),
        )

    def close(half, c):
        at = at_chunk(half, c)
        slot = lax.rem(c, 2)
        take_hidden(half, c).wait()

        @pl.when(c >= 2)
        def _():
            for item in puts(half, c - 2):
                item.wait()

        d_mid = held[at]
        scale = scale_ref[at, :]
        normed = hidden_tile[half, slot] * scale
        acc_ref[...] += fold_rows(d_mid * normed)
        grad_normed = d_mid * gain_ref[...]
        mean = jnp.mean(grad_normed * normed, axis=1, keepdims=True)
        d_hidden = cot_ref[at].astype(jnp.float32) + scale * (grad_normed - normed * mean)
        d_tile[half, slot] = d_hidden
        low_tile[half, slot] = d_hidden.astype(low_tile.dtype)
        for item in puts(half, c):
            item.start()

    line_steps(axis, n, chunks, lag, x_ref, held, red, sems, lambda at: None, after_step)
    for half in (0, 1):
        for c in range(max(chunks - 2, 0), chunks):
            for item in puts(half, c):
                item.wait()
    wide_copy(1, wide_count - 1).wait()
    out_copy(two_ref, half_blocks - 1).wait()


def mid_sum(x, scale, gain, mid, act, d_gate, d_up, cot, w_down, hidden, axis, n, parts, cid):
    rows, width = x.shape
    units = act.shape[1]
    tile = min(256, rows // 2)
    chunks = chunk_count(rows, 32, 16)
    vmem = pl.BlockSpec(memory_space=pltpu.VMEM)
    anywhere = pl.BlockSpec(memory_space=pl.ANY)
    loaded = (mid, act, d_gate, d_up, cot, w_down)
    tall = tile if units % 128 == 0 and units >= tile else max(tile, units)
    return pl.pallas_call(
        functools.partial(mid_kernel, axis, n, chunks, 2),
        out_shape=(
            jax.ShapeDtypeStruct(x.shape, jnp.float32),
            jax.ShapeDtypeStruct(x.shape, jnp.bfloat16),
            jax.ShapeDtypeStruct((8, width), jnp.float32),
            jax.ShapeDtypeStruct((2 * width, units), jnp.float32),
            jax.ShapeDtypeStruct((units, width), jnp.float32),
            jax.ShapeDtypeStruct((rows // 2, width), jnp.float32),
            jax.ShapeDtypeStruct((rows // 2, width), jnp.float32),
        ),
        in_specs=[vmem] * 3 + [anywhere] * 7,
        out_specs=(anywhere, anywhere, vmem) + (anywhere,) * 4,
        scratch_shapes=[pltpu.VMEM(x.shape, jnp.float32)] * 2
        + [pltpu.VMEM(item.shape, item.dtype) for item in loaded]
        + [
            pltpu.VMEM((width // parts, units), jnp.float32),
            pltpu.VMEM((tall, width), jnp.float32),
            pltpu.VMEM((tile, width), jnp.float32),
            pltpu.VMEM((2, 2, rows // (2 * chunks), width), jnp.float32),
            pltpu.VMEM((2, 2, rows // (2 * chunks), width), jnp.float32),
            pltpu.VMEM((2, 2, rows // (2 * chunks), width), jnp.bfloat16),
            pltpu.SemaphoreType.DMA((len(loaded),)),
        ]
        + [pltpu.SemaphoreType.DMA((1,))] * 3
        + [pltpu.SemaphoreType.DMA((2, 2))] * 3
        + [pltpu.SemaphoreType.DMA((2, chunks))] * 4,
        compiler_params=pltpu.CompilerParams(
            collective_id=cid, has_side_effects=True, vmem_limit_bytes=62 << 20
        ),
        name="mid_sum",
    )(x, scale, gain, *loaded, hidden)


def tail_kernel(
    axis,
    n,
    chunks,
    lag,
    block,
    x_ref,
    scale_one_ref,
    scale_mid_ref,
    cos_ref,
    sin_ref,
    gain_one_ref,
    gain_mid_ref,
    unit_hbm,
    down_hbm,
    key_hbm,
    val_hbm,
    own_hbm,
    input_hbm,
    hidden_hbm,
    grad_hbm,
    own_ref,
    acc_one_ref,
    acc_mid_ref,
    held,
    red,
    unit_ref,
    down_ref,
    key_ref,
    val_ref,
    own_in_ref,
    input_ref,
    hidden_ref,
    grad_ref,
    low_ref,
    load_sem,
    block_sem,
    store_sem,
    *sems,
):
    me = lax.axis_index(axis)
    rows = x_ref.shape[0]
    rank = unit_ref.shape[1]
    head_dim = key_ref.shape[1]
    half_dim = head_dim // 2
    pairs = rows // (2 * block)
    per = chunks // pairs
    loads = [
        pltpu.make_async_copy(src, dst, load_sem.at[i])
        for i, (src, dst) in enumerate(
            (
                (unit_hbm, unit_ref),
                (down_hbm, down_ref),
                (key_hbm, key_ref),
                (val_hbm, val_ref),
                (own_hbm, own_in_ref),
            )
        )
    ]
    for load in loads:
        load.start()
    acc_one_ref[...] = jnp.zeros_like(acc_one_ref)
    acc_mid_ref[...] = jnp.zeros_like(acc_mid_ref)
    own_ref[...] = jnp.zeros_like(own_ref)

    def store(own):
        return pltpu.make_async_copy(grad_ref, grad_hbm.at[own], store_sem.at[0])

    def consume(row_block):
        own = pl.ds(pl.multiple_of(row_block * block, block), block)
        take_input = pltpu.make_async_copy(input_hbm.at[own], input_ref, block_sem.at[0])
        take_hidden = pltpu.make_async_copy(hidden_hbm.at[own], hidden_ref, block_sem.at[1])
        take_input.start()
        take_hidden.start()
        d_bq = held[own, 0:rank]
        unit = unit_ref[own, :]
        acc_mid_ref[...] += fold_rows(d_bq * unit)
        eq = d_bq * gain_mid_ref[...]
        mean_mid = jnp.mean(eq * unit, axis=1, keepdims=True)
        d_latent = (scale_mid_ref[own, :] * (eq - unit * mean_mid)).astype(jnp.bfloat16)
        first = held[own, rank : rank + half_dim]
        second = held[own, rank + half_dim : rank + head_dim]
        cos_tab = cos_ref[own, :]
        sin_tab = sin_ref[own, :]
        low_ref[own, 0:rank] = d_latent
        low_ref[own, rank : rank + half_dim] = (first * cos_tab + second * sin_tab).astype(
            jnp.bfloat16
        )
        low_ref[own, rank + half_dim : rank + head_dim] = (
            second * cos_tab - first * sin_tab
        ).astype(jnp.bfloat16)
        low_ref[own, rank + head_dim :] = held[own, rank + head_dim :].astype(jnp.bfloat16)
        d_in = (
            right_dot(d_latent, down_ref[...])
            + right_dot(low_ref[own, rank : rank + head_dim], key_ref[...])
            + right_dot(low_ref[own, rank + head_dim :], val_ref[...])
        )
        take_input.wait()
        take_hidden.wait()
        scale_one = scale_one_ref[own, :]
        normed = input_ref[...].astype(jnp.float32) * scale_one
        acc_one_ref[...] += fold_rows(d_in * normed)
        e_in = d_in * gain_one_ref[...]
        mean_one = jnp.mean(e_in * normed, axis=1, keepdims=True)
        grad_ref[...] = (hidden_ref[...] + scale_one * (e_in - normed * mean_one)).astype(
            grad_ref.dtype
        )
        store(own).start()
        store(own).wait()

    def after_step(s, steps):
        @pl.when(s == lag)
        def _():
            for load in loads:
                load.wait()

        for half in (0, 1):
            back = me if half == 0 else (n - 1 - me)
            c = s - lag * (n - 1) - lag * back

            @pl.when((c >= 0) & (c < chunks) & (lax.rem(c + 1, per) == 0))
            def _():
                consume(half * pairs + lax.div(c, per))

    line_steps(axis, n, chunks, lag, x_ref, held, red, sems, lambda at: None, after_step)
    grads = left_dot(own_in_ref[...], low_ref[...])
    parts, _, _ = own_ref.shape
    kept = grads.shape[0] // parts
    for part in range(parts):
        own_ref[part, 0:kept, :] = grads[part * kept : (part + 1) * kept]


def tail_sum(
    x,
    scale_one,
    scale_mid,
    cos_tab,
    sin_tab,
    gain_one,
    gain_mid,
    unit,
    q_down,
    k_proj,
    v_proj,
    own_in,
    block_input,
    d_hidden,
    axis,
    n,
    parts,
    cid,
):
    rows, width = block_input.shape
    block = min(128, rows // 2)
    chunks = chunk_count(rows, 32, 8)
    kept = -(-(own_in.shape[1] // parts) // 8) * 8 + 8
    vmem = pl.BlockSpec(memory_space=pltpu.VMEM)
    anywhere = pl.BlockSpec(memory_space=pl.ANY)
    loaded = (unit, q_down, k_proj, v_proj, own_in)
    return pl.pallas_call(
        functools.partial(tail_kernel, axis, n, chunks, 2, block),
        out_shape=(
            jax.ShapeDtypeStruct((rows, width), jnp.bfloat16),
            jax.ShapeDtypeStruct((parts, kept, x.shape[1]), jnp.float32),
            jax.ShapeDtypeStruct((8, width), jnp.float32),
            jax.ShapeDtypeStruct((8, unit.shape[1]), jnp.float32),
        ),
        in_specs=[vmem] * 7 + [anywhere] * 7,
        out_specs=(anywhere, vmem, vmem, vmem),
        scratch_shapes=[pltpu.VMEM(x.shape, jnp.float32)] * 2
        + [pltpu.VMEM(item.shape, item.dtype) for item in loaded]
        + [
            pltpu.VMEM((block, width), jnp.bfloat16),
            pltpu.VMEM((block, width), jnp.float32),
            pltpu.VMEM((block, width), jnp.bfloat16),
            pltpu.VMEM(x.shape, jnp.bfloat16),
            pltpu.SemaphoreType.DMA((len(loaded),)),
            pltpu.SemaphoreType.DMA((2,)),
            pltpu.SemaphoreType.DMA((1,)),
        ]
        + [pltpu.SemaphoreType.DMA((2, chunks))] * 4,
        compiler_params=pltpu.CompilerParams(
            collective_id=cid, has_side_effects=True, vmem_limit_bytes=60 << 20
        ),
        name="tail_sum",
    )(x, scale_one, scale_mid, cos_tab, sin_tab, gain_one, gain_mid, *loaded, block_input, d_hidden)


def attend_kernel(
    axis,
    n,
    chunks,
    lag,
    seq_len,
    block,
    raw_ref,
    k_ref,
    v_ref,
    own_ref,
    all_ref,
    cos_ref,
    sin_ref,
    out_ref,
    base_ref,
    gain_ref,
    o_ref,
    q_ref,
    mixed_ref,
    norm_ref,
    normed_ref,
    scale_ref,
    part,
    red,
    *sems,
):
    rows, head_dim = k_ref.shape
    heads = raw_ref.shape[1] // head_dim
    half_dim = head_dim // 2
    blocks = seq_len // block
    scale = head_dim ** (-0.5)
    pairs = rows // (2 * block)
    turns = heads + 1
    pair_jobs = 2 * turns

    def job(j, carry):
        pair = lax.div(j, pair_jobs)
        side = lax.div(lax.rem(j, pair_jobs), turns)
        head = lax.rem(j, turns)
        row_block = side * pairs + pair
        seq = lax.div(row_block, blocks)
        block_at = lax.rem(row_block, blocks)
        own = pl.ds(pl.multiple_of(row_block * block, block), block)
        cols = pl.ds(pl.multiple_of(head * head_dim, head_dim), head_dim)
        low_cols = pl.ds(pl.multiple_of(head * head_dim, half_dim), half_dim)
        high_cols = pl.ds(pl.multiple_of(head * head_dim + half_dim, half_dim), half_dim)

        def run(reach):
            keys = pl.ds(pl.multiple_of(seq * seq_len, seq_len), reach)
            first = raw_ref[own, low_cols]
            second = raw_ref[own, high_cols]
            cos_tab = cos_ref[own, :]
            sin_tab = sin_ref[own, :]
            q_ref[own, low_cols] = (first * cos_tab - second * sin_tab).astype(q_ref.dtype)
            q_ref[own, high_cols] = (second * cos_tab + first * sin_tab).astype(q_ref.dtype)
            scores = right_dot(q_ref[own, cols], k_ref[keys, :]) * scale
            q_pos = block_at * block + lax.broadcasted_iota(jnp.int32, scores.shape, 0)
            k_pos = lax.broadcasted_iota(jnp.int32, scores.shape, 1)
            same = own_ref[own, :] == all_ref[:, keys]
            scores = jnp.where((k_pos <= q_pos) | same, scores, masked_score)
            row_max = jnp.max(scores, axis=1, keepdims=True)
            exp_terms = jnp.exp(scores - row_max)
            row_sum = jnp.sum(exp_terms, axis=1, keepdims=True)
            probs = (exp_terms * (1.0 / row_sum)).astype(jnp.bfloat16)
            mixed = jnp.dot(probs, v_ref[keys, :], preferred_element_type=jnp.float32)
            mixed_ref[own, cols] = mixed.astype(mixed_ref.dtype)
            norm_ref[head, own, :] = row_max + jnp.log(row_sum)

        reaches = reach_list(seq_len, block)
        for reach in sorted(set(reaches)):
            first = reaches.index(reach)
            last = first + reaches.count(reach) - 1

            @pl.when((head < heads) & (block_at >= first) & (block_at <= last))
            def _():
                run(reach)

        @pl.when(head == heads)
        def _():
            part[own, :] = jnp.dot(
                mixed_ref[own, :], out_ref[...], preferred_element_type=jnp.float32
            )

        @pl.when((head == heads) & (lax.axis_index(axis) == 0))
        def _():
            part[own, :] += base_ref[own, :].astype(jnp.float32)

        return carry

    lax.fori_loop(0, pair_jobs, job, 0)
    pair_steps = chunks // pairs

    def after_step(s, steps):
        bounds = tuple(
            jnp.minimum((pair_steps + at) * pair_jobs // pair_steps, pairs * pair_jobs)
            for at in (s, s + 1)
        )
        lax.fori_loop(*bounds, job, 0)

    def finish(at):
        hidden = o_ref[at]
        scale_rows = lax.rsqrt(jnp.mean(hidden * hidden, axis=1, keepdims=True) + epsilon)
        scale_ref[at, :] = scale_rows
        normed_ref[at] = (hidden * scale_rows * gain_ref[...]).astype(normed_ref.dtype)

    line_steps(axis, n, chunks, lag, part, o_ref, red, sems, finish, after_step)


def reach_list(seq_len, block):
    step = max(256, block)
    ends = [(b + 1) * block + PIECE for b in range(seq_len // block)]
    return [min(seq_len, -(-end // step) * step) for end in ends]


def attend(
    raw, k, v, own_ids, all_ids, cos_tab, sin_tab, out_proj, base, gain, axis, n, seq_len, cid
):
    rows, width = base.shape
    block = min(64, seq_len)
    chunks = chunk_count(rows, 32, 16)
    vmem = pl.BlockSpec(memory_space=pltpu.VMEM)
    return pl.pallas_call(
        functools.partial(attend_kernel, axis, n, chunks, 2, seq_len, block),
        out_shape=(
            jax.ShapeDtypeStruct((rows, width), jnp.float32),
            jax.ShapeDtypeStruct(raw.shape, jnp.bfloat16),
            jax.ShapeDtypeStruct(raw.shape, jnp.bfloat16),
            jax.ShapeDtypeStruct((raw.shape[1] // k.shape[1], rows, 1), jnp.float32),
            jax.ShapeDtypeStruct((rows, width), jnp.bfloat16),
            jax.ShapeDtypeStruct((rows, 1), jnp.float32),
        ),
        in_specs=[vmem] * 10,
        out_specs=(vmem,) * 6,
        scratch_shapes=[pltpu.VMEM((rows, width), jnp.float32)] * 2
        + [pltpu.SemaphoreType.DMA((2, chunks))] * 4,
        compiler_params=pltpu.CompilerParams(
            collective_id=cid, has_side_effects=True, vmem_limit_bytes=60 << 20
        ),
        name="attend",
    )(raw, k, v, own_ids, all_ids, cos_tab, sin_tab, out_proj, base, gain)


def attend_back_kernel(
    axis,
    n,
    chunks,
    lag,
    seq_len,
    block,
    x_ref,
    q_ref,
    dm_ref,
    k_ref,
    v_ref,
    norm_ref,
    own_ref,
    all_ref,
    cos_ref,
    sin_ref,
    up_ref,
    o_ref,
    dq_ref,
    sums_ref,
    red,
    held,
    *sems,
):
    rows, head_dim = k_ref.shape
    heads = q_ref.shape[1] // head_dim
    half_dim = head_dim // 2
    blocks = seq_len // block
    scale = head_dim ** (-0.5)
    rank = up_ref.shape[0]
    key_cols = slice(rank, rank + head_dim)
    val_cols = slice(rank + head_dim, rank + 2 * head_dim)
    sums_ref[:, rank:] = jnp.zeros((rows, 2 * head_dim), jnp.float32)

    def finish(at):
        o_ref[at] = held[at].astype(o_ref.dtype)

    def job(j, carry):
        head = lax.rem(j, heads)
        row_block = lax.div(j, heads)
        seq = lax.div(row_block, blocks)
        block_at = lax.rem(row_block, blocks)
        own = pl.ds(pl.multiple_of(row_block * block, block), block)
        cols = pl.ds(pl.multiple_of(head * head_dim, head_dim), head_dim)
        low_cols = pl.ds(pl.multiple_of(head * head_dim, half_dim), half_dim)
        high_cols = pl.ds(pl.multiple_of(head * head_dim + half_dim, half_dim), half_dim)

        def run(reach):
            keys = pl.ds(pl.multiple_of(seq * seq_len, seq_len), reach)
            q = q_ref[own, cols]
            dm = dm_ref[own, cols]
            k = k_ref[keys, :]
            v = v_ref[keys, :]
            scores = right_dot(q, k) * scale
            q_pos = block_at * block + lax.broadcasted_iota(jnp.int32, scores.shape, 0)
            k_pos = lax.broadcasted_iota(jnp.int32, scores.shape, 1)
            same = own_ref[own, :] == all_ref[:, keys]
            probs = jnp.where(
                (k_pos <= q_pos) | same, jnp.exp(scores - norm_ref[head, own, :]), 0.0
            )
            d_probs = right_dot(dm, v)
            row_sum = jnp.sum(probs * d_probs, axis=1, keepdims=True)
            d_scores = (probs * (d_probs - row_sum)).astype(jnp.bfloat16)
            sums_ref[keys, key_cols] += left_dot(d_scores, q) * scale
            sums_ref[keys, val_cols] += left_dot(probs.astype(jnp.bfloat16), dm)
            dq = jnp.dot(d_scores, k, preferred_element_type=jnp.float32) * scale
            first = dq[:, :half_dim]
            second = dq[:, half_dim:]
            cos_tab = cos_ref[own, :]
            sin_tab = sin_ref[own, :]
            dq_ref[own, low_cols] = (first * cos_tab + second * sin_tab).astype(dq_ref.dtype)
            dq_ref[own, high_cols] = (second * cos_tab - first * sin_tab).astype(dq_ref.dtype)

        reaches = reach_list(seq_len, block)
        for reach in sorted(set(reaches)):
            first = reaches.index(reach)
            last = first + reaches.count(reach) - 1

            @pl.when((block_at >= first) & (block_at <= last))
            def _():
                run(reach)

        @pl.when(head == heads - 1)
        def _():
            sums_ref[own, 0:rank] = right_dot(dq_ref[own, :], up_ref[...])

        return carry

    job_count = heads * (rows // block)

    def after_step(s, steps):
        lax.fori_loop(s * job_count // steps, (s + 1) * job_count // steps, job, 0)

    line_steps(axis, n, chunks, lag, x_ref, held, red, sems, finish, after_step)


def attend_back(
    x, q, dm, k, v, norm, own_ids, all_ids, cos_tab, sin_tab, q_up, axis, n, seq_len, cid
):
    chunks = chunk_count(x.shape[0], 32, 16)
    block = min(256, seq_len)
    vmem = pl.BlockSpec(memory_space=pltpu.VMEM)
    return pl.pallas_call(
        functools.partial(attend_back_kernel, axis, n, chunks, 2, seq_len, block),
        out_shape=(
            jax.ShapeDtypeStruct(x.shape, jnp.bfloat16),
            jax.ShapeDtypeStruct(q.shape, jnp.bfloat16),
            jax.ShapeDtypeStruct((k.shape[0], q_up.shape[0] + 2 * k.shape[1]), jnp.float32),
        ),
        in_specs=[vmem] * 11,
        out_specs=(vmem, vmem, vmem),
        scratch_shapes=[pltpu.VMEM(x.shape, x.dtype)] * 2
        + [pltpu.SemaphoreType.DMA((2, chunks))] * 4,
        compiler_params=line_params(cid),
        name="attend_back",
    )(x, q, dm, k, v, norm, own_ids, all_ids, cos_tab, sin_tab, q_up)


def shards(
    block_input,
    image_starts,
    norm_gain,
    q_down,
    q_gain,
    q_up,
    k_proj,
    v_proj,
    out_proj,
    mlp_gain,
    w_gate,
    w_up,
    w_down,
    d_output,
):
    row_count, model_width = block_input.shape
    dp_count = lax.axis_size("dp")
    tp_count = lax.axis_size("tensor")
    tp_index = lax.axis_index("tensor")

    def own_part(values, axis):
        split = values.shape[axis] // (dp_count * tp_count)
        shape = values.shape[:axis] + (dp_count, tp_count, split) + values.shape[axis + 1 :]
        picked = lax.dynamic_index_in_dim(values.reshape(shape), tp_index, axis + 1, keepdims=False)
        return picked

    seq_count = image_starts.shape[0]
    seq_len = row_count // seq_count
    head_dim = k_proj.shape[1]
    positions = jnp.arange(seq_len, dtype=jnp.float32)
    inv_freq = 10000.0 ** (-(jnp.arange(head_dim // 2, dtype=jnp.float32) * 2.0) / head_dim)
    angles = positions[:, None] * inv_freq[None, :]
    cos_all = jnp.tile(jnp.cos(angles), (seq_count, 1))
    sin_all = jnp.tile(jnp.sin(angles), (seq_count, 1))
    pos_int = jnp.arange(seq_len, dtype=jnp.int32)
    inside = (pos_int[None, :, None] >= image_starts[:, None, :]) & (
        pos_int[None, :, None] < image_starts[:, None, :] + PIECE
    )
    labels = jnp.arange(1, image_starts.shape[1] + 1, dtype=jnp.int32)
    piece_ids = jnp.sum(jnp.where(inside, labels, 0), axis=2)

    own_ids = jnp.where(piece_ids > 0, piece_ids, -1).reshape(row_count, 1)
    all_ids = piece_ids.reshape(1, row_count)
    input_f32 = block_input.astype(jnp.float32)
    gain_attn = norm_gain.astype(jnp.float32)
    gain_query = q_gain.astype(jnp.float32)
    gain_mlp = mlp_gain.astype(jnp.float32)
    cotan_f32 = d_output.astype(jnp.float32)
    normed_one, scale_one = normalize(input_f32)
    normed_in = (normed_one * gain_attn).astype(jnp.bfloat16)
    q_latent = jnp.dot(normed_in, q_down, preferred_element_type=jnp.float32)
    q_latent = lax.optimization_barrier(q_latent)
    q_unit, q_scale = normalize(q_latent)
    q_normed = (q_unit * gain_query).astype(jnp.bfloat16)
    q_raw = jnp.dot(q_normed, q_up, preferred_element_type=jnp.float32)
    key_rows = rotate(
        jnp.dot(normed_in, k_proj, preferred_element_type=jnp.float32), cos_all, sin_all
    ).astype(jnp.bfloat16)
    val_rows = jnp.dot(normed_in, v_proj, preferred_element_type=jnp.float32).astype(jnp.bfloat16)
    hidden_in, queries, mixed_heads, log_norm, normed_mid, scale_two = attend(
        q_raw,
        key_rows,
        val_rows,
        own_ids,
        all_ids,
        cos_all,
        sin_all,
        out_proj,
        block_input,
        gain_mlp.reshape(1, -1),
        "tensor",
        tp_count,
        seq_len,
        5,
    )
    gate_pre = jnp.dot(normed_mid, w_gate, preferred_element_type=jnp.float32)
    up_pre = jnp.dot(normed_mid, w_up, preferred_element_type=jnp.float32)
    gate_sig = jax.nn.sigmoid(gate_pre)
    hidden_act = (gate_pre * gate_sig * up_pre).astype(jnp.bfloat16)
    d_act = right_dot(d_output, w_down)
    d_gate = (d_act * up_pre * gate_sig * (1.0 + gate_pre * (1.0 - gate_sig))).astype(jnp.bfloat16)
    d_up = (d_act * gate_pre * gate_sig).astype(jnp.bfloat16)
    d_mid_part = right_dot(d_gate, w_gate) + right_dot(d_up, w_up)
    d_hidden, d_hidden_low, acc_two, grad_wide, grad_down, out_part_one, out_part_two = mid_sum(
        d_mid_part,
        scale_two,
        gain_mlp.reshape(1, -1),
        normed_mid,
        hidden_act,
        d_gate,
        d_up,
        d_output,
        w_down,
        hidden_in,
        "tensor",
        tp_count,
        dp_count,
        1,
    )
    grad_wide = lax.psum_scatter(grad_wide, "dp", scatter_dimension=0, tiled=True)
    grad_gate = grad_wide[: grad_wide.shape[0] // 2]
    grad_up = grad_wide[grad_wide.shape[0] // 2 :]
    grad_down = lax.psum_scatter(grad_down, "dp", scatter_dimension=1, tiled=True)
    grad_out = left_dot(mixed_heads, d_hidden_low)
    d_mixed = right_dot(d_hidden_low, out_proj).astype(jnp.bfloat16)
    out_part_one, grad_out = lax.optimization_barrier((out_part_one, grad_out))
    grad_out = lax.psum_scatter(grad_out, "dp", scatter_dimension=1, tiled=True)
    output_one, d_q_raw, query_key_val = attend_back(
        out_part_one,
        queries,
        d_mixed,
        key_rows,
        val_rows,
        log_norm,
        own_ids,
        all_ids,
        cos_all,
        sin_all,
        q_up,
        "tensor",
        tp_count,
        seq_len,
        3,
    )
    grad_query_up = left_dot(q_normed, d_q_raw)
    query_key_val, grad_query_up = lax.optimization_barrier((query_key_val, grad_query_up))
    grad_query_up = lax.psum_scatter(grad_query_up, "dp", scatter_dimension=0, tiled=True)
    own_width = model_width // (dp_count * tp_count)
    own_at = jnp.arange(model_width // tp_count)
    own_at = (own_at // own_width * tp_count + tp_index) * own_width + own_at % own_width
    pick = (jnp.arange(model_width)[:, None] == own_at[None, :]).astype(jnp.bfloat16)
    own_in = jnp.dot(normed_in, pick, preferred_element_type=jnp.float32).astype(jnp.bfloat16)
    grad_input, own_grads, acc_one, acc_mid = tail_sum(
        query_key_val,
        scale_one,
        q_scale,
        cos_all,
        sin_all,
        gain_attn.reshape(1, -1),
        gain_query.reshape(1, -1),
        q_unit,
        q_down,
        k_proj,
        v_proj,
        own_in,
        block_input,
        d_hidden,
        "tensor",
        tp_count,
        dp_count,
        2,
    )
    gains = jnp.concatenate(
        [
            own_part(jnp.sum(acc_one, axis=0), 0),
            own_part(jnp.sum(acc_two, axis=0), 0),
            own_part(jnp.sum(acc_mid, axis=0), 0),
        ],
        axis=1,
    )
    kept = own_width
    gain_row = own_grads.shape[1] - 8
    own_grads = lax.dynamic_update_slice(own_grads, gains[:, None, :], (0, gain_row, 0))
    own_grads = own_grads.reshape(-1, own_grads.shape[2])
    own_sum = lax.psum_scatter(own_grads, "dp", scatter_dimension=0, tiled=True)
    rank = q_down.shape[1]
    own_mid = rank // (dp_count * tp_count)
    grad_qd = own_sum[:kept, :rank]
    grad_key = own_sum[:kept, rank : rank + head_dim]
    grad_val = own_sum[:kept, rank + head_dim :]
    grad_g1 = own_sum[gain_row, :kept]
    grad_g2 = own_sum[gain_row, kept : 2 * kept]
    grad_gq = own_sum[gain_row, 2 * kept : 2 * kept + own_mid]
    output_two = line_sum(out_part_two, "tensor", tp_count, 4)
    block_output = jnp.concatenate([output_one, output_two], axis=0)
    return (
        block_output,
        grad_input,
        grad_g1,
        grad_qd,
        grad_gq,
        grad_query_up,
        grad_key,
        grad_val,
        grad_out,
        grad_g2,
        grad_gate,
        grad_up,
        grad_down,
    )


def solution(mesh):
    placed = (
        P("dp", None),
        P("dp", None),
        P(),
        P(),
        P(),
        P(None, "tensor"),
        P(),
        P(),
        P("tensor", None),
        P(),
        P(None, "tensor"),
        P(None, "tensor"),
        P("tensor", None),
        P("dp", None),
    )

    return jax.shard_map(
        shards,
        mesh=mesh,
        in_specs=placed,
        out_specs=(
            P("dp", None),
            P("dp", None),
            P(("dp", "tensor")),
            P(("dp", "tensor"), None),
            P(("dp", "tensor")),
            P("dp", "tensor"),
            P(("dp", "tensor"), None),
            P(("dp", "tensor"), None),
            P("tensor", "dp"),
            P(("dp", "tensor")),
            P("dp", "tensor"),
            P("dp", "tensor"),
            P("tensor", "dp"),
        ),
        check_vma=False,
    )
```

```python
import functools
import math

import jax
import jax.numpy as jnp
from jax import lax
from jax.experimental import pallas as pl
from jax.experimental.pallas import tpu as pltpu
from jax.sharding import PartitionSpec as P


MESH = pl.DeviceIdType.MESH

PIECE = 256


epsilon = 1e-06
masked_score = -1e30


def normalize(values):
    scale_rows = lax.rsqrt(jnp.mean(values * values, axis=-1, keepdims=True) + epsilon)
    return (values * scale_rows, scale_rows)


def left_dot(left, right):
    return lax.dot_general(
        left, right, (((0,), (0,)), ((), ())), preferred_element_type=jnp.float32
    )


def right_dot(left, right):
    return lax.dot_general(
        left, right, (((1,), (1,)), ((), ())), preferred_element_type=jnp.float32
    )


def rotate(values, cos_tab, sin_tab):
    half = values.shape[-1] // 2
    first_half = values[..., :half]
    second_half = values[..., half:]
    return jnp.concatenate(
        [
            first_half * cos_tab - second_half * sin_tab,
            second_half * cos_tab + first_half * sin_tab,
        ],
        axis=-1,
    )


def line_steps(axis, n, chunks, lag, x_ref, held, red, sems, finish, after_step):
    me = lax.axis_index(axis)
    rows = x_ref.shape[0] // (2 * chunks)
    s_red, r_red, s_fin, r_fin = sems
    barrier = pltpu.get_barrier_semaphore()

    @pl.when(me > 0)
    def _():
        pl.semaphore_signal(barrier, inc=1, device_id={axis: me - 1}, device_id_type=MESH)

    @pl.when(me < n - 1)
    def _():
        pl.semaphore_signal(barrier, inc=1, device_id={axis: me + 1}, device_id_type=MESH)

    @pl.when((me == 0) | (me == n - 1))
    def _():
        pl.semaphore_wait(barrier, 1)

    @pl.when((me > 0) & (me < n - 1))
    def _():
        pl.semaphore_wait(barrier, 2)

    def at(half, c):
        return pl.ds(pl.multiple_of((half * chunks + c) * rows, rows), rows)

    def sum_copy(src, half, c):
        return pltpu.make_async_remote_copy(
            src_ref=src.at[at(half, c)],
            dst_ref=red.at[at(half, c)],
            send_sem=s_red.at[half, c],
            recv_sem=r_red.at[half, c],
            device_id={axis: me - 1 if half == 0 else me + 1},
            device_id_type=MESH,
        )

    def fin_copy(half, c):
        return pltpu.make_async_remote_copy(
            src_ref=held.at[at(half, c)],
            dst_ref=held.at[at(half, c)],
            send_sem=s_fin.at[half, c],
            recv_sem=r_fin.at[half, c],
            device_id={axis: me + 1 if half == 0 else me - 1},
            device_id_type=MESH,
        )

    steps = chunks + 2 * lag * (n - 1)

    def step(s, carry):
        for half in (0, 1):
            hop = (n - 1 - me) if half == 0 else me
            c = s - lag * hop
            ok = (c >= 0) & (c < chunks)

            @pl.when(ok & (hop == 0))
            def _():
                sum_copy(x_ref, half, c).start()

            @pl.when(ok & (hop > 0) & (hop < n - 1))
            def _():
                sum_copy(x_ref, half, c).wait_recv()
                red[at(half, c)] = red[at(half, c)] + x_ref[at(half, c)]
                sum_copy(red, half, c).start()

            @pl.when(ok & (hop == n - 1))
            def _():
                sum_copy(x_ref, half, c).wait_recv()
                held[at(half, c)] = red[at(half, c)] + x_ref[at(half, c)]
                fin_copy(half, c).start()
                finish(at(half, c))

        for half in (0, 1):
            back = me if half == 0 else (n - 1 - me)
            c = s - lag * (n - 1) - lag * back
            ok = (c >= 0) & (c < chunks)

            @pl.when(ok & (back > 0))
            def _():
                fin_copy(half, c).wait_recv()

            @pl.when(ok & (back > 0) & (back < n - 1))
            def _():
                fin_copy(half, c).start()

            @pl.when(ok & (back > 0))
            def _():
                finish(at(half, c))

        if after_step is not None:
            after_step(s, steps)
        return carry

    lax.fori_loop(0, steps, step, 0)

    def drain(c, carry):
        for half in (0, 1):
            hop = (n - 1 - me) if half == 0 else me

            @pl.when(hop < n - 1)
            def _():
                sum_copy(x_ref, half, c).wait_send()

            @pl.when(hop > 0)
            def _():
                fin_copy(half, c).wait_send()

        return carry

    lax.fori_loop(0, chunks, drain, 0)


def line_low_kernel(axis, n, chunks, lag, x_ref, o_ref, red, held, *sems):
    def finish(at):
        o_ref[at] = held[at].astype(o_ref.dtype)

    line_steps(axis, n, chunks, lag, x_ref, held, red, sems, finish, None)


def chunk_count(rows, most, tile):
    chunks = most
    while rows % (2 * chunks * tile):
        chunks -= 1
    return chunks


def line_params(cid):
    return pltpu.CompilerParams(
        collective_id=cid, has_side_effects=True, vmem_limit_bytes=56 << 20
    )


def line_sum(x, axis, n, cid):
    chunks = chunk_count(x.shape[0], 32, 16)
    return pl.pallas_call(
        functools.partial(line_low_kernel, axis, n, chunks, 2),
        out_shape=jax.ShapeDtypeStruct(x.shape, jnp.bfloat16),
        in_specs=[pl.BlockSpec(memory_space=pltpu.VMEM)],
        out_specs=pl.BlockSpec(memory_space=pltpu.VMEM),
        scratch_shapes=[pltpu.VMEM(x.shape, x.dtype)] * 2
        + [pltpu.SemaphoreType.DMA((2, chunks))] * 4,
        compiler_params=line_params(cid),
        name="line_sum",
    )(x)


def fold_rows(values):
    return jnp.sum(values.reshape(values.shape[0] // 8, 8, values.shape[1]), axis=0)


def mid_kernel(
    axis,
    n,
    chunks,
    lag,
    x_ref,
    scale_ref,
    gain_ref,
    mid_hbm,
    act_hbm,
    gate_hbm,
    up_hbm,
    cot_hbm,
    down_hbm,
    hidden_hbm,
    d_hidden_ref,
    d_low_ref,
    acc_ref,
    grad_wide_ref,
    grad_down_ref,
    one_ref,
    two_ref,
    held,
    red,
    mid_ref,
    act_ref,
    gate_ref,
    up_ref,
    cot_ref,
    down_ref,
    wide_tile,
    row_tile,
    base_tile,
    hidden_tile,
    d_tile,
    low_tile,
    load_sem,
    wide_sem,
    row_sem,
    base_sem,
    hidden_sem,
    d_sem,
    low_sem,
    *sems,
):
    me = lax.axis_index(axis)
    rows, width = cot_ref.shape
    part_rows = rows // (2 * chunks)
    acc_ref[...] = jnp.zeros_like(acc_ref)
    units = act_ref.shape[1]
    wide = wide_tile.shape[0]
    wide_count = width // wide
    tile = min(256, rows // 2)
    by_units = units % 128 == 0 and units >= tile
    tall_count = -(-units // tile) if by_units else width // tile
    loads = [
        pltpu.make_async_copy(src, dst, load_sem.at[i])
        for i, (src, dst) in enumerate(
            (
                (mid_hbm, mid_ref),
                (gate_hbm, gate_ref),
                (up_hbm, up_ref),
                (act_hbm, act_ref),
                (cot_hbm, cot_ref),
                (down_hbm, down_ref),
            )
        )
    ]
    for load in loads:
        load.start()

    def block(t):
        return pl.ds(pl.multiple_of(t * tile, tile), tile)

    def wide_copy(which, t):
        to = pl.ds(pl.multiple_of((2 * t + which) * wide, wide), wide)
        return pltpu.make_async_copy(wide_tile, grad_wide_ref.at[to], wide_sem.at[0])

    def tall_at(t):
        return pl.ds(pl.multiple_of(jnp.minimum(t * tile, units - tile), 128), tile)

    def tall_copy(t):
        if by_units:
            return pltpu.make_async_copy(
                row_tile.at[0:tile], grad_down_ref.at[tall_at(t)], row_sem.at[0]
            )
        return pltpu.make_async_copy(
            row_tile.at[0:units, 0:tile], grad_down_ref.at[0:units, block(t)], row_sem.at[0]
        )

    def out_block(t):
        return pl.ds(pl.multiple_of(t * out_tile, out_tile), out_tile)

    def out_copy(dst, t):
        return pltpu.make_async_copy(row_tile.at[0:out_tile], dst.at[out_block(t)], row_sem.at[0])

    out_tile = base_tile.shape[0]
    out_counts = (one_ref.shape[0] // out_tile, two_ref.shape[0] // out_tile)
    tall_from = 2 * wide_count
    out_from = tall_from + tall_count
    job_count = out_from + sum(out_counts)

    def job(j, carry):
        @pl.when(j == 0)
        def _():
            for load in loads:
                load.wait()

        for which, src in enumerate((gate_ref, up_ref)):
            t = lax.div(j, 2)

            @pl.when((j < tall_from) & (lax.rem(j, 2) == which))
            def _():
                cols = pl.ds(pl.multiple_of(t * wide, wide), wide)
                value = left_dot(mid_ref[:, cols], src[...])
                if which:
                    wide_copy(0, t).wait()
                else:

                    @pl.when(t > 0)
                    def _():
                        wide_copy(1, t - 1).wait()

                wide_tile[...] = value
                wide_copy(which, t).start()

        @pl.when((j >= tall_from) & (j < out_from))
        def _():
            t = j - tall_from

            @pl.when(t > 0)
            def _():
                tall_copy(t - 1).wait()

            if by_units:
                row_tile[...] = left_dot(act_ref[:, tall_at(t)], cot_ref[...])
            else:
                row_tile[0:units, 0:tile] = left_dot(act_ref[...], cot_ref[:, block(t)])
            tall_copy(t).start()

        for side, dst in enumerate((one_ref, two_ref)):
            begin = side * out_counts[0]
            t = j - out_from - begin

            @pl.when((t >= 0) & (t < out_counts[side]))
            def _():
                @pl.when(t > 0)
                def _():
                    out_copy(dst, t - 1).wait()

                @pl.when(t == 0)
                def _():
                    if side == 0:
                        tall_copy(tall_count - 1).wait()
                    else:
                        out_copy(one_ref, out_counts[0] - 1).wait()

                base = pltpu.make_async_copy(
                    hidden_hbm.at[out_block(t + begin)], base_tile, base_sem.at[0]
                )
                base.start()
                row_tile[0:out_tile, :] = jnp.dot(
                    act_ref[out_block(t + begin), :],
                    down_ref[...],
                    preferred_element_type=jnp.float32,
                )
                base.wait()

                @pl.when(me == 0)
                def _():
                    row_tile[0:out_tile, :] += base_tile[...]

                out_copy(dst, t).start()

        return carry

    def after_step(s, steps):
        late = steps - 4
        bounds = tuple(jnp.clip(at - 2, 0, late) * job_count // late for at in (s, s + 1))
        lax.fori_loop(*bounds, job, 0)
        for half in (0, 1):
            back = me if half == 0 else (n - 1 - me)
            c = s - lag * (n - 1) - lag * back

            @pl.when((c + 1 >= 0) & (c + 1 < chunks))
            def _():
                take_hidden(half, c + 1).start()

            @pl.when((c >= 0) & (c < chunks))
            def _():
                close(half, c)

    def at_chunk(half, c):
        return pl.ds(pl.multiple_of((half * chunks + c) * part_rows, part_rows), part_rows)

    def take_hidden(half, c):
        slot = lax.rem(c, 2)
        return pltpu.make_async_copy(
            hidden_hbm.at[at_chunk(half, c)], hidden_tile.at[half, slot], hidden_sem.at[half, slot]
        )

    def put(tile_ref, dst, sem, half, c):
        slot = lax.rem(c, 2)
        return pltpu.make_async_copy(
            tile_ref.at[half, slot], dst.at[at_chunk(half, c)], sem.at[half, slot]
        )

    def puts(half, c):
        return (
            put(d_tile, d_hidden_ref, d_sem, half, c),
            put(low_tile, d_low_ref, low_sem, half, c),
        )

    def close(half, c):
        at = at_chunk(half, c)
        slot = lax.rem(c, 2)
        take_hidden(half, c).wait()

        @pl.when(c >= 2)
        def _():
            for item in puts(half, c - 2):
                item.wait()

        d_mid = held[at]
        scale = scale_ref[at, :]
        normed = hidden_tile[half, slot] * scale
        acc_ref[...] += fold_rows(d_mid * normed)
        grad_normed = d_mid * gain_ref[...]
        mean = jnp.mean(grad_normed * normed, axis=1, keepdims=True)
        d_hidden = cot_ref[at].astype(jnp.float32) + scale * (grad_normed - normed * mean)
        d_tile[half, slot] = d_hidden
        low_tile[half, slot] = d_hidden.astype(low_tile.dtype)
        for item in puts(half, c):
            item.start()

    line_steps(axis, n, chunks, lag, x_ref, held, red, sems, lambda at: None, after_step)
    for half in (0, 1):
        for c in range(max(chunks - 2, 0), chunks):
            for item in puts(half, c):
                item.wait()
    wide_copy(1, wide_count - 1).wait()
    out_copy(two_ref, out_counts[1] - 1).wait()


def mid_sum(x, scale, gain, mid, act, d_gate, d_up, cot, w_down, hidden, more, axis, n, parts, cid):
    rows, width = x.shape
    units = act.shape[1]
    tile = min(256, rows // 2)
    chunks = chunk_count(rows, 32, 16)
    vmem = pl.BlockSpec(memory_space=pltpu.VMEM)
    anywhere = pl.BlockSpec(memory_space=pl.ANY)
    loaded = (mid, act, d_gate, d_up, cot, w_down)
    tall = tile if units % 128 == 0 and units >= tile else max(tile, units)
    return pl.pallas_call(
        functools.partial(mid_kernel, axis, n, chunks, 2),
        out_shape=(
            jax.ShapeDtypeStruct(x.shape, jnp.float32),
            jax.ShapeDtypeStruct(x.shape, jnp.bfloat16),
            jax.ShapeDtypeStruct((8, width), jnp.float32),
            jax.ShapeDtypeStruct((2 * width, units), jnp.float32),
            jax.ShapeDtypeStruct((units + more, width), jnp.float32),
            jax.ShapeDtypeStruct((rows * 5 // 8, width), jnp.float32),
            jax.ShapeDtypeStruct((rows - rows * 5 // 8, width), jnp.float32),
        ),
        in_specs=[vmem] * 3 + [anywhere] * 7,
        out_specs=(anywhere, anywhere, vmem) + (anywhere,) * 4,
        scratch_shapes=[pltpu.VMEM(x.shape, jnp.float32)] * 2
        + [pltpu.VMEM(item.shape, item.dtype) for item in loaded]
        + [
            pltpu.VMEM((width // parts, units), jnp.float32),
            pltpu.VMEM((tall, width), jnp.float32),
            pltpu.VMEM((rows // 8, width), jnp.float32),
            pltpu.VMEM((2, 2, rows // (2 * chunks), width), jnp.float32),
            pltpu.VMEM((2, 2, rows // (2 * chunks), width), jnp.float32),
            pltpu.VMEM((2, 2, rows // (2 * chunks), width), jnp.bfloat16),
            pltpu.SemaphoreType.DMA((len(loaded),)),
        ]
        + [pltpu.SemaphoreType.DMA((1,))] * 3
        + [pltpu.SemaphoreType.DMA((2, 2))] * 3
        + [pltpu.SemaphoreType.DMA((2, chunks))] * 4,
        compiler_params=pltpu.CompilerParams(
            collective_id=cid, has_side_effects=True, vmem_limit_bytes=62 << 20
        ),
        name="mid_sum",
    )(x, scale, gain, *loaded, hidden)


def tail_kernel(
    axis,
    n,
    chunks,
    lag,
    block,
    x_ref,
    scale_one_ref,
    scale_mid_ref,
    cos_ref,
    sin_ref,
    gain_one_ref,
    gain_mid_ref,
    unit_hbm,
    down_hbm,
    key_hbm,
    val_hbm,
    pick_hbm,
    q_hbm,
    dq_hbm,
    input_hbm,
    hidden_hbm,
    grad_hbm,
    own_ref,
    acc_one_ref,
    acc_mid_ref,
    held,
    red,
    unit_ref,
    down_ref,
    key_ref,
    val_ref,
    pick_ref,
    q_ref,
    dq_ref,
    own_in_ref,
    input_ref,
    hidden_ref,
    grad_ref,
    low_ref,
    load_sem,
    block_sem,
    store_sem,
    *sems,
):
    me = lax.axis_index(axis)
    rows = x_ref.shape[0]
    rank = unit_ref.shape[1]
    head_dim = key_ref.shape[1]
    half_dim = head_dim // 2
    pairs = rows // (2 * block)
    per = chunks // pairs
    loads = [
        pltpu.make_async_copy(src, dst, load_sem.at[i])
        for i, (src, dst) in enumerate(
            (
                (unit_hbm, unit_ref),
                (down_hbm, down_ref),
                (key_hbm, key_ref),
                (val_hbm, val_ref),
                (pick_hbm, pick_ref),
                (q_hbm, q_ref),
                (dq_hbm, dq_ref),
            )
        )
    ]
    for load in loads:
        load.start()
    acc_one_ref[...] = jnp.zeros_like(acc_one_ref)
    acc_mid_ref[...] = jnp.zeros_like(acc_mid_ref)
    parts, all_rows, group = own_ref.shape
    own_groups = x_ref.shape[1] // group
    up_groups = dq_ref.shape[1] // group
    up_rows = q_ref.shape[1] // parts
    kept = (all_rows - up_groups * up_rows) // own_groups
    used = own_in_ref.shape[1] // parts
    for part in range(parts):
        for g in range(own_groups):
            own_ref[part, g * kept + used : (g + 1) * kept, :] = jnp.zeros(
                (kept - used, group), jnp.float32
            )
    up_tile = max(128, up_rows)
    up_count = q_ref.shape[1] // up_tile

    def up_job(t):
        cols = pl.ds(pl.multiple_of(t * up_tile, up_tile), up_tile)
        value = left_dot(q_ref[:, cols], dq_ref[...])
        for i in range(up_tile // up_rows):
            for g in range(up_groups):
                at = own_groups * kept + g * up_rows
                own_ref[t * (up_tile // up_rows) + i, at : at + up_rows, :] = value[
                    i * up_rows : (i + 1) * up_rows, g * group : (g + 1) * group
                ]

    def store(own):
        return pltpu.make_async_copy(grad_ref, grad_hbm.at[own], store_sem.at[0])

    def consume(row_block):
        own = pl.ds(pl.multiple_of(row_block * block, block), block)
        take_input = pltpu.make_async_copy(input_hbm.at[own], input_ref, block_sem.at[0])
        take_hidden = pltpu.make_async_copy(hidden_hbm.at[own], hidden_ref, block_sem.at[1])
        take_input.start()
        take_hidden.start()
        d_bq = held[own, 0:rank]
        unit = unit_ref[own, :]
        acc_mid_ref[...] += fold_rows(d_bq * unit)
        eq = d_bq * gain_mid_ref[...]
        mean_mid = jnp.mean(eq * unit, axis=1, keepdims=True)
        d_latent = (scale_mid_ref[own, :] * (eq - unit * mean_mid)).astype(jnp.bfloat16)
        first = held[own, rank : rank + half_dim]
        second = held[own, rank + half_dim : rank + head_dim]
        cos_tab = cos_ref[own, :]
        sin_tab = sin_ref[own, :]
        low_ref[own, 0:rank] = d_latent
        low_ref[own, rank : rank + half_dim] = (first * cos_tab + second * sin_tab).astype(
            jnp.bfloat16
        )
        low_ref[own, rank + half_dim : rank + head_dim] = (
            second * cos_tab - first * sin_tab
        ).astype(jnp.bfloat16)
        low_ref[own, rank + head_dim :] = held[own, rank + head_dim :].astype(jnp.bfloat16)
        d_in = (
            right_dot(d_latent, down_ref[...])
            + right_dot(low_ref[own, rank : rank + head_dim], key_ref[...])
            + right_dot(low_ref[own, rank + head_dim :], val_ref[...])
        )
        take_input.wait()
        take_hidden.wait()
        scale_one = scale_one_ref[own, :]
        normed = input_ref[...].astype(jnp.float32) * scale_one
        low_in = (normed * gain_one_ref[...]).astype(jnp.bfloat16)
        own_in_ref[own, :] = jnp.dot(
            low_in, pick_ref[...], preferred_element_type=jnp.float32
        ).astype(jnp.bfloat16)
        acc_one_ref[...] += fold_rows(d_in * normed)
        e_in = d_in * gain_one_ref[...]
        mean_one = jnp.mean(e_in * normed, axis=1, keepdims=True)
        grad_ref[...] = (hidden_ref[...] + scale_one * (e_in - normed * mean_one)).astype(
            grad_ref.dtype
        )
        store(own).start()
        store(own).wait()

    def after_step(s, steps):
        @pl.when(s == lag)
        def _():
            for load in loads:
                load.wait()

        @pl.when((s >= lag) & (s < lag + up_count))
        def _():
            up_job(s - lag)

        for half in (0, 1):
            back = me if half == 0 else (n - 1 - me)
            c = s - lag * (n - 1) - lag * back

            @pl.when((c >= 0) & (c < chunks) & (lax.rem(c + 1, per) == 0))
            def _():
                consume(half * pairs + lax.div(c, per))

    line_steps(axis, n, chunks, lag, x_ref, held, red, sems, lambda at: None, after_step)
    grads = left_dot(own_in_ref[...], low_ref[...])
    for part in range(parts):
        for g in range(own_groups):
            own_ref[part, g * kept : g * kept + used, :] = grads[
                part * used : (part + 1) * used, g * group : (g + 1) * group
            ]


def tail_sum(
    x,
    scale_one,
    scale_mid,
    cos_tab,
    sin_tab,
    gain_one,
    gain_mid,
    unit,
    q_down,
    k_proj,
    v_proj,
    pick,
    q_normed,
    d_q,
    block_input,
    d_hidden,
    axis,
    n,
    parts,
    cid,
):
    rows, width = block_input.shape
    block = min(128, rows // 2)
    chunks = chunk_count(rows, 32, 8)
    kept = -(-(pick.shape[1] // parts) // 8) * 8 + 8
    group = math.gcd(x.shape[1], d_q.shape[1])
    all_rows = x.shape[1] // group * kept + d_q.shape[1] // group * (q_normed.shape[1] // parts)
    vmem = pl.BlockSpec(memory_space=pltpu.VMEM)
    anywhere = pl.BlockSpec(memory_space=pl.ANY)
    loaded = (unit, q_down, k_proj, v_proj, pick, q_normed, d_q)
    return pl.pallas_call(
        functools.partial(tail_kernel, axis, n, chunks, 2, block),
        out_shape=(
            jax.ShapeDtypeStruct((rows, width), jnp.bfloat16),
            jax.ShapeDtypeStruct((parts, all_rows, group), jnp.float32),
            jax.ShapeDtypeStruct((8, width), jnp.float32),
            jax.ShapeDtypeStruct((8, unit.shape[1]), jnp.float32),
        ),
        in_specs=[vmem] * 7 + [anywhere] * 9,
        out_specs=(anywhere, vmem, vmem, vmem),
        scratch_shapes=[pltpu.VMEM(x.shape, jnp.float32)] * 2
        + [pltpu.VMEM(item.shape, item.dtype) for item in loaded]
        + [
            pltpu.VMEM((rows, pick.shape[1]), jnp.bfloat16),
            pltpu.VMEM((block, width), jnp.bfloat16),
            pltpu.VMEM((block, width), jnp.float32),
            pltpu.VMEM((block, width), jnp.bfloat16),
            pltpu.VMEM(x.shape, jnp.bfloat16),
            pltpu.SemaphoreType.DMA((len(loaded),)),
            pltpu.SemaphoreType.DMA((2,)),
            pltpu.SemaphoreType.DMA((1,)),
        ]
        + [pltpu.SemaphoreType.DMA((2, chunks))] * 4,
        compiler_params=pltpu.CompilerParams(
            collective_id=cid, has_side_effects=True, vmem_limit_bytes=60 << 20
        ),
        name="tail_sum",
    )(x, scale_one, scale_mid, cos_tab, sin_tab, gain_one, gain_mid, *loaded, block_input, d_hidden)


def attend_kernel(
    axis,
    n,
    chunks,
    lag,
    seq_len,
    block,
    raw_ref,
    k_ref,
    v_ref,
    own_ref,
    all_ref,
    cos_ref,
    sin_ref,
    out_ref,
    base_ref,
    gain_ref,
    o_ref,
    q_ref,
    mixed_ref,
    norm_ref,
    normed_ref,
    scale_ref,
    part,
    red,
    *sems,
):
    rows, head_dim = k_ref.shape
    heads = raw_ref.shape[1] // head_dim
    half_dim = head_dim // 2
    blocks = seq_len // block
    scale = head_dim ** (-0.5)
    pairs = rows // (2 * block)
    turns = heads + 1
    pair_jobs = 2 * turns

    def job(j, carry):
        pair = lax.div(j, pair_jobs)
        side = lax.div(lax.rem(j, pair_jobs), turns)
        head = lax.rem(j, turns)
        row_block = side * pairs + pair
        seq = lax.div(row_block, blocks)
        block_at = lax.rem(row_block, blocks)
        own = pl.ds(pl.multiple_of(row_block * block, block), block)
        cols = pl.ds(pl.multiple_of(head * head_dim, head_dim), head_dim)
        low_cols = pl.ds(pl.multiple_of(head * head_dim, half_dim), half_dim)
        high_cols = pl.ds(pl.multiple_of(head * head_dim + half_dim, half_dim), half_dim)

        def run(reach):
            keys = pl.ds(pl.multiple_of(seq * seq_len, seq_len), reach)
            first = raw_ref[own, low_cols]
            second = raw_ref[own, high_cols]
            cos_tab = cos_ref[own, :]
            sin_tab = sin_ref[own, :]
            q_ref[own, low_cols] = (first * cos_tab - second * sin_tab).astype(q_ref.dtype)
            q_ref[own, high_cols] = (second * cos_tab + first * sin_tab).astype(q_ref.dtype)
            scores = right_dot(q_ref[own, cols], k_ref[keys, :]) * scale
            q_pos = block_at * block + lax.broadcasted_iota(jnp.int32, scores.shape, 0)
            k_pos = lax.broadcasted_iota(jnp.int32, scores.shape, 1)
            same = own_ref[own, :] == all_ref[:, keys]
            scores = jnp.where((k_pos <= q_pos) | same, scores, masked_score)
            row_max = jnp.max(scores, axis=1, keepdims=True)
            exp_terms = jnp.exp(scores - row_max)
            row_sum = jnp.sum(exp_terms, axis=1, keepdims=True)
            probs = (exp_terms * (1.0 / row_sum)).astype(jnp.bfloat16)
            mixed = jnp.dot(probs, v_ref[keys, :], preferred_element_type=jnp.float32)
            mixed_ref[own, cols] = mixed.astype(mixed_ref.dtype)
            norm_ref[head, own, :] = row_max + jnp.log(row_sum)

        reaches = reach_list(seq_len, block)
        for reach in sorted(set(reaches)):
            first = reaches.index(reach)
            last = first + reaches.count(reach) - 1

            @pl.when((head < heads) & (block_at >= first) & (block_at <= last))
            def _():
                run(reach)

        @pl.when(head == heads)
        def _():
            part[own, :] = jnp.dot(
                mixed_ref[own, :], out_ref[...], preferred_element_type=jnp.float32
            )

        @pl.when((head == heads) & (lax.axis_index(axis) == 0))
        def _():
            part[own, :] += base_ref[own, :].astype(jnp.float32)

        return carry

    lax.fori_loop(0, pair_jobs, job, 0)
    pair_steps = chunks // pairs

    def after_step(s, steps):
        bounds = tuple(
            jnp.minimum((pair_steps + at) * pair_jobs // pair_steps, pairs * pair_jobs)
            for at in (s, s + 1)
        )
        lax.fori_loop(*bounds, job, 0)

    def finish(at):
        hidden = o_ref[at]
        scale_rows = lax.rsqrt(jnp.mean(hidden * hidden, axis=1, keepdims=True) + epsilon)
        scale_ref[at, :] = scale_rows
        normed_ref[at] = (hidden * scale_rows * gain_ref[...]).astype(normed_ref.dtype)

    line_steps(axis, n, chunks, lag, part, o_ref, red, sems, finish, after_step)


def reach_list(seq_len, block):
    step = max(256, block)
    ends = [(b + 1) * block + PIECE for b in range(seq_len // block)]
    return [min(seq_len, -(-end // step) * step) for end in ends]


def attend(
    raw, k, v, own_ids, all_ids, cos_tab, sin_tab, out_proj, base, gain, axis, n, seq_len, cid
):
    rows, width = base.shape
    block = min(64, seq_len)
    chunks = chunk_count(rows, 32, 16)
    vmem = pl.BlockSpec(memory_space=pltpu.VMEM)
    return pl.pallas_call(
        functools.partial(attend_kernel, axis, n, chunks, 2, seq_len, block),
        out_shape=(
            jax.ShapeDtypeStruct((rows, width), jnp.float32),
            jax.ShapeDtypeStruct(raw.shape, jnp.bfloat16),
            jax.ShapeDtypeStruct(raw.shape, jnp.bfloat16),
            jax.ShapeDtypeStruct((raw.shape[1] // k.shape[1], rows, 1), jnp.float32),
            jax.ShapeDtypeStruct((rows, width), jnp.bfloat16),
            jax.ShapeDtypeStruct((rows, 1), jnp.float32),
        ),
        in_specs=[vmem] * 10,
        out_specs=(vmem,) * 6,
        scratch_shapes=[pltpu.VMEM((rows, width), jnp.float32)] * 2
        + [pltpu.SemaphoreType.DMA((2, chunks))] * 4,
        compiler_params=pltpu.CompilerParams(
            collective_id=cid, has_side_effects=True, vmem_limit_bytes=60 << 20
        ),
        name="attend",
    )(raw, k, v, own_ids, all_ids, cos_tab, sin_tab, out_proj, base, gain)


def attend_back_kernel(
    axis,
    n,
    chunks,
    lag,
    seq_len,
    block,
    x_ref,
    k_ref,
    v_ref,
    norm_ref,
    own_ref,
    all_ref,
    cos_ref,
    sin_ref,
    q_hbm,
    low_hbm,
    proj_hbm,
    up_hbm,
    mixed_hbm,
    grads_hbm,
    o_ref,
    dq_ref,
    sums_ref,
    grads_ref,
    red,
    held,
    q_ref,
    low_ref,
    proj_ref,
    up_ref,
    mixed_ref,
    dm_ref,
    row_tile,
    load_sem,
    row_sem,
    *sems,
):
    rows, head_dim = k_ref.shape
    heads = q_ref.shape[1] // head_dim
    half_dim = head_dim // 2
    blocks = seq_len // block
    scale = head_dim ** (-0.5)
    rank = up_ref.shape[0]
    key_cols = slice(rank, rank + head_dim)
    val_cols = slice(rank + head_dim, rank + 2 * head_dim)
    loads = [
        pltpu.make_async_copy(src, dst, load_sem.at[i])
        for i, (src, dst) in enumerate(
            (
                (low_hbm, low_ref),
                (proj_hbm, proj_ref),
                (q_hbm, q_ref),
                (up_hbm, up_ref),
                (mixed_hbm, mixed_ref),
            )
        )
    ]
    for load in loads:
        load.start()
    sums_ref[:, rank:] = jnp.zeros((rows, 2 * head_dim), jnp.float32)
    tile = row_tile.shape[0]
    tile_count = mixed_ref.shape[1] // tile
    grads_at = grads_ref.shape[0] - mixed_ref.shape[1]

    def finish(at):
        o_ref[at] = held[at].astype(o_ref.dtype)

    def put(t):
        to = pl.ds(pl.multiple_of(grads_at + t * tile, 8), tile)
        return pltpu.make_async_copy(row_tile, grads_ref.at[to], row_sem.at[0])

    turns = heads + 1
    tiles_from = turns * (rows // block)
    job_count = tiles_from + tile_count

    def job(j, carry):
        @pl.when(j == 0)
        def _():
            for load in loads:
                load.wait()

        turn = lax.rem(j, turns)
        head = jnp.maximum(turn - 1, 0)
        row_block = jnp.minimum(lax.div(j, turns), rows // block - 1)
        in_blocks = j < tiles_from
        seq = lax.div(row_block, blocks)
        block_at = lax.rem(row_block, blocks)
        own = pl.ds(pl.multiple_of(row_block * block, block), block)
        cols = pl.ds(pl.multiple_of(head * head_dim, head_dim), head_dim)
        low_cols = pl.ds(pl.multiple_of(head * head_dim, half_dim), half_dim)
        high_cols = pl.ds(pl.multiple_of(head * head_dim + half_dim, half_dim), half_dim)

        @pl.when(in_blocks & (turn == 0))
        def _():
            dm_ref[own, :] = right_dot(low_ref[own, :], proj_ref[...]).astype(dm_ref.dtype)

        def run(reach):
            keys = pl.ds(pl.multiple_of(seq * seq_len, seq_len), reach)
            q = q_ref[own, cols]
            dm = dm_ref[own, cols]
            k = k_ref[keys, :]
            v = v_ref[keys, :]
            scores = right_dot(q, k) * scale
            q_pos = block_at * block + lax.broadcasted_iota(jnp.int32, scores.shape, 0)
            k_pos = lax.broadcasted_iota(jnp.int32, scores.shape, 1)
            same = own_ref[own, :] == all_ref[:, keys]
            probs = jnp.where(
                (k_pos <= q_pos) | same, jnp.exp(scores - norm_ref[head, own, :]), 0.0
            )
            d_probs = right_dot(dm, v)
            row_sum = jnp.sum(probs * d_probs, axis=1, keepdims=True)
            d_scores = (probs * (d_probs - row_sum)).astype(jnp.bfloat16)
            sums_ref[keys, key_cols] += left_dot(d_scores, q) * scale
            sums_ref[keys, val_cols] += left_dot(probs.astype(jnp.bfloat16), dm)
            dq = jnp.dot(d_scores, k, preferred_element_type=jnp.float32) * scale
            first = dq[:, :half_dim]
            second = dq[:, half_dim:]
            cos_tab = cos_ref[own, :]
            sin_tab = sin_ref[own, :]
            dq_ref[own, low_cols] = (first * cos_tab + second * sin_tab).astype(dq_ref.dtype)
            dq_ref[own, high_cols] = (second * cos_tab - first * sin_tab).astype(dq_ref.dtype)

        reaches = reach_list(seq_len, block)
        for reach in sorted(set(reaches)):
            first = reaches.index(reach)
            last = first + reaches.count(reach) - 1

            @pl.when(in_blocks & (turn > 0) & (block_at >= first) & (block_at <= last))
            def _():
                run(reach)

        @pl.when(in_blocks & (turn == heads))
        def _():
            sums_ref[own, 0:rank] = right_dot(dq_ref[own, :], up_ref[...])

        @pl.when(j >= tiles_from)
        def _():
            t = j - tiles_from

            @pl.when(t > 0)
            def _():
                put(t - 1).wait()

            part = pl.ds(pl.multiple_of(t * tile, tile), tile)
            row_tile[...] = left_dot(mixed_ref[:, part], low_ref[...])
            put(t).start()

        return carry

    def after_step(s, steps):
        late = steps - 2
        bounds = tuple(jnp.clip(at - 1, 0, late) * job_count // late for at in (s, s + 1))
        lax.fori_loop(*bounds, job, 0)

    line_steps(axis, n, chunks, lag, x_ref, held, red, sems, finish, after_step)
    put(tile_count - 1).wait()


def attend_back(
    x,
    k,
    v,
    norm,
    own_ids,
    all_ids,
    cos_tab,
    sin_tab,
    q,
    d_low,
    out_proj,
    q_up,
    mixed,
    grads,
    axis,
    n,
    seq_len,
    cid,
):
    chunks = chunk_count(x.shape[0], 32, 16)
    block = min(128, seq_len)
    vmem = pl.BlockSpec(memory_space=pltpu.VMEM)
    anywhere = pl.BlockSpec(memory_space=pl.ANY)
    loaded = (q, d_low, out_proj, q_up, mixed)
    return pl.pallas_call(
        functools.partial(attend_back_kernel, axis, n, chunks, 2, seq_len, block),
        out_shape=(
            jax.ShapeDtypeStruct(x.shape, jnp.bfloat16),
            jax.ShapeDtypeStruct(q.shape, jnp.bfloat16),
            jax.ShapeDtypeStruct((k.shape[0], q_up.shape[0] + 2 * k.shape[1]), jnp.float32),
            jax.ShapeDtypeStruct(grads.shape, grads.dtype),
        ),
        in_specs=[vmem] * 8 + [anywhere] * 6,
        out_specs=(vmem, vmem, vmem, anywhere),
        input_output_aliases={13: 3},
        scratch_shapes=[pltpu.VMEM(x.shape, x.dtype)] * 2
        + [pltpu.VMEM(item.shape, item.dtype) for item in loaded]
        + [
            pltpu.VMEM(q.shape, jnp.bfloat16),
            pltpu.VMEM((min(256, q.shape[1]), d_low.shape[1]), jnp.float32),
            pltpu.SemaphoreType.DMA((len(loaded),)),
            pltpu.SemaphoreType.DMA((1,)),
        ]
        + [pltpu.SemaphoreType.DMA((2, chunks))] * 4,
        compiler_params=pltpu.CompilerParams(
            collective_id=cid, has_side_effects=True, vmem_limit_bytes=61 << 20
        ),
        name="attend_back",
    )(x, k, v, norm, own_ids, all_ids, cos_tab, sin_tab, *loaded, grads)


def shards(
    block_input,
    image_starts,
    norm_gain,
    q_down,
    q_gain,
    q_up,
    k_proj,
    v_proj,
    out_proj,
    mlp_gain,
    w_gate,
    w_up,
    w_down,
    d_output,
):
    row_count, model_width = block_input.shape
    dp_count = lax.axis_size("dp")
    tp_count = lax.axis_size("tensor")
    tp_index = lax.axis_index("tensor")

    def own_part(values, axis):
        split = values.shape[axis] // (dp_count * tp_count)
        shape = values.shape[:axis] + (dp_count, tp_count, split) + values.shape[axis + 1 :]
        picked = lax.dynamic_index_in_dim(values.reshape(shape), tp_index, axis + 1, keepdims=False)
        return picked

    seq_count = image_starts.shape[0]
    seq_len = row_count // seq_count
    head_dim = k_proj.shape[1]
    positions = jnp.arange(seq_len, dtype=jnp.float32)
    inv_freq = 10000.0 ** (-(jnp.arange(head_dim // 2, dtype=jnp.float32) * 2.0) / head_dim)
    angles = positions[:, None] * inv_freq[None, :]
    cos_all = jnp.tile(jnp.cos(angles), (seq_count, 1))
    sin_all = jnp.tile(jnp.sin(angles), (seq_count, 1))
    pos_int = jnp.arange(seq_len, dtype=jnp.int32)
    inside = (pos_int[None, :, None] >= image_starts[:, None, :]) & (
        pos_int[None, :, None] < image_starts[:, None, :] + PIECE
    )
    labels = jnp.arange(1, image_starts.shape[1] + 1, dtype=jnp.int32)
    piece_ids = jnp.sum(jnp.where(inside, labels, 0), axis=2)

    own_ids = jnp.where(piece_ids > 0, piece_ids, -1).reshape(row_count, 1)
    all_ids = piece_ids.reshape(1, row_count)
    input_f32 = block_input.astype(jnp.float32)
    gain_attn = norm_gain.astype(jnp.float32)
    gain_query = q_gain.astype(jnp.float32)
    gain_mlp = mlp_gain.astype(jnp.float32)
    cotan_f32 = d_output.astype(jnp.float32)
    normed_one, scale_one = normalize(input_f32)
    normed_in = (normed_one * gain_attn).astype(jnp.bfloat16)
    q_latent = jnp.dot(normed_in, q_down, preferred_element_type=jnp.float32)
    q_latent = lax.optimization_barrier(q_latent)
    q_unit, q_scale = normalize(q_latent)
    q_normed = (q_unit * gain_query).astype(jnp.bfloat16)
    q_raw = jnp.dot(q_normed, q_up, preferred_element_type=jnp.float32)
    key_rows = rotate(
        jnp.dot(normed_in, k_proj, preferred_element_type=jnp.float32), cos_all, sin_all
    ).astype(jnp.bfloat16)
    val_rows = jnp.dot(normed_in, v_proj, preferred_element_type=jnp.float32).astype(jnp.bfloat16)
    hidden_in, queries, mixed_heads, log_norm, normed_mid, scale_two = attend(
        q_raw,
        key_rows,
        val_rows,
        own_ids,
        all_ids,
        cos_all,
        sin_all,
        out_proj,
        block_input,
        gain_mlp.reshape(1, -1),
        "tensor",
        tp_count,
        seq_len,
        5,
    )
    gate_pre = jnp.dot(normed_mid, w_gate, preferred_element_type=jnp.float32)
    up_pre = jnp.dot(normed_mid, w_up, preferred_element_type=jnp.float32)
    gate_sig = jax.nn.sigmoid(gate_pre)
    hidden_act = (gate_pre * gate_sig * up_pre).astype(jnp.bfloat16)
    d_act = right_dot(d_output, w_down)
    d_gate = (d_act * up_pre * gate_sig * (1.0 + gate_pre * (1.0 - gate_sig))).astype(jnp.bfloat16)
    d_up = (d_act * gate_pre * gate_sig).astype(jnp.bfloat16)
    d_mid_part = right_dot(d_gate, w_gate) + right_dot(d_up, w_up)
    d_hidden, d_hidden_low, acc_two, grad_wide, grad_rows, out_part_one, out_part_two = mid_sum(
        d_mid_part,
        scale_two,
        gain_mlp.reshape(1, -1),
        normed_mid,
        hidden_act,
        d_gate,
        d_up,
        d_output,
        w_down,
        hidden_in,
        out_proj.shape[0],
        "tensor",
        tp_count,
        dp_count,
        1,
    )
    grad_wide = lax.psum_scatter(grad_wide, "dp", scatter_dimension=0, tiled=True)
    grad_gate = grad_wide[: grad_wide.shape[0] // 2]
    grad_up = grad_wide[grad_wide.shape[0] // 2 :]
    output_one, d_q_raw, query_key_val, grad_rows = attend_back(
        out_part_one,
        key_rows,
        val_rows,
        log_norm,
        own_ids,
        all_ids,
        cos_all,
        sin_all,
        queries,
        d_hidden_low,
        out_proj,
        q_up,
        mixed_heads,
        grad_rows,
        "tensor",
        tp_count,
        seq_len,
        3,
    )
    grad_rows = lax.psum_scatter(grad_rows, "dp", scatter_dimension=1, tiled=True)
    grad_down = grad_rows[: w_down.shape[0]]
    grad_out = grad_rows[w_down.shape[0] :]
    own_width = model_width // (dp_count * tp_count)
    own_at = jnp.arange(model_width // tp_count)
    own_at = (own_at // own_width * tp_count + tp_index) * own_width + own_at % own_width
    pick = (jnp.arange(model_width)[:, None] == own_at[None, :]).astype(jnp.bfloat16)
    grad_input, own_grads, acc_one, acc_mid = tail_sum(
        query_key_val,
        scale_one,
        q_scale,
        cos_all,
        sin_all,
        gain_attn.reshape(1, -1),
        gain_query.reshape(1, -1),
        q_unit,
        q_down,
        k_proj,
        v_proj,
        pick,
        q_normed,
        d_q_raw,
        block_input,
        d_hidden,
        "tensor",
        tp_count,
        dp_count,
        2,
    )
    gains = jnp.concatenate(
        [
            own_part(jnp.sum(acc_one, axis=0), 0),
            own_part(jnp.sum(acc_two, axis=0), 0),
            own_part(jnp.sum(acc_mid, axis=0), 0),
        ],
        axis=1,
    )
    kept = own_width
    group_rows = -(-kept // 8) * 8 + 8
    gain_row = group_rows - 8
    own_grads = lax.dynamic_update_slice(own_grads, gains[:, None, :], (0, gain_row, 0))
    group = own_grads.shape[2]
    own_grads = own_grads.reshape(-1, group)
    own_sum = lax.psum_scatter(own_grads, "dp", scatter_dimension=0, tiled=True)
    rank = q_down.shape[1]
    own_mid = rank // (dp_count * tp_count)
    own_groups = (rank + 2 * head_dim) // group
    own_rows = jnp.concatenate(
        [own_sum[g * group_rows : g * group_rows + kept] for g in range(own_groups)], axis=1
    )
    up_rows = rank // dp_count
    grad_query_up = jnp.concatenate(
        [own_sum[at : at + up_rows] for at in range(own_groups * group_rows, own_sum.shape[0], up_rows)],
        axis=1,
    )
    grad_qd = own_rows[:, :rank]
    grad_key = own_rows[:, rank : rank + head_dim]
    grad_val = own_rows[:, rank + head_dim :]
    grad_g1 = own_sum[gain_row, :kept]
    grad_g2 = own_sum[gain_row, kept : 2 * kept]
    grad_gq = own_sum[gain_row, 2 * kept : 2 * kept + own_mid]
    output_two = line_sum(out_part_two, "tensor", tp_count, 4)
    block_output = jnp.concatenate([output_one, output_two], axis=0)
    return (
        block_output,
        grad_input,
        grad_g1,
        grad_qd,
        grad_gq,
        grad_query_up,
        grad_key,
        grad_val,
        grad_out,
        grad_g2,
        grad_gate,
        grad_up,
        grad_down,
    )


def solution(mesh):
    placed = (
        P("dp", None),
        P("dp", None),
        P(),
        P(),
        P(),
        P(None, "tensor"),
        P(),
        P(),
        P("tensor", None),
        P(),
        P(None, "tensor"),
        P(None, "tensor"),
        P("tensor", None),
        P("dp", None),
    )

    return jax.shard_map(
        shards,
        mesh=mesh,
        in_specs=placed,
        out_specs=(
            P("dp", None),
            P("dp", None),
            P(("dp", "tensor")),
            P(("dp", "tensor"), None),
            P(("dp", "tensor")),
            P("dp", "tensor"),
            P(("dp", "tensor"), None),
            P(("dp", "tensor"), None),
            P("tensor", "dp"),
            P(("dp", "tensor")),
            P("dp", "tensor"),
            P("dp", "tensor"),
            P("tensor", "dp"),
        ),
        check_vma=False,
    )
```

```python
import functools
import math

import jax
import jax.numpy as jnp
from jax import lax
from jax.experimental import pallas as pl
from jax.experimental.pallas import tpu as pltpu
from jax.sharding import PartitionSpec as P


MESH = pl.DeviceIdType.MESH

PIECE = 256


epsilon = 1e-06
masked_score = -1e30


def normalize(values):
    scale_rows = lax.rsqrt(jnp.mean(values * values, axis=-1, keepdims=True) + epsilon)
    return (values * scale_rows, scale_rows)


def left_dot(left, right):
    return lax.dot_general(
        left, right, (((0,), (0,)), ((), ())), preferred_element_type=jnp.float32
    )


def right_dot(left, right):
    return lax.dot_general(
        left, right, (((1,), (1,)), ((), ())), preferred_element_type=jnp.float32
    )


def rotate(values, cos_tab, sin_tab):
    half = values.shape[-1] // 2
    first_half = values[..., :half]
    second_half = values[..., half:]
    return jnp.concatenate(
        [
            first_half * cos_tab - second_half * sin_tab,
            second_half * cos_tab + first_half * sin_tab,
        ],
        axis=-1,
    )


def line_steps(axis, n, chunks, lag, x_ref, held, red, sems, finish, after_step):
    me = lax.axis_index(axis)
    rows = x_ref.shape[0] // (2 * chunks)
    s_red, r_red, s_fin, r_fin = sems
    barrier = pltpu.get_barrier_semaphore()

    @pl.when(me > 0)
    def _():
        pl.semaphore_signal(barrier, inc=1, device_id={axis: me - 1}, device_id_type=MESH)

    @pl.when(me < n - 1)
    def _():
        pl.semaphore_signal(barrier, inc=1, device_id={axis: me + 1}, device_id_type=MESH)

    @pl.when((me == 0) | (me == n - 1))
    def _():
        pl.semaphore_wait(barrier, 1)

    @pl.when((me > 0) & (me < n - 1))
    def _():
        pl.semaphore_wait(barrier, 2)

    def at(half, c):
        return pl.ds(pl.multiple_of((half * chunks + c) * rows, rows), rows)

    def sum_copy(src, half, c):
        return pltpu.make_async_remote_copy(
            src_ref=src.at[at(half, c)],
            dst_ref=red.at[at(half, c)],
            send_sem=s_red.at[half, c],
            recv_sem=r_red.at[half, c],
            device_id={axis: me - 1 if half == 0 else me + 1},
            device_id_type=MESH,
        )

    def fin_copy(half, c):
        return pltpu.make_async_remote_copy(
            src_ref=held.at[at(half, c)],
            dst_ref=held.at[at(half, c)],
            send_sem=s_fin.at[half, c],
            recv_sem=r_fin.at[half, c],
            device_id={axis: me + 1 if half == 0 else me - 1},
            device_id_type=MESH,
        )

    steps = chunks + 2 * lag * (n - 1)

    def step(s, carry):
        for half in (0, 1):
            hop = (n - 1 - me) if half == 0 else me
            c = s - lag * hop
            ok = (c >= 0) & (c < chunks)

            @pl.when(ok & (hop == 0))
            def _():
                sum_copy(x_ref, half, c).start()

            @pl.when(ok & (hop > 0) & (hop < n - 1))
            def _():
                sum_copy(x_ref, half, c).wait_recv()
                red[at(half, c)] = red[at(half, c)] + x_ref[at(half, c)]
                sum_copy(red, half, c).start()

            @pl.when(ok & (hop == n - 1))
            def _():
                sum_copy(x_ref, half, c).wait_recv()
                held[at(half, c)] = red[at(half, c)] + x_ref[at(half, c)]
                fin_copy(half, c).start()
                finish(at(half, c))

        for half in (0, 1):
            back = me if half == 0 else (n - 1 - me)
            c = s - lag * (n - 1) - lag * back
            ok = (c >= 0) & (c < chunks)

            @pl.when(ok & (back > 0))
            def _():
                fin_copy(half, c).wait_recv()

            @pl.when(ok & (back > 0) & (back < n - 1))
            def _():
                fin_copy(half, c).start()

            @pl.when(ok & (back > 0))
            def _():
                finish(at(half, c))

        if after_step is not None:
            after_step(s, steps)
        return carry

    lax.fori_loop(0, steps, step, 0)

    def drain(c, carry):
        for half in (0, 1):
            hop = (n - 1 - me) if half == 0 else me

            @pl.when(hop < n - 1)
            def _():
                sum_copy(x_ref, half, c).wait_send()

            @pl.when(hop > 0)
            def _():
                fin_copy(half, c).wait_send()

        return carry

    lax.fori_loop(0, chunks, drain, 0)


def line_low_kernel(axis, n, chunks, lag, x_ref, o_ref, red, held, *sems):
    def finish(at):
        o_ref[at] = held[at].astype(o_ref.dtype)

    line_steps(axis, n, chunks, lag, x_ref, held, red, sems, finish, None)


def chunk_count(rows, most, tile):
    chunks = most
    while rows % (2 * chunks * tile):
        chunks -= 1
    return chunks


def line_params(cid):
    return pltpu.CompilerParams(
        collective_id=cid, has_side_effects=True, vmem_limit_bytes=56 << 20
    )


def line_sum(x, axis, n, cid):
    chunks = chunk_count(x.shape[0], 32, 16)
    return pl.pallas_call(
        functools.partial(line_low_kernel, axis, n, chunks, 2),
        out_shape=jax.ShapeDtypeStruct(x.shape, jnp.bfloat16),
        in_specs=[pl.BlockSpec(memory_space=pltpu.VMEM)],
        out_specs=pl.BlockSpec(memory_space=pltpu.VMEM),
        scratch_shapes=[pltpu.VMEM(x.shape, x.dtype)] * 2
        + [pltpu.SemaphoreType.DMA((2, chunks))] * 4,
        compiler_params=line_params(cid),
        name="line_sum",
    )(x)


def fold_rows(values):
    return jnp.sum(values.reshape(values.shape[0] // 8, 8, values.shape[1]), axis=0)


def mid_kernel(
    axis,
    n,
    chunks,
    lag,
    x_ref,
    scale_ref,
    gain_ref,
    mid_hbm,
    act_hbm,
    gate_hbm,
    up_hbm,
    cot_hbm,
    down_hbm,
    hidden_hbm,
    d_hidden_ref,
    d_low_ref,
    acc_ref,
    grad_wide_ref,
    grad_down_ref,
    one_ref,
    two_ref,
    held,
    red,
    mid_ref,
    act_ref,
    gate_ref,
    up_ref,
    cot_ref,
    down_ref,
    wide_tile,
    row_tile,
    base_tile,
    hidden_tile,
    d_tile,
    low_tile,
    load_sem,
    wide_sem,
    row_sem,
    base_sem,
    hidden_sem,
    d_sem,
    low_sem,
    *sems,
):
    me = lax.axis_index(axis)
    rows, width = cot_ref.shape
    part_rows = rows // (2 * chunks)
    acc_ref[...] = jnp.zeros_like(acc_ref)
    units = act_ref.shape[1]
    wide = wide_tile.shape[0]
    wide_count = width // wide
    tile = min(256, rows // 2)
    by_units = units % 128 == 0 and units >= tile
    tall_count = -(-units // tile) if by_units else width // tile
    loads = [
        pltpu.make_async_copy(src, dst, load_sem.at[i])
        for i, (src, dst) in enumerate(
            (
                (mid_hbm, mid_ref),
                (gate_hbm, gate_ref),
                (up_hbm, up_ref),
                (act_hbm, act_ref),
                (cot_hbm, cot_ref),
                (down_hbm, down_ref),
            )
        )
    ]
    for load in loads:
        load.start()

    def block(t):
        return pl.ds(pl.multiple_of(t * tile, tile), tile)

    def wide_copy(which, t):
        to = pl.ds(pl.multiple_of((2 * t + which) * wide, wide), wide)
        return pltpu.make_async_copy(wide_tile, grad_wide_ref.at[to], wide_sem.at[0])

    def tall_at(t):
        return pl.ds(pl.multiple_of(jnp.minimum(t * tile, units - tile), 128), tile)

    def tall_copy(t):
        if by_units:
            return pltpu.make_async_copy(
                row_tile.at[0:tile], grad_down_ref.at[tall_at(t)], row_sem.at[0]
            )
        return pltpu.make_async_copy(
            row_tile.at[0:units, 0:tile], grad_down_ref.at[0:units, block(t)], row_sem.at[0]
        )

    def out_block(t):
        return pl.ds(pl.multiple_of(t * out_tile, out_tile), out_tile)

    def out_copy(dst, t):
        return pltpu.make_async_copy(row_tile.at[0:out_tile], dst.at[out_block(t)], row_sem.at[0])

    out_tile = base_tile.shape[0]
    out_counts = (one_ref.shape[0] // out_tile, two_ref.shape[0] // out_tile)
    tall_from = 2 * wide_count
    out_from = tall_from + tall_count
    job_count = out_from + sum(out_counts)

    def job(j, carry):
        @pl.when(j == 0)
        def _():
            for load in loads:
                load.wait()

        for which, src in enumerate((gate_ref, up_ref)):
            t = lax.div(j, 2)

            @pl.when((j < tall_from) & (lax.rem(j, 2) == which))
            def _():
                cols = pl.ds(pl.multiple_of(t * wide, wide), wide)
                value = left_dot(mid_ref[:, cols], src[...])
                if which:
                    wide_copy(0, t).wait()
                else:

                    @pl.when(t > 0)
                    def _():
                        wide_copy(1, t - 1).wait()

                wide_tile[...] = value
                wide_copy(which, t).start()

        @pl.when((j >= tall_from) & (j < out_from))
        def _():
            t = j - tall_from

            @pl.when(t > 0)
            def _():
                tall_copy(t - 1).wait()

            if by_units:
                row_tile[...] = left_dot(act_ref[:, tall_at(t)], cot_ref[...])
            else:
                row_tile[0:units, 0:tile] = left_dot(act_ref[...], cot_ref[:, block(t)])
            tall_copy(t).start()

        for side, dst in enumerate((one_ref, two_ref)):
            begin = side * out_counts[0]
            t = j - out_from - begin

            @pl.when((t >= 0) & (t < out_counts[side]))
            def _():
                @pl.when(t > 0)
                def _():
                    out_copy(dst, t - 1).wait()

                @pl.when(t == 0)
                def _():
                    if side == 0:
                        tall_copy(tall_count - 1).wait()
                    else:
                        out_copy(one_ref, out_counts[0] - 1).wait()

                base = pltpu.make_async_copy(
                    hidden_hbm.at[out_block(t + begin)], base_tile, base_sem.at[0]
                )
                base.start()
                row_tile[0:out_tile, :] = jnp.dot(
                    act_ref[out_block(t + begin), :],
                    down_ref[...],
                    preferred_element_type=jnp.float32,
                )
                base.wait()

                @pl.when(me == 0)
                def _():
                    row_tile[0:out_tile, :] += base_tile[...]

                out_copy(dst, t).start()

        return carry

    def after_step(s, steps):
        late = steps - 4
        bounds = tuple(jnp.clip(at - 2, 0, late) * job_count // late for at in (s, s + 1))
        lax.fori_loop(*bounds, job, 0)
        for half in (0, 1):
            back = me if half == 0 else (n - 1 - me)
            c = s - lag * (n - 1) - lag * back

            @pl.when((c + 1 >= 0) & (c + 1 < chunks))
            def _():
                take_hidden(half, c + 1).start()

            @pl.when((c >= 0) & (c < chunks))
            def _():
                close(half, c)

    def at_chunk(half, c):
        return pl.ds(pl.multiple_of((half * chunks + c) * part_rows, part_rows), part_rows)

    def take_hidden(half, c):
        slot = lax.rem(c, 2)
        return pltpu.make_async_copy(
            hidden_hbm.at[at_chunk(half, c)], hidden_tile.at[half, slot], hidden_sem.at[half, slot]
        )

    def put(tile_ref, dst, sem, half, c):
        slot = lax.rem(c, 2)
        return pltpu.make_async_copy(
            tile_ref.at[half, slot], dst.at[at_chunk(half, c)], sem.at[half, slot]
        )

    def puts(half, c):
        return (
            put(d_tile, d_hidden_ref, d_sem, half, c),
            put(low_tile, d_low_ref, low_sem, half, c),
        )

    def close(half, c):
        at = at_chunk(half, c)
        slot = lax.rem(c, 2)
        take_hidden(half, c).wait()

        @pl.when(c >= 2)
        def _():
            for item in puts(half, c - 2):
                item.wait()

        d_mid = held[at]
        scale = scale_ref[at, :]
        normed = hidden_tile[half, slot] * scale
        acc_ref[...] += fold_rows(d_mid * normed)
        grad_normed = d_mid * gain_ref[...]
        mean = jnp.mean(grad_normed * normed, axis=1, keepdims=True)
        d_hidden = cot_ref[at].astype(jnp.float32) + scale * (grad_normed - normed * mean)
        d_tile[half, slot] = d_hidden
        low_tile[half, slot] = d_hidden.astype(low_tile.dtype)
        for item in puts(half, c):
            item.start()

    line_steps(axis, n, chunks, lag, x_ref, held, red, sems, lambda at: None, after_step)
    for half in (0, 1):
        for c in range(max(chunks - 2, 0), chunks):
            for item in puts(half, c):
                item.wait()
    wide_copy(1, wide_count - 1).wait()
    out_copy(two_ref, out_counts[1] - 1).wait()


def mid_sum(x, scale, gain, mid, act, d_gate, d_up, cot, w_down, hidden, axis, n, parts, cid):
    rows, width = x.shape
    units = act.shape[1]
    tile = min(256, rows // 2)
    chunks = chunk_count(rows, 32, 16)
    vmem = pl.BlockSpec(memory_space=pltpu.VMEM)
    anywhere = pl.BlockSpec(memory_space=pl.ANY)
    loaded = (mid, act, d_gate, d_up, cot, w_down)
    tall = tile if units % 128 == 0 and units >= tile else max(tile, units)
    return pl.pallas_call(
        functools.partial(mid_kernel, axis, n, chunks, 2),
        out_shape=(
            jax.ShapeDtypeStruct(x.shape, jnp.float32),
            jax.ShapeDtypeStruct(x.shape, jnp.bfloat16),
            jax.ShapeDtypeStruct((8, width), jnp.float32),
            jax.ShapeDtypeStruct((2 * width, units), jnp.float32),
            jax.ShapeDtypeStruct((units, width), jnp.float32),
            jax.ShapeDtypeStruct((rows * 5 // 8, width), jnp.float32),
            jax.ShapeDtypeStruct((rows - rows * 5 // 8, width), jnp.float32),
        ),
        in_specs=[vmem] * 3 + [anywhere] * 7,
        out_specs=(anywhere, anywhere, vmem) + (anywhere,) * 4,
        scratch_shapes=[pltpu.VMEM(x.shape, jnp.float32)] * 2
        + [pltpu.VMEM(item.shape, item.dtype) for item in loaded]
        + [
            pltpu.VMEM((width // parts, units), jnp.float32),
            pltpu.VMEM((tall, width), jnp.float32),
            pltpu.VMEM((rows // 8, width), jnp.float32),
            pltpu.VMEM((2, 2, rows // (2 * chunks), width), jnp.float32),
            pltpu.VMEM((2, 2, rows // (2 * chunks), width), jnp.float32),
            pltpu.VMEM((2, 2, rows // (2 * chunks), width), jnp.bfloat16),
            pltpu.SemaphoreType.DMA((len(loaded),)),
        ]
        + [pltpu.SemaphoreType.DMA((1,))] * 3
        + [pltpu.SemaphoreType.DMA((2, 2))] * 3
        + [pltpu.SemaphoreType.DMA((2, chunks))] * 4,
        compiler_params=pltpu.CompilerParams(
            collective_id=cid, has_side_effects=True, vmem_limit_bytes=62 << 20
        ),
        name="mid_sum",
    )(x, scale, gain, *loaded, hidden)


def tail_kernel(
    axis,
    n,
    chunks,
    lag,
    block,
    x_ref,
    scale_one_ref,
    scale_mid_ref,
    cos_ref,
    sin_ref,
    gain_one_ref,
    gain_mid_ref,
    unit_hbm,
    down_hbm,
    key_hbm,
    val_hbm,
    pick_hbm,
    q_hbm,
    dq_hbm,
    input_hbm,
    hidden_hbm,
    grad_hbm,
    own_ref,
    acc_one_ref,
    acc_mid_ref,
    held,
    red,
    unit_ref,
    down_ref,
    key_ref,
    val_ref,
    pick_ref,
    q_ref,
    dq_ref,
    own_in_ref,
    input_ref,
    hidden_ref,
    grad_ref,
    low_ref,
    load_sem,
    block_sem,
    store_sem,
    *sems,
):
    me = lax.axis_index(axis)
    rows = x_ref.shape[0]
    rank = unit_ref.shape[1]
    head_dim = key_ref.shape[1]
    half_dim = head_dim // 2
    pairs = rows // (2 * block)
    per = chunks // pairs
    loads = [
        pltpu.make_async_copy(src, dst, load_sem.at[i])
        for i, (src, dst) in enumerate(
            (
                (unit_hbm, unit_ref),
                (down_hbm, down_ref),
                (key_hbm, key_ref),
                (val_hbm, val_ref),
                (pick_hbm, pick_ref),
                (q_hbm, q_ref),
                (dq_hbm, dq_ref),
            )
        )
    ]
    for load in loads:
        load.start()
    acc_one_ref[...] = jnp.zeros_like(acc_one_ref)
    acc_mid_ref[...] = jnp.zeros_like(acc_mid_ref)
    parts, all_rows, group = own_ref.shape
    own_groups = x_ref.shape[1] // group
    up_groups = dq_ref.shape[1] // group
    up_rows = q_ref.shape[1] // parts
    kept = (all_rows - up_groups * up_rows) // own_groups
    used = own_in_ref.shape[1] // parts
    for part in range(parts):
        for g in range(own_groups):
            own_ref[part, g * kept + used : (g + 1) * kept, :] = jnp.zeros(
                (kept - used, group), jnp.float32
            )
    up_tile = max(128, up_rows)
    up_count = q_ref.shape[1] // up_tile

    def up_job(t):
        cols = pl.ds(pl.multiple_of(t * up_tile, up_tile), up_tile)
        value = left_dot(q_ref[:, cols], dq_ref[...])
        for i in range(up_tile // up_rows):
            for g in range(up_groups):
                at = own_groups * kept + g * up_rows
                own_ref[t * (up_tile // up_rows) + i, at : at + up_rows, :] = value[
                    i * up_rows : (i + 1) * up_rows, g * group : (g + 1) * group
                ]

    def store(own):
        return pltpu.make_async_copy(grad_ref, grad_hbm.at[own], store_sem.at[0])

    def consume(row_block):
        own = pl.ds(pl.multiple_of(row_block * block, block), block)
        take_input = pltpu.make_async_copy(input_hbm.at[own], input_ref, block_sem.at[0])
        take_hidden = pltpu.make_async_copy(hidden_hbm.at[own], hidden_ref, block_sem.at[1])
        take_input.start()
        take_hidden.start()
        d_bq = held[own, 0:rank]
        unit = unit_ref[own, :]
        acc_mid_ref[...] += fold_rows(d_bq * unit)
        eq = d_bq * gain_mid_ref[...]
        mean_mid = jnp.mean(eq * unit, axis=1, keepdims=True)
        d_latent = (scale_mid_ref[own, :] * (eq - unit * mean_mid)).astype(jnp.bfloat16)
        first = held[own, rank : rank + half_dim]
        second = held[own, rank + half_dim : rank + head_dim]
        cos_tab = cos_ref[own, :]
        sin_tab = sin_ref[own, :]
        low_ref[own, 0:rank] = d_latent
        low_ref[own, rank : rank + half_dim] = (first * cos_tab + second * sin_tab).astype(
            jnp.bfloat16
        )
        low_ref[own, rank + half_dim : rank + head_dim] = (
            second * cos_tab - first * sin_tab
        ).astype(jnp.bfloat16)
        low_ref[own, rank + head_dim :] = held[own, rank + head_dim :].astype(jnp.bfloat16)
        d_in = (
            right_dot(d_latent, down_ref[...])
            + right_dot(low_ref[own, rank : rank + head_dim], key_ref[...])
            + right_dot(low_ref[own, rank + head_dim :], val_ref[...])
        )
        take_input.wait()
        take_hidden.wait()
        scale_one = scale_one_ref[own, :]
        normed = input_ref[...].astype(jnp.float32) * scale_one
        low_in = (normed * gain_one_ref[...]).astype(jnp.bfloat16)
        own_in_ref[own, :] = jnp.dot(
            low_in, pick_ref[...], preferred_element_type=jnp.float32
        ).astype(jnp.bfloat16)
        acc_one_ref[...] += fold_rows(d_in * normed)
        e_in = d_in * gain_one_ref[...]
        mean_one = jnp.mean(e_in * normed, axis=1, keepdims=True)
        grad_ref[...] = (hidden_ref[...] + scale_one * (e_in - normed * mean_one)).astype(
            grad_ref.dtype
        )
        store(own).start()
        store(own).wait()

    def after_step(s, steps):
        @pl.when(s == lag)
        def _():
            for load in loads:
                load.wait()

        @pl.when((s >= lag) & (s < lag + up_count))
        def _():
            up_job(s - lag)

        for half in (0, 1):
            back = me if half == 0 else (n - 1 - me)
            c = s - lag * (n - 1) - lag * back

            @pl.when((c >= 0) & (c < chunks) & (lax.rem(c + 1, per) == 0))
            def _():
                consume(half * pairs + lax.div(c, per))

    line_steps(axis, n, chunks, lag, x_ref, held, red, sems, lambda at: None, after_step)
    grads = left_dot(own_in_ref[...], low_ref[...])
    for part in range(parts):
        for g in range(own_groups):
            own_ref[part, g * kept : g * kept + used, :] = grads[
                part * used : (part + 1) * used, g * group : (g + 1) * group
            ]


def tail_sum(
    x,
    scale_one,
    scale_mid,
    cos_tab,
    sin_tab,
    gain_one,
    gain_mid,
    unit,
    q_down,
    k_proj,
    v_proj,
    pick,
    q_normed,
    d_q,
    block_input,
    d_hidden,
    axis,
    n,
    parts,
    cid,
):
    rows, width = block_input.shape
    block = min(128, rows // 2)
    chunks = chunk_count(rows, 32, 8)
    kept = -(-(pick.shape[1] // parts) // 8) * 8 + 8
    group = math.gcd(x.shape[1], d_q.shape[1])
    all_rows = x.shape[1] // group * kept + d_q.shape[1] // group * (q_normed.shape[1] // parts)
    vmem = pl.BlockSpec(memory_space=pltpu.VMEM)
    anywhere = pl.BlockSpec(memory_space=pl.ANY)
    loaded = (unit, q_down, k_proj, v_proj, pick, q_normed, d_q)
    return pl.pallas_call(
        functools.partial(tail_kernel, axis, n, chunks, 2, block),
        out_shape=(
            jax.ShapeDtypeStruct((rows, width), jnp.bfloat16),
            jax.ShapeDtypeStruct((parts, all_rows, group), jnp.float32),
            jax.ShapeDtypeStruct((8, width), jnp.float32),
            jax.ShapeDtypeStruct((8, unit.shape[1]), jnp.float32),
        ),
        in_specs=[vmem] * 7 + [anywhere] * 9,
        out_specs=(anywhere, vmem, vmem, vmem),
        scratch_shapes=[pltpu.VMEM(x.shape, jnp.float32)] * 2
        + [pltpu.VMEM(item.shape, item.dtype) for item in loaded]
        + [
            pltpu.VMEM((rows, pick.shape[1]), jnp.bfloat16),
            pltpu.VMEM((block, width), jnp.bfloat16),
            pltpu.VMEM((block, width), jnp.float32),
            pltpu.VMEM((block, width), jnp.bfloat16),
            pltpu.VMEM(x.shape, jnp.bfloat16),
            pltpu.SemaphoreType.DMA((len(loaded),)),
            pltpu.SemaphoreType.DMA((2,)),
            pltpu.SemaphoreType.DMA((1,)),
        ]
        + [pltpu.SemaphoreType.DMA((2, chunks))] * 4,
        compiler_params=pltpu.CompilerParams(
            collective_id=cid, has_side_effects=True, vmem_limit_bytes=60 << 20
        ),
        name="tail_sum",
    )(x, scale_one, scale_mid, cos_tab, sin_tab, gain_one, gain_mid, *loaded, block_input, d_hidden)


def attend_kernel(
    axis,
    n,
    chunks,
    lag,
    seq_len,
    block,
    raw_ref,
    k_ref,
    v_ref,
    own_ref,
    all_ref,
    cos_ref,
    sin_ref,
    gain_ref,
    out_hbm,
    down_hbm,
    base_hbm,
    cot_hbm,
    o_ref,
    q_ref,
    mixed_ref,
    norm_ref,
    normed_ref,
    scale_ref,
    d_act_ref,
    part,
    red,
    out_ref,
    down_ref,
    base_tile,
    cot_tile,
    act_tile,
    load_sem,
    tile_sem,
    *sems,
):
    me = lax.axis_index(axis)
    rows, head_dim = k_ref.shape
    heads = raw_ref.shape[1] // head_dim
    half_dim = head_dim // 2
    blocks = seq_len // block
    scale = head_dim ** (-0.5)
    pairs = rows // (2 * block)
    turns = heads + 1
    pair_jobs = 2 * turns
    act_rows = cot_tile.shape[0]
    act_count = rows // act_rows
    out_load = pltpu.make_async_copy(out_hbm, out_ref, load_sem.at[0])
    down_load = pltpu.make_async_copy(down_hbm, down_ref, load_sem.at[1])
    out_load.start()
    down_load.start()

    def act_block(t):
        return pl.ds(pl.multiple_of(t * act_rows, act_rows), act_rows)

    def take_cot(t):
        return pltpu.make_async_copy(cot_hbm.at[act_block(t)], cot_tile, tile_sem.at[0])

    def put_act(t):
        return pltpu.make_async_copy(act_tile, d_act_ref.at[act_block(t)], tile_sem.at[1])

    take_cot(0).start()

    def act_job(t, carry):
        @pl.when(t == 0)
        def _():
            down_load.wait()

        take_cot(t).wait()
        value = right_dot(cot_tile[...], down_ref[...])

        @pl.when(t + 1 < act_count)
        def _():
            take_cot(t + 1).start()

        @pl.when(t > 0)
        def _():
            put_act(t - 1).wait()

        act_tile[...] = value
        put_act(t).start()
        return carry

    def job(j, carry):
        pair = lax.div(j, pair_jobs)
        turn_side = lax.div(lax.rem(j, pair_jobs), turns)
        side = jnp.where(2 * me >= n, turn_side, 1 - turn_side)
        head = lax.rem(j, turns)
        row_block = side * pairs + pair
        seq = lax.div(row_block, blocks)
        block_at = lax.rem(row_block, blocks)
        own = pl.ds(pl.multiple_of(row_block * block, block), block)
        cols = pl.ds(pl.multiple_of(head * head_dim, head_dim), head_dim)
        low_cols = pl.ds(pl.multiple_of(head * head_dim, half_dim), half_dim)
        high_cols = pl.ds(pl.multiple_of(head * head_dim + half_dim, half_dim), half_dim)

        def run(reach):
            keys = pl.ds(pl.multiple_of(seq * seq_len, seq_len), reach)
            first = raw_ref[own, low_cols]
            second = raw_ref[own, high_cols]
            cos_tab = cos_ref[own, :]
            sin_tab = sin_ref[own, :]
            q_ref[own, low_cols] = (first * cos_tab - second * sin_tab).astype(q_ref.dtype)
            q_ref[own, high_cols] = (second * cos_tab + first * sin_tab).astype(q_ref.dtype)
            scores = right_dot(q_ref[own, cols], k_ref[keys, :]) * scale
            q_pos = block_at * block + lax.broadcasted_iota(jnp.int32, scores.shape, 0)
            k_pos = lax.broadcasted_iota(jnp.int32, scores.shape, 1)
            same = own_ref[own, :] == all_ref[:, keys]
            scores = jnp.where((k_pos <= q_pos) | same, scores, masked_score)
            row_max = jnp.max(scores, axis=1, keepdims=True)
            exp_terms = jnp.exp(scores - row_max)
            row_sum = jnp.sum(exp_terms, axis=1, keepdims=True)
            probs = (exp_terms * (1.0 / row_sum)).astype(jnp.bfloat16)
            mixed = jnp.dot(probs, v_ref[keys, :], preferred_element_type=jnp.float32)
            mixed_ref[own, cols] = mixed.astype(mixed_ref.dtype)
            norm_ref[head, own, :] = row_max + jnp.log(row_sum)

        reaches = reach_list(seq_len, block)
        for reach in sorted(set(reaches)):
            first = reaches.index(reach)
            last = first + reaches.count(reach) - 1

            @pl.when((head < heads) & (block_at >= first) & (block_at <= last))
            def _():
                run(reach)

        @pl.when(j == heads)
        def _():
            out_load.wait()

        @pl.when(head == heads)
        def _():
            base = pltpu.make_async_copy(base_hbm.at[own], base_tile, tile_sem.at[2])

            @pl.when(me == 0)
            def _():
                base.start()

            part[own, :] = jnp.dot(
                mixed_ref[own, :], out_ref[...], preferred_element_type=jnp.float32
            )

            @pl.when(me == 0)
            def _():
                base.wait()
                part[own, :] += base_tile[...].astype(jnp.float32)

        return carry

    lax.fori_loop(0, turns, job, 0)
    pair_steps = chunks // pairs

    def after_step(s, steps):
        bounds = tuple(
            jnp.minimum(turns + at * pair_jobs // pair_steps, pairs * pair_jobs)
            for at in (s, s + 1)
        )
        lax.fori_loop(*bounds, job, 0)
        late = steps - chunks - 1
        bounds = tuple(
            jnp.clip(at - chunks, 0, late) * act_count // late for at in (s, s + 1)
        )
        lax.fori_loop(*bounds, act_job, 0)

    def finish(at):
        hidden = o_ref[at]
        scale_rows = lax.rsqrt(jnp.mean(hidden * hidden, axis=1, keepdims=True) + epsilon)
        scale_ref[at, :] = scale_rows
        normed_ref[at] = (hidden * scale_rows * gain_ref[...]).astype(normed_ref.dtype)

    line_steps(axis, n, chunks, lag, part, o_ref, red, sems, finish, after_step)
    put_act(act_count - 1).wait()


def reach_list(seq_len, block):
    step = max(256, block)
    ends = [(b + 1) * block + PIECE for b in range(seq_len // block)]
    return [min(seq_len, -(-end // step) * step) for end in ends]


def attend(
    raw,
    k,
    v,
    own_ids,
    all_ids,
    cos_tab,
    sin_tab,
    gain,
    out_proj,
    w_down,
    base,
    cot,
    axis,
    n,
    seq_len,
    cid,
):
    rows, width = base.shape
    units = w_down.shape[0]
    block = min(64, seq_len)
    act_rows = min(128, rows)
    chunks = chunk_count(rows, 32, 16)
    vmem = pl.BlockSpec(memory_space=pltpu.VMEM)
    anywhere = pl.BlockSpec(memory_space=pl.ANY)
    return pl.pallas_call(
        functools.partial(attend_kernel, axis, n, chunks, 2, seq_len, block),
        out_shape=(
            jax.ShapeDtypeStruct((rows, width), jnp.float32),
            jax.ShapeDtypeStruct(raw.shape, jnp.bfloat16),
            jax.ShapeDtypeStruct(raw.shape, jnp.bfloat16),
            jax.ShapeDtypeStruct((raw.shape[1] // k.shape[1], rows, 1), jnp.float32),
            jax.ShapeDtypeStruct((rows, width), jnp.bfloat16),
            jax.ShapeDtypeStruct((rows, 1), jnp.float32),
            jax.ShapeDtypeStruct((rows, units), jnp.float32),
        ),
        in_specs=[vmem] * 8 + [anywhere] * 4,
        out_specs=(vmem,) * 6 + (anywhere,),
        scratch_shapes=[pltpu.VMEM((rows, width), jnp.float32)] * 2
        + [
            pltpu.VMEM(out_proj.shape, out_proj.dtype),
            pltpu.VMEM(w_down.shape, w_down.dtype),
            pltpu.VMEM((block, width), base.dtype),
            pltpu.VMEM((act_rows, width), cot.dtype),
            pltpu.VMEM((act_rows, units), jnp.float32),
            pltpu.SemaphoreType.DMA((2,)),
            pltpu.SemaphoreType.DMA((3,)),
        ]
        + [pltpu.SemaphoreType.DMA((2, chunks))] * 4,
        compiler_params=pltpu.CompilerParams(
            collective_id=cid, has_side_effects=True, vmem_limit_bytes=62 << 20
        ),
        name="attend",
    )(
        raw,
        k,
        v,
        own_ids,
        all_ids,
        cos_tab,
        sin_tab,
        gain,
        out_proj,
        w_down,
        base,
        cot,
    )


def attend_back_kernel(
    axis,
    n,
    chunks,
    lag,
    seq_len,
    block,
    x_ref,
    k_ref,
    v_ref,
    norm_ref,
    own_ref,
    all_ref,
    cos_ref,
    sin_ref,
    q_hbm,
    low_hbm,
    proj_hbm,
    up_hbm,
    mixed_hbm,
    o_ref,
    dq_ref,
    sums_ref,
    grads_ref,
    red,
    held,
    q_ref,
    low_ref,
    proj_ref,
    up_ref,
    mixed_ref,
    dm_ref,
    row_tile,
    load_sem,
    row_sem,
    *sems,
):
    rows, head_dim = k_ref.shape
    heads = q_ref.shape[1] // head_dim
    half_dim = head_dim // 2
    blocks = seq_len // block
    scale = head_dim ** (-0.5)
    rank = up_ref.shape[0]
    key_cols = slice(rank, rank + head_dim)
    val_cols = slice(rank + head_dim, rank + 2 * head_dim)
    loads = [
        pltpu.make_async_copy(src, dst, load_sem.at[i])
        for i, (src, dst) in enumerate(
            (
                (low_hbm, low_ref),
                (proj_hbm, proj_ref),
                (q_hbm, q_ref),
                (up_hbm, up_ref),
                (mixed_hbm, mixed_ref),
            )
        )
    ]
    for load in loads:
        load.start()
    sums_ref[:, rank:] = jnp.zeros((rows, 2 * head_dim), jnp.float32)
    tile = row_tile.shape[0]
    tile_count = mixed_ref.shape[1] // tile

    def finish(at):
        o_ref[at] = held[at].astype(o_ref.dtype)

    def put(t):
        to = pl.ds(pl.multiple_of(t * tile, tile), tile)
        return pltpu.make_async_copy(row_tile, grads_ref.at[to], row_sem.at[0])

    turns = heads + 1
    tiles_from = turns * (rows // block)
    job_count = tiles_from + tile_count

    def job(j, carry):
        @pl.when(j == 0)
        def _():
            for load in loads:
                load.wait()

        turn = lax.rem(j, turns)
        head = jnp.maximum(turn - 1, 0)
        row_block = jnp.minimum(lax.div(j, turns), rows // block - 1)
        in_blocks = j < tiles_from
        seq = lax.div(row_block, blocks)
        block_at = lax.rem(row_block, blocks)
        own = pl.ds(pl.multiple_of(row_block * block, block), block)
        cols = pl.ds(pl.multiple_of(head * head_dim, head_dim), head_dim)
        low_cols = pl.ds(pl.multiple_of(head * head_dim, half_dim), half_dim)
        high_cols = pl.ds(pl.multiple_of(head * head_dim + half_dim, half_dim), half_dim)

        @pl.when(in_blocks & (turn == 0))
        def _():
            dm_ref[own, :] = right_dot(low_ref[own, :], proj_ref[...]).astype(dm_ref.dtype)

        def run(reach):
            keys = pl.ds(pl.multiple_of(seq * seq_len, seq_len), reach)
            q = q_ref[own, cols]
            dm = dm_ref[own, cols]
            k = k_ref[keys, :]
            v = v_ref[keys, :]
            scores = right_dot(q, k) * scale
            q_pos = block_at * block + lax.broadcasted_iota(jnp.int32, scores.shape, 0)
            k_pos = lax.broadcasted_iota(jnp.int32, scores.shape, 1)
            same = own_ref[own, :] == all_ref[:, keys]
            probs = jnp.where(
                (k_pos <= q_pos) | same, jnp.exp(scores - norm_ref[head, own, :]), 0.0
            )
            d_probs = right_dot(dm, v)
            row_sum = jnp.sum(probs * d_probs, axis=1, keepdims=True)
            d_scores = (probs * (d_probs - row_sum)).astype(jnp.bfloat16)
            sums_ref[keys, key_cols] += left_dot(d_scores, q) * scale
            sums_ref[keys, val_cols] += left_dot(probs.astype(jnp.bfloat16), dm)
            dq = jnp.dot(d_scores, k, preferred_element_type=jnp.float32) * scale
            first = dq[:, :half_dim]
            second = dq[:, half_dim:]
            cos_tab = cos_ref[own, :]
            sin_tab = sin_ref[own, :]
            dq_ref[own, low_cols] = (first * cos_tab + second * sin_tab).astype(dq_ref.dtype)
            dq_ref[own, high_cols] = (second * cos_tab - first * sin_tab).astype(dq_ref.dtype)

        reaches = reach_list(seq_len, block)
        for reach in sorted(set(reaches)):
            first = reaches.index(reach)
            last = first + reaches.count(reach) - 1

            @pl.when(in_blocks & (turn > 0) & (block_at >= first) & (block_at <= last))
            def _():
                run(reach)

        @pl.when(in_blocks & (turn == heads))
        def _():
            sums_ref[own, 0:rank] = right_dot(dq_ref[own, :], up_ref[...])

        @pl.when(j >= tiles_from)
        def _():
            t = j - tiles_from

            @pl.when(t > 0)
            def _():
                put(t - 1).wait()

            part = pl.ds(pl.multiple_of(t * tile, tile), tile)
            row_tile[...] = left_dot(mixed_ref[:, part], low_ref[...])
            put(t).start()

        return carry

    def after_step(s, steps):
        late = steps - 2
        bounds = tuple(jnp.clip(at - 1, 0, late) * job_count // late for at in (s, s + 1))
        lax.fori_loop(*bounds, job, 0)

    line_steps(axis, n, chunks, lag, x_ref, held, red, sems, finish, after_step)
    put(tile_count - 1).wait()


def attend_back(
    x,
    k,
    v,
    norm,
    own_ids,
    all_ids,
    cos_tab,
    sin_tab,
    q,
    d_low,
    out_proj,
    q_up,
    mixed,
    axis,
    n,
    seq_len,
    cid,
):
    chunks = chunk_count(x.shape[0], 32, 16)
    block = min(128, seq_len)
    vmem = pl.BlockSpec(memory_space=pltpu.VMEM)
    anywhere = pl.BlockSpec(memory_space=pl.ANY)
    loaded = (q, d_low, out_proj, q_up, mixed)
    return pl.pallas_call(
        functools.partial(attend_back_kernel, axis, n, chunks, 2, seq_len, block),
        out_shape=(
            jax.ShapeDtypeStruct(x.shape, jnp.bfloat16),
            jax.ShapeDtypeStruct(q.shape, jnp.bfloat16),
            jax.ShapeDtypeStruct((k.shape[0], q_up.shape[0] + 2 * k.shape[1]), jnp.float32),
            jax.ShapeDtypeStruct((mixed.shape[1], d_low.shape[1]), jnp.float32),
        ),
        in_specs=[vmem] * 8 + [anywhere] * 5,
        out_specs=(vmem, vmem, vmem, anywhere),
        scratch_shapes=[pltpu.VMEM(x.shape, x.dtype)] * 2
        + [pltpu.VMEM(item.shape, item.dtype) for item in loaded]
        + [
            pltpu.VMEM(q.shape, jnp.bfloat16),
            pltpu.VMEM((min(256, q.shape[1]), d_low.shape[1]), jnp.float32),
            pltpu.SemaphoreType.DMA((len(loaded),)),
            pltpu.SemaphoreType.DMA((1,)),
        ]
        + [pltpu.SemaphoreType.DMA((2, chunks))] * 4,
        compiler_params=pltpu.CompilerParams(
            collective_id=cid, has_side_effects=True, vmem_limit_bytes=61 << 20
        ),
        name="attend_back",
    )(x, k, v, norm, own_ids, all_ids, cos_tab, sin_tab, *loaded)


def shards(
    block_input,
    image_starts,
    norm_gain,
    q_down,
    q_gain,
    q_up,
    k_proj,
    v_proj,
    out_proj,
    mlp_gain,
    w_gate,
    w_up,
    w_down,
    d_output,
):
    row_count, model_width = block_input.shape
    dp_count = lax.axis_size("dp")
    tp_count = lax.axis_size("tensor")
    tp_index = lax.axis_index("tensor")

    def own_part(values, axis):
        split = values.shape[axis] // (dp_count * tp_count)
        shape = values.shape[:axis] + (dp_count, tp_count, split) + values.shape[axis + 1 :]
        picked = lax.dynamic_index_in_dim(values.reshape(shape), tp_index, axis + 1, keepdims=False)
        return picked

    seq_count = image_starts.shape[0]
    seq_len = row_count // seq_count
    head_dim = k_proj.shape[1]
    positions = jnp.arange(seq_len, dtype=jnp.float32)
    inv_freq = 10000.0 ** (-(jnp.arange(head_dim // 2, dtype=jnp.float32) * 2.0) / head_dim)
    angles = positions[:, None] * inv_freq[None, :]
    cos_all = jnp.tile(jnp.cos(angles), (seq_count, 1))
    sin_all = jnp.tile(jnp.sin(angles), (seq_count, 1))
    pos_int = jnp.arange(seq_len, dtype=jnp.int32)
    inside = (pos_int[None, :, None] >= image_starts[:, None, :]) & (
        pos_int[None, :, None] < image_starts[:, None, :] + PIECE
    )
    labels = jnp.arange(1, image_starts.shape[1] + 1, dtype=jnp.int32)
    piece_ids = jnp.sum(jnp.where(inside, labels, 0), axis=2)

    own_ids = jnp.where(piece_ids > 0, piece_ids, -1).reshape(row_count, 1)
    all_ids = piece_ids.reshape(1, row_count)
    input_f32 = block_input.astype(jnp.float32)
    gain_attn = norm_gain.astype(jnp.float32)
    gain_query = q_gain.astype(jnp.float32)
    gain_mlp = mlp_gain.astype(jnp.float32)
    cotan_f32 = d_output.astype(jnp.float32)
    normed_one, scale_one = normalize(input_f32)
    normed_in = (normed_one * gain_attn).astype(jnp.bfloat16)
    q_latent = jnp.dot(normed_in, q_down, preferred_element_type=jnp.float32)
    q_latent = lax.optimization_barrier(q_latent)
    q_unit, q_scale = normalize(q_latent)
    q_normed = (q_unit * gain_query).astype(jnp.bfloat16)
    q_raw = jnp.dot(q_normed, q_up, preferred_element_type=jnp.float32)
    key_rows = rotate(
        jnp.dot(normed_in, k_proj, preferred_element_type=jnp.float32), cos_all, sin_all
    ).astype(jnp.bfloat16)
    val_rows = jnp.dot(normed_in, v_proj, preferred_element_type=jnp.float32).astype(jnp.bfloat16)
    hidden_in, queries, mixed_heads, log_norm, normed_mid, scale_two, d_act = attend(
        q_raw,
        key_rows,
        val_rows,
        own_ids,
        all_ids,
        cos_all,
        sin_all,
        gain_mlp.reshape(1, -1),
        out_proj,
        w_down,
        block_input,
        d_output,
        "tensor",
        tp_count,
        seq_len,
        5,
    )
    gate_pre = jnp.dot(normed_mid, w_gate, preferred_element_type=jnp.float32)
    up_pre = jnp.dot(normed_mid, w_up, preferred_element_type=jnp.float32)
    gate_sig = jax.nn.sigmoid(gate_pre)
    hidden_act = (gate_pre * gate_sig * up_pre).astype(jnp.bfloat16)
    d_gate = (d_act * up_pre * gate_sig * (1.0 + gate_pre * (1.0 - gate_sig))).astype(jnp.bfloat16)
    d_up = (d_act * gate_pre * gate_sig).astype(jnp.bfloat16)
    d_mid_part = right_dot(d_gate, w_gate) + right_dot(d_up, w_up)
    d_hidden, d_hidden_low, acc_two, grad_wide, grad_down, out_part_one, out_part_two = mid_sum(
        d_mid_part,
        scale_two,
        gain_mlp.reshape(1, -1),
        normed_mid,
        hidden_act,
        d_gate,
        d_up,
        d_output,
        w_down,
        hidden_in,
        "tensor",
        tp_count,
        dp_count,
        1,
    )
    grad_wide = lax.psum_scatter(grad_wide, "dp", scatter_dimension=0, tiled=True)
    grad_down = lax.psum_scatter(grad_down, "dp", scatter_dimension=1, tiled=True)
    grad_gate = grad_wide[: grad_wide.shape[0] // 2]
    grad_up = grad_wide[grad_wide.shape[0] // 2 :]
    output_one, d_q_raw, query_key_val, grad_out = attend_back(
        out_part_one,
        key_rows,
        val_rows,
        log_norm,
        own_ids,
        all_ids,
        cos_all,
        sin_all,
        queries,
        d_hidden_low,
        out_proj,
        q_up,
        mixed_heads,
        "tensor",
        tp_count,
        seq_len,
        3,
    )
    grad_out = lax.psum_scatter(grad_out, "dp", scatter_dimension=1, tiled=True)
    own_width = model_width // (dp_count * tp_count)
    own_at = jnp.arange(model_width // tp_count)
    own_at = (own_at // own_width * tp_count + tp_index) * own_width + own_at % own_width
    pick = (jnp.arange(model_width)[:, None] == own_at[None, :]).astype(jnp.bfloat16)
    grad_input, own_grads, acc_one, acc_mid = tail_sum(
        query_key_val,
        scale_one,
        q_scale,
        cos_all,
        sin_all,
        gain_attn.reshape(1, -1),
        gain_query.reshape(1, -1),
        q_unit,
        q_down,
        k_proj,
        v_proj,
        pick,
        q_normed,
        d_q_raw,
        block_input,
        d_hidden,
        "tensor",
        tp_count,
        dp_count,
        2,
    )
    gains = jnp.concatenate(
        [
            own_part(jnp.sum(acc_one, axis=0), 0),
            own_part(jnp.sum(acc_two, axis=0), 0),
            own_part(jnp.sum(acc_mid, axis=0), 0),
        ],
        axis=1,
    )
    kept = own_width
    group_rows = -(-kept // 8) * 8 + 8
    gain_row = group_rows - 8
    own_grads = lax.dynamic_update_slice(own_grads, gains[:, None, :], (0, gain_row, 0))
    group = own_grads.shape[2]
    own_grads = own_grads.reshape(-1, group)
    own_sum = lax.psum_scatter(own_grads, "dp", scatter_dimension=0, tiled=True)
    rank = q_down.shape[1]
    own_mid = rank // (dp_count * tp_count)
    own_groups = (rank + 2 * head_dim) // group
    own_rows = jnp.concatenate(
        [own_sum[g * group_rows : g * group_rows + kept] for g in range(own_groups)], axis=1
    )
    up_rows = rank // dp_count
    grad_query_up = jnp.concatenate(
        [own_sum[at : at + up_rows] for at in range(own_groups * group_rows, own_sum.shape[0], up_rows)],
        axis=1,
    )
    grad_qd = own_rows[:, :rank]
    grad_key = own_rows[:, rank : rank + head_dim]
    grad_val = own_rows[:, rank + head_dim :]
    grad_g1 = own_sum[gain_row, :kept]
    grad_g2 = own_sum[gain_row, kept : 2 * kept]
    grad_gq = own_sum[gain_row, 2 * kept : 2 * kept + own_mid]
    output_two = line_sum(out_part_two, "tensor", tp_count, 4)
    block_output = jnp.concatenate([output_one, output_two], axis=0)
    return (
        block_output,
        grad_input,
        grad_g1,
        grad_qd,
        grad_gq,
        grad_query_up,
        grad_key,
        grad_val,
        grad_out,
        grad_g2,
        grad_gate,
        grad_up,
        grad_down,
    )


def solution(mesh):
    placed = (
        P("dp", None),
        P("dp", None),
        P(),
        P(),
        P(),
        P(None, "tensor"),
        P(),
        P(),
        P("tensor", None),
        P(),
        P(None, "tensor"),
        P(None, "tensor"),
        P("tensor", None),
        P("dp", None),
    )

    return jax.shard_map(
        shards,
        mesh=mesh,
        in_specs=placed,
        out_specs=(
            P("dp", None),
            P("dp", None),
            P(("dp", "tensor")),
            P(("dp", "tensor"), None),
            P(("dp", "tensor")),
            P("dp", "tensor"),
            P(("dp", "tensor"), None),
            P(("dp", "tensor"), None),
            P("tensor", "dp"),
            P(("dp", "tensor")),
            P("dp", "tensor"),
            P("dp", "tensor"),
            P("tensor", "dp"),
        ),
        check_vma=False,
    )
```

```python
import functools
import math

import jax
import jax.numpy as jnp
from jax import lax
from jax.experimental import pallas as pl
from jax.experimental.pallas import tpu as pltpu
from jax.sharding import PartitionSpec as P


MESH = pl.DeviceIdType.MESH

PIECE = 256


epsilon = 1e-06
masked_score = -1e30


def normalize(values):
    scale_rows = lax.rsqrt(jnp.mean(values * values, axis=-1, keepdims=True) + epsilon)
    return (values * scale_rows, scale_rows)


def left_dot(left, right):
    return lax.dot_general(
        left, right, (((0,), (0,)), ((), ())), preferred_element_type=jnp.float32
    )


def right_dot(left, right):
    return lax.dot_general(
        left, right, (((1,), (1,)), ((), ())), preferred_element_type=jnp.float32
    )


def rotate(values, cos_tab, sin_tab):
    half = values.shape[-1] // 2
    first_half = values[..., :half]
    second_half = values[..., half:]
    return jnp.concatenate(
        [
            first_half * cos_tab - second_half * sin_tab,
            second_half * cos_tab + first_half * sin_tab,
        ],
        axis=-1,
    )


def line_steps(axis, n, chunks, lag, x_ref, held, red, sems, finish, after_step):
    me = lax.axis_index(axis)
    rows = x_ref.shape[0] // (2 * chunks)
    s_red, r_red, s_fin, r_fin = sems
    barrier = pltpu.get_barrier_semaphore()

    @pl.when(me > 0)
    def _():
        pl.semaphore_signal(barrier, inc=1, device_id={axis: me - 1}, device_id_type=MESH)

    @pl.when(me < n - 1)
    def _():
        pl.semaphore_signal(barrier, inc=1, device_id={axis: me + 1}, device_id_type=MESH)

    @pl.when((me == 0) | (me == n - 1))
    def _():
        pl.semaphore_wait(barrier, 1)

    @pl.when((me > 0) & (me < n - 1))
    def _():
        pl.semaphore_wait(barrier, 2)

    def at(half, c):
        return pl.ds(pl.multiple_of((half * chunks + c) * rows, rows), rows)

    def sum_copy(src, half, c):
        return pltpu.make_async_remote_copy(
            src_ref=src.at[at(half, c)],
            dst_ref=red.at[at(half, c)],
            send_sem=s_red.at[half, c],
            recv_sem=r_red.at[half, c],
            device_id={axis: me - 1 if half == 0 else me + 1},
            device_id_type=MESH,
        )

    def fin_copy(half, c):
        return pltpu.make_async_remote_copy(
            src_ref=held.at[at(half, c)],
            dst_ref=held.at[at(half, c)],
            send_sem=s_fin.at[half, c],
            recv_sem=r_fin.at[half, c],
            device_id={axis: me + 1 if half == 0 else me - 1},
            device_id_type=MESH,
        )

    steps = chunks + 2 * lag * (n - 1)

    def step(s, carry):
        for half in (0, 1):
            hop = (n - 1 - me) if half == 0 else me
            c = s - lag * hop
            ok = (c >= 0) & (c < chunks)

            @pl.when(ok & (hop == 0))
            def _():
                sum_copy(x_ref, half, c).start()

            @pl.when(ok & (hop > 0) & (hop < n - 1))
            def _():
                sum_copy(x_ref, half, c).wait_recv()
                red[at(half, c)] = red[at(half, c)] + x_ref[at(half, c)]
                sum_copy(red, half, c).start()

            @pl.when(ok & (hop == n - 1))
            def _():
                sum_copy(x_ref, half, c).wait_recv()
                held[at(half, c)] = red[at(half, c)] + x_ref[at(half, c)]
                fin_copy(half, c).start()
                finish(at(half, c))

        for half in (0, 1):
            back = me if half == 0 else (n - 1 - me)
            c = s - lag * (n - 1) - lag * back
            ok = (c >= 0) & (c < chunks)

            @pl.when(ok & (back > 0))
            def _():
                fin_copy(half, c).wait_recv()

            @pl.when(ok & (back > 0) & (back < n - 1))
            def _():
                fin_copy(half, c).start()

            @pl.when(ok & (back > 0))
            def _():
                finish(at(half, c))

        if after_step is not None:
            after_step(s, steps)
        return carry

    lax.fori_loop(0, steps, step, 0)

    def drain(c, carry):
        for half in (0, 1):
            hop = (n - 1 - me) if half == 0 else me

            @pl.when(hop < n - 1)
            def _():
                sum_copy(x_ref, half, c).wait_send()

            @pl.when(hop > 0)
            def _():
                fin_copy(half, c).wait_send()

        return carry

    lax.fori_loop(0, chunks, drain, 0)


def line_low_kernel(axis, n, chunks, lag, x_ref, o_ref, red, held, *sems):
    def finish(at):
        o_ref[at] = held[at].astype(o_ref.dtype)

    line_steps(axis, n, chunks, lag, x_ref, held, red, sems, finish, None)


def chunk_count(rows, most, tile):
    chunks = most
    while rows % (2 * chunks * tile):
        chunks -= 1
    return chunks


def line_params(cid):
    return pltpu.CompilerParams(
        collective_id=cid, has_side_effects=True, vmem_limit_bytes=56 << 20
    )


def line_sum(x, axis, n, cid):
    chunks = chunk_count(x.shape[0], 32, 16)
    return pl.pallas_call(
        functools.partial(line_low_kernel, axis, n, chunks, 2),
        out_shape=jax.ShapeDtypeStruct(x.shape, jnp.bfloat16),
        in_specs=[pl.BlockSpec(memory_space=pltpu.VMEM)],
        out_specs=pl.BlockSpec(memory_space=pltpu.VMEM),
        scratch_shapes=[pltpu.VMEM(x.shape, x.dtype)] * 2
        + [pltpu.SemaphoreType.DMA((2, chunks))] * 4,
        compiler_params=line_params(cid),
        name="line_sum",
    )(x)


def fold_rows(values):
    return jnp.sum(values.reshape(values.shape[0] // 8, 8, values.shape[1]), axis=0)


def mid_kernel(
    axis,
    n,
    chunks,
    lag,
    scale_ref,
    gain_ref,
    gate_hbm,
    up_hbm,
    gate_w_hbm,
    up_w_hbm,
    act_hbm,
    cot_hbm,
    down_hbm,
    mid_hbm,
    hidden_hbm,
    d_hidden_ref,
    d_low_ref,
    acc_ref,
    grad_wide_ref,
    grad_down_ref,
    one_ref,
    two_ref,
    part,
    held,
    red,
    gate_ref,
    up_ref,
    gate_w_ref,
    up_w_ref,
    act_ref,
    cot_ref,
    down_ref,
    mid_tile,
    wide_tile,
    row_tile,
    base_tile,
    hidden_tile,
    d_tile,
    low_tile,
    load_sem,
    mid_sem,
    wide_sem,
    row_sem,
    base_sem,
    hidden_sem,
    d_sem,
    low_sem,
    *sems,
):
    me = lax.axis_index(axis)
    rows, width = cot_ref.shape
    part_rows = rows // (2 * chunks)
    acc_ref[...] = jnp.zeros_like(acc_ref)
    units = act_ref.shape[1]
    wide = wide_tile.shape[0]
    wide_count = width // wide
    tile = min(256, rows // 2)
    by_units = units % 128 == 0 and units >= tile
    tall_count = -(-units // tile) if by_units else width // tile
    loads = [
        pltpu.make_async_copy(src, dst, load_sem.at[i])
        for i, (src, dst) in enumerate(
            (
                (gate_hbm, gate_ref),
                (up_hbm, up_ref),
                (gate_w_hbm, gate_w_ref),
                (up_w_hbm, up_w_ref),
                (act_hbm, act_ref),
                (cot_hbm, cot_ref),
                (down_hbm, down_ref),
            )
        )
    ]
    for load in loads:
        load.start()

    def take_mid(t):
        cols = pl.ds(pl.multiple_of(t * wide, wide), wide)
        slot = lax.rem(t, 2)
        return pltpu.make_async_copy(mid_hbm.at[:, cols], mid_tile.at[slot], mid_sem.at[slot])

    take_mid(0).start()
    made = min(128, rows // 2)
    pairs = rows // (2 * made)
    pair_steps = chunks // pairs

    def produce(i, carry):
        side = lax.rem(i, 2)
        side = jnp.where(2 * me >= n, side, 1 - side)
        row_block = side * pairs + lax.div(i, 2)
        own = pl.ds(pl.multiple_of(row_block * made, made), made)
        part[own, :] = right_dot(gate_ref[own, :], gate_w_ref[...]) + right_dot(
            up_ref[own, :], up_w_ref[...]
        )
        return carry

    for load in loads[:4]:
        load.wait()
    produce(0, 0)

    def block(t):
        return pl.ds(pl.multiple_of(t * tile, tile), tile)

    def wide_copy(which, t):
        to = pl.ds(pl.multiple_of((2 * t + which) * wide, wide), wide)
        return pltpu.make_async_copy(wide_tile, grad_wide_ref.at[to], wide_sem.at[0])

    def tall_at(t):
        return pl.ds(pl.multiple_of(jnp.minimum(t * tile, units - tile), 128), tile)

    def tall_copy(t):
        if by_units:
            return pltpu.make_async_copy(
                row_tile.at[0:tile], grad_down_ref.at[tall_at(t)], row_sem.at[0]
            )
        return pltpu.make_async_copy(
            row_tile.at[0:units, 0:tile], grad_down_ref.at[0:units, block(t)], row_sem.at[0]
        )

    def out_block(t):
        return pl.ds(pl.multiple_of(t * out_tile, out_tile), out_tile)

    def out_copy(dst, t):
        return pltpu.make_async_copy(row_tile.at[0:out_tile], dst.at[out_block(t)], row_sem.at[0])

    out_tile = base_tile.shape[0]
    out_counts = (one_ref.shape[0] // out_tile, two_ref.shape[0] // out_tile)
    tall_from = 2 * wide_count
    out_from = tall_from + tall_count
    job_count = out_from + sum(out_counts)

    def job(j, carry):
        @pl.when(j == 0)
        def _():
            for load in loads[4:]:
                load.wait()

        for which, src in enumerate((gate_ref, up_ref)):
            t = lax.div(j, 2)

            @pl.when((j < tall_from) & (lax.rem(j, 2) == which))
            def _():
                if which == 0:
                    take_mid(t).wait()

                    @pl.when(t + 1 < wide_count)
                    def _():
                        take_mid(t + 1).start()

                value = left_dot(mid_tile[lax.rem(t, 2)], src[...])
                if which:
                    wide_copy(0, t).wait()
                else:

                    @pl.when(t > 0)
                    def _():
                        wide_copy(1, t - 1).wait()

                wide_tile[...] = value
                wide_copy(which, t).start()

        @pl.when((j >= tall_from) & (j < out_from))
        def _():
            t = j - tall_from

            @pl.when(t > 0)
            def _():
                tall_copy(t - 1).wait()

            if by_units:
                row_tile[...] = left_dot(act_ref[:, tall_at(t)], cot_ref[...])
            else:
                row_tile[0:units, 0:tile] = left_dot(act_ref[...], cot_ref[:, block(t)])
            tall_copy(t).start()

        for side, dst in enumerate((one_ref, two_ref)):
            begin = side * out_counts[0]
            t = j - out_from - begin

            @pl.when((t >= 0) & (t < out_counts[side]))
            def _():
                @pl.when(t > 0)
                def _():
                    out_copy(dst, t - 1).wait()

                @pl.when(t == 0)
                def _():
                    if side == 0:
                        tall_copy(tall_count - 1).wait()
                    else:
                        out_copy(one_ref, out_counts[0] - 1).wait()

                base = pltpu.make_async_copy(
                    hidden_hbm.at[out_block(t + begin)], base_tile, base_sem.at[0]
                )
                base.start()
                row_tile[0:out_tile, :] = jnp.dot(
                    act_ref[out_block(t + begin), :],
                    down_ref[...],
                    preferred_element_type=jnp.float32,
                )
                base.wait()

                @pl.when(me == 0)
                def _():
                    row_tile[0:out_tile, :] += base_tile[...]

                out_copy(dst, t).start()

        return carry

    def after_step(s, steps):
        made_bounds = tuple(
            jnp.minimum(1 + (at + 2) * 2 // pair_steps, 2 * pairs) for at in (s, s + 1)
        )
        made_from = jnp.where(s == 0, 1, made_bounds[0])
        lax.fori_loop(made_from, made_bounds[1], produce, 0)
        late = steps - 4
        bounds = tuple(jnp.clip(at - 2, 0, late) * job_count // late for at in (s, s + 1))
        lax.fori_loop(*bounds, job, 0)
        for half in (0, 1):
            back = me if half == 0 else (n - 1 - me)
            c = s - lag * (n - 1) - lag * back

            @pl.when((c + 1 >= 0) & (c + 1 < chunks))
            def _():
                take_hidden(half, c + 1).start()

            @pl.when((c >= 0) & (c < chunks))
            def _():
                close(half, c)

    def at_chunk(half, c):
        return pl.ds(pl.multiple_of((half * chunks + c) * part_rows, part_rows), part_rows)

    def take_hidden(half, c):
        slot = lax.rem(c, 2)
        return pltpu.make_async_copy(
            hidden_hbm.at[at_chunk(half, c)], hidden_tile.at[half, slot], hidden_sem.at[half, slot]
        )

    def put(tile_ref, dst, sem, half, c):
        slot = lax.rem(c, 2)
        return pltpu.make_async_copy(
            tile_ref.at[half, slot], dst.at[at_chunk(half, c)], sem.at[half, slot]
        )

    def puts(half, c):
        return (
            put(d_tile, d_hidden_ref, d_sem, half, c),
            put(low_tile, d_low_ref, low_sem, half, c),
        )

    def close(half, c):
        at = at_chunk(half, c)
        slot = lax.rem(c, 2)
        take_hidden(half, c).wait()

        @pl.when(c >= 2)
        def _():
            for item in puts(half, c - 2):
                item.wait()

        d_mid = held[at]
        scale = scale_ref[at, :]
        normed = hidden_tile[half, slot] * scale
        acc_ref[...] += fold_rows(d_mid * normed)
        grad_normed = d_mid * gain_ref[...]
        mean = jnp.mean(grad_normed * normed, axis=1, keepdims=True)
        d_hidden = cot_ref[at].astype(jnp.float32) + scale * (grad_normed - normed * mean)
        d_tile[half, slot] = d_hidden
        low_tile[half, slot] = d_hidden.astype(low_tile.dtype)
        for item in puts(half, c):
            item.start()

    line_steps(axis, n, chunks, lag, part, held, red, sems, lambda at: None, after_step)
    for half in (0, 1):
        for c in range(max(chunks - 2, 0), chunks):
            for item in puts(half, c):
                item.wait()
    wide_copy(1, wide_count - 1).wait()
    out_copy(two_ref, out_counts[1] - 1).wait()


def mid_sum(
    scale, gain, d_gate, d_up, w_gate, w_up, act, cot, w_down, mid, hidden, axis, n, parts, cid
):
    rows, width = hidden.shape
    units = act.shape[1]
    tile = min(256, rows // 2)
    chunks = chunk_count(rows, 32, 16)
    vmem = pl.BlockSpec(memory_space=pltpu.VMEM)
    anywhere = pl.BlockSpec(memory_space=pl.ANY)
    loaded = (d_gate, d_up, w_gate, w_up, act, cot, w_down)
    tall = tile if units % 128 == 0 and units >= tile else max(tile, units)
    return pl.pallas_call(
        functools.partial(mid_kernel, axis, n, chunks, 2),
        out_shape=(
            jax.ShapeDtypeStruct(hidden.shape, jnp.float32),
            jax.ShapeDtypeStruct(hidden.shape, jnp.bfloat16),
            jax.ShapeDtypeStruct((8, width), jnp.float32),
            jax.ShapeDtypeStruct((2 * width, units), jnp.float32),
            jax.ShapeDtypeStruct((units, width), jnp.float32),
            jax.ShapeDtypeStruct((rows * 5 // 8, width), jnp.float32),
            jax.ShapeDtypeStruct((rows - rows * 5 // 8, width), jnp.float32),
        ),
        in_specs=[vmem] * 2 + [anywhere] * 9,
        out_specs=(anywhere, anywhere, vmem) + (anywhere,) * 4,
        scratch_shapes=[pltpu.VMEM(hidden.shape, jnp.float32)] * 3
        + [pltpu.VMEM(item.shape, item.dtype) for item in loaded]
        + [
            pltpu.VMEM((2, rows, width // parts), mid.dtype),
            pltpu.VMEM((width // parts, units), jnp.float32),
            pltpu.VMEM((tall, width), jnp.float32),
            pltpu.VMEM((rows // 8, width), jnp.float32),
            pltpu.VMEM((2, 2, rows // (2 * chunks), width), jnp.float32),
            pltpu.VMEM((2, 2, rows // (2 * chunks), width), jnp.float32),
            pltpu.VMEM((2, 2, rows // (2 * chunks), width), jnp.bfloat16),
            pltpu.SemaphoreType.DMA((len(loaded),)),
            pltpu.SemaphoreType.DMA((2,)),
        ]
        + [pltpu.SemaphoreType.DMA((1,))] * 3
        + [pltpu.SemaphoreType.DMA((2, 2))] * 3
        + [pltpu.SemaphoreType.DMA((2, chunks))] * 4,
        compiler_params=pltpu.CompilerParams(
            collective_id=cid, has_side_effects=True, vmem_limit_bytes=67043328
        ),
        name="mid_sum",
    )(scale, gain, *loaded, mid, hidden)


def tail_kernel(
    axis,
    n,
    chunks,
    lag,
    block,
    x_ref,
    scale_one_ref,
    scale_mid_ref,
    cos_ref,
    sin_ref,
    gain_one_ref,
    gain_mid_ref,
    unit_hbm,
    down_hbm,
    key_hbm,
    val_hbm,
    pick_hbm,
    q_hbm,
    dq_hbm,
    input_hbm,
    hidden_hbm,
    grad_hbm,
    own_ref,
    acc_one_ref,
    acc_mid_ref,
    held,
    red,
    unit_ref,
    down_ref,
    key_ref,
    val_ref,
    pick_ref,
    q_ref,
    dq_ref,
    own_in_ref,
    input_ref,
    hidden_ref,
    grad_ref,
    low_ref,
    load_sem,
    block_sem,
    store_sem,
    *sems,
):
    me = lax.axis_index(axis)
    rows = x_ref.shape[0]
    rank = unit_ref.shape[1]
    head_dim = key_ref.shape[1]
    half_dim = head_dim // 2
    pairs = rows // (2 * block)
    per = chunks // pairs
    loads = [
        pltpu.make_async_copy(src, dst, load_sem.at[i])
        for i, (src, dst) in enumerate(
            (
                (unit_hbm, unit_ref),
                (down_hbm, down_ref),
                (key_hbm, key_ref),
                (val_hbm, val_ref),
                (pick_hbm, pick_ref),
                (q_hbm, q_ref),
                (dq_hbm, dq_ref),
            )
        )
    ]
    for load in loads:
        load.start()
    acc_one_ref[...] = jnp.zeros_like(acc_one_ref)
    acc_mid_ref[...] = jnp.zeros_like(acc_mid_ref)
    parts, all_rows, group = own_ref.shape
    own_groups = x_ref.shape[1] // group
    up_groups = dq_ref.shape[1] // group
    up_rows = q_ref.shape[1] // parts
    kept = (all_rows - up_groups * up_rows) // own_groups
    used = own_in_ref.shape[1] // parts
    for part in range(parts):
        for g in range(own_groups):
            own_ref[part, g * kept + used : (g + 1) * kept, :] = jnp.zeros(
                (kept - used, group), jnp.float32
            )
    up_tile = max(128, up_rows)
    up_count = q_ref.shape[1] // up_tile

    def up_job(t):
        cols = pl.ds(pl.multiple_of(t * up_tile, up_tile), up_tile)
        value = left_dot(q_ref[:, cols], dq_ref[...])
        for i in range(up_tile // up_rows):
            for g in range(up_groups):
                at = own_groups * kept + g * up_rows
                own_ref[t * (up_tile // up_rows) + i, at : at + up_rows, :] = value[
                    i * up_rows : (i + 1) * up_rows, g * group : (g + 1) * group
                ]

    def store(own):
        return pltpu.make_async_copy(grad_ref, grad_hbm.at[own], store_sem.at[0])

    def consume(row_block):
        own = pl.ds(pl.multiple_of(row_block * block, block), block)
        take_input = pltpu.make_async_copy(input_hbm.at[own], input_ref, block_sem.at[0])
        take_hidden = pltpu.make_async_copy(hidden_hbm.at[own], hidden_ref, block_sem.at[1])
        take_input.start()
        take_hidden.start()
        d_bq = held[own, 0:rank]
        unit = unit_ref[own, :]
        acc_mid_ref[...] += fold_rows(d_bq * unit)
        eq = d_bq * gain_mid_ref[...]
        mean_mid = jnp.mean(eq * unit, axis=1, keepdims=True)
        d_latent = (scale_mid_ref[own, :] * (eq - unit * mean_mid)).astype(jnp.bfloat16)
        first = held[own, rank : rank + half_dim]
        second = held[own, rank + half_dim : rank + head_dim]
        cos_tab = cos_ref[own, :]
        sin_tab = sin_ref[own, :]
        low_ref[own, 0:rank] = d_latent
        low_ref[own, rank : rank + half_dim] = (first * cos_tab + second * sin_tab).astype(
            jnp.bfloat16
        )
        low_ref[own, rank + half_dim : rank + head_dim] = (
            second * cos_tab - first * sin_tab
        ).astype(jnp.bfloat16)
        low_ref[own, rank + head_dim :] = held[own, rank + head_dim :].astype(jnp.bfloat16)
        d_in = (
            right_dot(d_latent, down_ref[...])
            + right_dot(low_ref[own, rank : rank + head_dim], key_ref[...])
            + right_dot(low_ref[own, rank + head_dim :], val_ref[...])
        )
        take_input.wait()
        take_hidden.wait()
        scale_one = scale_one_ref[own, :]
        normed = input_ref[...].astype(jnp.float32) * scale_one
        low_in = (normed * gain_one_ref[...]).astype(jnp.bfloat16)
        own_in_ref[own, :] = jnp.dot(
            low_in, pick_ref[...], preferred_element_type=jnp.float32
        ).astype(jnp.bfloat16)
        acc_one_ref[...] += fold_rows(d_in * normed)
        e_in = d_in * gain_one_ref[...]
        mean_one = jnp.mean(e_in * normed, axis=1, keepdims=True)
        grad_ref[...] = (hidden_ref[...] + scale_one * (e_in - normed * mean_one)).astype(
            grad_ref.dtype
        )
        store(own).start()
        store(own).wait()

    def after_step(s, steps):
        @pl.when(s == lag)
        def _():
            for load in loads:
                load.wait()

        @pl.when((s >= lag) & (s < lag + up_count))
        def _():
            up_job(s - lag)

        for half in (0, 1):
            back = me if half == 0 else (n - 1 - me)
            c = s - lag * (n - 1) - lag * back

            @pl.when((c >= 0) & (c < chunks) & (lax.rem(c + 1, per) == 0))
            def _():
                consume(half * pairs + lax.div(c, per))

    line_steps(axis, n, chunks, lag, x_ref, held, red, sems, lambda at: None, after_step)
    grads = left_dot(own_in_ref[...], low_ref[...])
    for part in range(parts):
        for g in range(own_groups):
            own_ref[part, g * kept : g * kept + used, :] = grads[
                part * used : (part + 1) * used, g * group : (g + 1) * group
            ]


def tail_sum(
    x,
    scale_one,
    scale_mid,
    cos_tab,
    sin_tab,
    gain_one,
    gain_mid,
    unit,
    q_down,
    k_proj,
    v_proj,
    pick,
    q_normed,
    d_q,
    block_input,
    d_hidden,
    axis,
    n,
    parts,
    cid,
):
    rows, width = block_input.shape
    block = min(128, rows // 2)
    chunks = chunk_count(rows, 32, 8)
    kept = -(-(pick.shape[1] // parts) // 8) * 8 + 8
    group = math.gcd(x.shape[1], d_q.shape[1])
    all_rows = x.shape[1] // group * kept + d_q.shape[1] // group * (q_normed.shape[1] // parts)
    vmem = pl.BlockSpec(memory_space=pltpu.VMEM)
    anywhere = pl.BlockSpec(memory_space=pl.ANY)
    loaded = (unit, q_down, k_proj, v_proj, pick, q_normed, d_q)
    return pl.pallas_call(
        functools.partial(tail_kernel, axis, n, chunks, 2, block),
        out_shape=(
            jax.ShapeDtypeStruct((rows, width), jnp.bfloat16),
            jax.ShapeDtypeStruct((parts, all_rows, group), jnp.float32),
            jax.ShapeDtypeStruct((8, width), jnp.float32),
            jax.ShapeDtypeStruct((8, unit.shape[1]), jnp.float32),
        ),
        in_specs=[vmem] * 7 + [anywhere] * 9,
        out_specs=(anywhere, vmem, vmem, vmem),
        scratch_shapes=[pltpu.VMEM(x.shape, jnp.float32)] * 2
        + [pltpu.VMEM(item.shape, item.dtype) for item in loaded]
        + [
            pltpu.VMEM((rows, pick.shape[1]), jnp.bfloat16),
            pltpu.VMEM((block, width), jnp.bfloat16),
            pltpu.VMEM((block, width), jnp.float32),
            pltpu.VMEM((block, width), jnp.bfloat16),
            pltpu.VMEM(x.shape, jnp.bfloat16),
            pltpu.SemaphoreType.DMA((len(loaded),)),
            pltpu.SemaphoreType.DMA((2,)),
            pltpu.SemaphoreType.DMA((1,)),
        ]
        + [pltpu.SemaphoreType.DMA((2, chunks))] * 4,
        compiler_params=pltpu.CompilerParams(
            collective_id=cid, has_side_effects=True, vmem_limit_bytes=60 << 20
        ),
        name="tail_sum",
    )(x, scale_one, scale_mid, cos_tab, sin_tab, gain_one, gain_mid, *loaded, block_input, d_hidden)


def attend_kernel(
    axis,
    n,
    chunks,
    lag,
    seq_len,
    block,
    raw_ref,
    k_ref,
    v_ref,
    own_ref,
    all_ref,
    cos_ref,
    sin_ref,
    gain_ref,
    out_hbm,
    down_hbm,
    base_hbm,
    cot_hbm,
    o_ref,
    q_ref,
    mixed_ref,
    norm_ref,
    normed_ref,
    scale_ref,
    d_act_ref,
    part,
    red,
    out_ref,
    down_ref,
    base_tile,
    cot_tile,
    act_tile,
    load_sem,
    tile_sem,
    *sems,
):
    me = lax.axis_index(axis)
    rows, head_dim = k_ref.shape
    heads = raw_ref.shape[1] // head_dim
    half_dim = head_dim // 2
    blocks = seq_len // block
    scale = head_dim ** (-0.5)
    pairs = rows // (2 * block)
    turns = heads + 1
    pair_jobs = 2 * turns
    act_rows = cot_tile.shape[0]
    act_count = rows // act_rows
    out_load = pltpu.make_async_copy(out_hbm, out_ref, load_sem.at[0])
    down_load = pltpu.make_async_copy(down_hbm, down_ref, load_sem.at[1])
    out_load.start()
    down_load.start()

    def act_block(t):
        return pl.ds(pl.multiple_of(t * act_rows, act_rows), act_rows)

    def take_cot(t):
        return pltpu.make_async_copy(cot_hbm.at[act_block(t)], cot_tile, tile_sem.at[0])

    def put_act(t):
        return pltpu.make_async_copy(act_tile, d_act_ref.at[act_block(t)], tile_sem.at[1])

    take_cot(0).start()

    def act_job(t, carry):
        @pl.when(t == 0)
        def _():
            down_load.wait()

        take_cot(t).wait()
        value = right_dot(cot_tile[...], down_ref[...])

        @pl.when(t + 1 < act_count)
        def _():
            take_cot(t + 1).start()

        @pl.when(t > 0)
        def _():
            put_act(t - 1).wait()

        act_tile[...] = value
        put_act(t).start()
        return carry

    def job(j, carry):
        pair = lax.div(j, pair_jobs)
        turn_side = lax.div(lax.rem(j, pair_jobs), turns)
        side = jnp.where(2 * me >= n, turn_side, 1 - turn_side)
        head = lax.rem(j, turns)
        row_block = side * pairs + pair
        seq = lax.div(row_block, blocks)
        block_at = lax.rem(row_block, blocks)
        own = pl.ds(pl.multiple_of(row_block * block, block), block)
        cols = pl.ds(pl.multiple_of(head * head_dim, head_dim), head_dim)
        low_cols = pl.ds(pl.multiple_of(head * head_dim, half_dim), half_dim)
        high_cols = pl.ds(pl.multiple_of(head * head_dim + half_dim, half_dim), half_dim)

        def run(reach):
            keys = pl.ds(pl.multiple_of(seq * seq_len, seq_len), reach)
            first = raw_ref[own, low_cols]
            second = raw_ref[own, high_cols]
            cos_tab = cos_ref[own, :]
            sin_tab = sin_ref[own, :]
            q_ref[own, low_cols] = (first * cos_tab - second * sin_tab).astype(q_ref.dtype)
            q_ref[own, high_cols] = (second * cos_tab + first * sin_tab).astype(q_ref.dtype)
            scores = right_dot(q_ref[own, cols], k_ref[keys, :]) * scale
            q_pos = block_at * block + lax.broadcasted_iota(jnp.int32, scores.shape, 0)
            k_pos = lax.broadcasted_iota(jnp.int32, scores.shape, 1)
            same = own_ref[own, :] == all_ref[:, keys]
            scores = jnp.where((k_pos <= q_pos) | same, scores, masked_score)
            row_max = jnp.max(scores, axis=1, keepdims=True)
            exp_terms = jnp.exp(scores - row_max)
            row_sum = jnp.sum(exp_terms, axis=1, keepdims=True)
            probs = (exp_terms * (1.0 / row_sum)).astype(jnp.bfloat16)
            mixed = jnp.dot(probs, v_ref[keys, :], preferred_element_type=jnp.float32)
            mixed_ref[own, cols] = mixed.astype(mixed_ref.dtype)
            norm_ref[head, own, :] = row_max + jnp.log(row_sum)

        reaches = reach_list(seq_len, block)
        for reach in sorted(set(reaches)):
            first = reaches.index(reach)
            last = first + reaches.count(reach) - 1

            @pl.when((head < heads) & (block_at >= first) & (block_at <= last))
            def _():
                run(reach)

        @pl.when(j == heads)
        def _():
            out_load.wait()

        @pl.when(head == heads)
        def _():
            base = pltpu.make_async_copy(base_hbm.at[own], base_tile, tile_sem.at[2])

            @pl.when(me == 0)
            def _():
                base.start()

            part[own, :] = jnp.dot(
                mixed_ref[own, :], out_ref[...], preferred_element_type=jnp.float32
            )

            @pl.when(me == 0)
            def _():
                base.wait()
                part[own, :] += base_tile[...].astype(jnp.float32)

        return carry

    lax.fori_loop(0, turns, job, 0)
    pair_steps = chunks // pairs

    def after_step(s, steps):
        bounds = tuple(
            jnp.minimum(turns + at * pair_jobs // pair_steps, pairs * pair_jobs)
            for at in (s, s + 1)
        )
        lax.fori_loop(*bounds, job, 0)
        late = steps - chunks - 1
        bounds = tuple(
            jnp.clip(at - chunks, 0, late) * act_count // late for at in (s, s + 1)
        )
        lax.fori_loop(*bounds, act_job, 0)

    def finish(at):
        hidden = o_ref[at]
        scale_rows = lax.rsqrt(jnp.mean(hidden * hidden, axis=1, keepdims=True) + epsilon)
        scale_ref[at, :] = scale_rows
        normed_ref[at] = (hidden * scale_rows * gain_ref[...]).astype(normed_ref.dtype)

    line_steps(axis, n, chunks, lag, part, o_ref, red, sems, finish, after_step)
    put_act(act_count - 1).wait()


def reach_list(seq_len, block):
    step = max(256, block)
    ends = [(b + 1) * block + PIECE for b in range(seq_len // block)]
    return [min(seq_len, -(-end // step) * step) for end in ends]


def attend(
    raw,
    k,
    v,
    own_ids,
    all_ids,
    cos_tab,
    sin_tab,
    gain,
    out_proj,
    w_down,
    base,
    cot,
    axis,
    n,
    seq_len,
    cid,
):
    rows, width = base.shape
    units = w_down.shape[0]
    block = min(64, seq_len)
    act_rows = min(128, rows)
    chunks = chunk_count(rows, 32, 16)
    vmem = pl.BlockSpec(memory_space=pltpu.VMEM)
    anywhere = pl.BlockSpec(memory_space=pl.ANY)
    return pl.pallas_call(
        functools.partial(attend_kernel, axis, n, chunks, 2, seq_len, block),
        out_shape=(
            jax.ShapeDtypeStruct((rows, width), jnp.float32),
            jax.ShapeDtypeStruct(raw.shape, jnp.bfloat16),
            jax.ShapeDtypeStruct(raw.shape, jnp.bfloat16),
            jax.ShapeDtypeStruct((raw.shape[1] // k.shape[1], rows, 1), jnp.float32),
            jax.ShapeDtypeStruct((rows, width), jnp.bfloat16),
            jax.ShapeDtypeStruct((rows, 1), jnp.float32),
            jax.ShapeDtypeStruct((rows, units), jnp.float32),
        ),
        in_specs=[vmem] * 8 + [anywhere] * 4,
        out_specs=(vmem,) * 6 + (anywhere,),
        scratch_shapes=[pltpu.VMEM((rows, width), jnp.float32)] * 2
        + [
            pltpu.VMEM(out_proj.shape, out_proj.dtype),
            pltpu.VMEM(w_down.shape, w_down.dtype),
            pltpu.VMEM((block, width), base.dtype),
            pltpu.VMEM((act_rows, width), cot.dtype),
            pltpu.VMEM((act_rows, units), jnp.float32),
            pltpu.SemaphoreType.DMA((2,)),
            pltpu.SemaphoreType.DMA((3,)),
        ]
        + [pltpu.SemaphoreType.DMA((2, chunks))] * 4,
        compiler_params=pltpu.CompilerParams(
            collective_id=cid, has_side_effects=True, vmem_limit_bytes=62 << 20
        ),
        name="attend",
    )(
        raw,
        k,
        v,
        own_ids,
        all_ids,
        cos_tab,
        sin_tab,
        gain,
        out_proj,
        w_down,
        base,
        cot,
    )


def attend_back_kernel(
    axis,
    n,
    chunks,
    lag,
    seq_len,
    block,
    x_ref,
    k_ref,
    v_ref,
    norm_ref,
    own_ref,
    all_ref,
    cos_ref,
    sin_ref,
    q_hbm,
    low_hbm,
    proj_hbm,
    up_hbm,
    mixed_hbm,
    o_ref,
    dq_ref,
    sums_ref,
    grads_ref,
    red,
    held,
    q_ref,
    low_ref,
    proj_ref,
    up_ref,
    mixed_ref,
    dm_ref,
    row_tile,
    load_sem,
    row_sem,
    *sems,
):
    rows, head_dim = k_ref.shape
    heads = q_ref.shape[1] // head_dim
    half_dim = head_dim // 2
    blocks = seq_len // block
    scale = head_dim ** (-0.5)
    rank = up_ref.shape[0]
    key_cols = slice(rank, rank + head_dim)
    val_cols = slice(rank + head_dim, rank + 2 * head_dim)
    loads = [
        pltpu.make_async_copy(src, dst, load_sem.at[i])
        for i, (src, dst) in enumerate(
            (
                (low_hbm, low_ref),
                (proj_hbm, proj_ref),
                (q_hbm, q_ref),
                (up_hbm, up_ref),
                (mixed_hbm, mixed_ref),
            )
        )
    ]
    for load in loads:
        load.start()
    sums_ref[:, rank:] = jnp.zeros((rows, 2 * head_dim), jnp.float32)
    tile = row_tile.shape[0]
    tile_count = mixed_ref.shape[1] // tile

    def finish(at):
        o_ref[at] = held[at].astype(o_ref.dtype)

    def put(t):
        to = pl.ds(pl.multiple_of(t * tile, tile), tile)
        return pltpu.make_async_copy(row_tile, grads_ref.at[to], row_sem.at[0])

    turns = heads + 1
    tiles_from = turns * (rows // block)
    job_count = tiles_from + tile_count

    def job(j, carry):
        @pl.when(j == 0)
        def _():
            for load in loads:
                load.wait()

        turn = lax.rem(j, turns)
        head = jnp.maximum(turn - 1, 0)
        row_block = jnp.minimum(lax.div(j, turns), rows // block - 1)
        in_blocks = j < tiles_from
        seq = lax.div(row_block, blocks)
        block_at = lax.rem(row_block, blocks)
        own = pl.ds(pl.multiple_of(row_block * block, block), block)
        cols = pl.ds(pl.multiple_of(head * head_dim, head_dim), head_dim)
        low_cols = pl.ds(pl.multiple_of(head * head_dim, half_dim), half_dim)
        high_cols = pl.ds(pl.multiple_of(head * head_dim + half_dim, half_dim), half_dim)

        @pl.when(in_blocks & (turn == 0))
        def _():
            dm_ref[own, :] = right_dot(low_ref[own, :], proj_ref[...]).astype(dm_ref.dtype)

        def run(reach):
            keys = pl.ds(pl.multiple_of(seq * seq_len, seq_len), reach)
            q = q_ref[own, cols]
            dm = dm_ref[own, cols]
            k = k_ref[keys, :]
            v = v_ref[keys, :]
            scores = right_dot(q, k) * scale
            q_pos = block_at * block + lax.broadcasted_iota(jnp.int32, scores.shape, 0)
            k_pos = lax.broadcasted_iota(jnp.int32, scores.shape, 1)
            same = own_ref[own, :] == all_ref[:, keys]
            probs = jnp.where(
                (k_pos <= q_pos) | same, jnp.exp(scores - norm_ref[head, own, :]), 0.0
            )
            d_probs = right_dot(dm, v)
            row_sum = jnp.sum(probs * d_probs, axis=1, keepdims=True)
            d_scores = (probs * (d_probs - row_sum)).astype(jnp.bfloat16)
            sums_ref[keys, key_cols] += left_dot(d_scores, q) * scale
            sums_ref[keys, val_cols] += left_dot(probs.astype(jnp.bfloat16), dm)
            dq = jnp.dot(d_scores, k, preferred_element_type=jnp.float32) * scale
            first = dq[:, :half_dim]
            second = dq[:, half_dim:]
            cos_tab = cos_ref[own, :]
            sin_tab = sin_ref[own, :]
            dq_ref[own, low_cols] = (first * cos_tab + second * sin_tab).astype(dq_ref.dtype)
            dq_ref[own, high_cols] = (second * cos_tab - first * sin_tab).astype(dq_ref.dtype)

        reaches = reach_list(seq_len, block)
        for reach in sorted(set(reaches)):
            first = reaches.index(reach)
            last = first + reaches.count(reach) - 1

            @pl.when(in_blocks & (turn > 0) & (block_at >= first) & (block_at <= last))
            def _():
                run(reach)

        @pl.when(in_blocks & (turn == heads))
        def _():
            sums_ref[own, 0:rank] = right_dot(dq_ref[own, :], up_ref[...])

        @pl.when(j >= tiles_from)
        def _():
            t = j - tiles_from

            @pl.when(t > 0)
            def _():
                put(t - 1).wait()

            part = pl.ds(pl.multiple_of(t * tile, tile), tile)
            row_tile[...] = left_dot(mixed_ref[:, part], low_ref[...])
            put(t).start()

        return carry

    def after_step(s, steps):
        late = steps - 2
        bounds = tuple(jnp.clip(at - 1, 0, late) * job_count // late for at in (s, s + 1))
        lax.fori_loop(*bounds, job, 0)

    line_steps(axis, n, chunks, lag, x_ref, held, red, sems, finish, after_step)
    put(tile_count - 1).wait()


def attend_back(
    x,
    k,
    v,
    norm,
    own_ids,
    all_ids,
    cos_tab,
    sin_tab,
    q,
    d_low,
    out_proj,
    q_up,
    mixed,
    axis,
    n,
    seq_len,
    cid,
):
    chunks = chunk_count(x.shape[0], 32, 16)
    block = min(256, seq_len)
    vmem = pl.BlockSpec(memory_space=pltpu.VMEM)
    anywhere = pl.BlockSpec(memory_space=pl.ANY)
    loaded = (q, d_low, out_proj, q_up, mixed)
    return pl.pallas_call(
        functools.partial(attend_back_kernel, axis, n, chunks, 2, seq_len, block),
        out_shape=(
            jax.ShapeDtypeStruct(x.shape, jnp.bfloat16),
            jax.ShapeDtypeStruct(q.shape, jnp.bfloat16),
            jax.ShapeDtypeStruct((k.shape[0], q_up.shape[0] + 2 * k.shape[1]), jnp.float32),
            jax.ShapeDtypeStruct((mixed.shape[1], d_low.shape[1]), jnp.float32),
        ),
        in_specs=[vmem] * 8 + [anywhere] * 5,
        out_specs=(vmem, vmem, vmem, anywhere),
        scratch_shapes=[pltpu.VMEM(x.shape, x.dtype)] * 2
        + [pltpu.VMEM(item.shape, item.dtype) for item in loaded]
        + [
            pltpu.VMEM(q.shape, jnp.bfloat16),
            pltpu.VMEM((min(256, q.shape[1]), d_low.shape[1]), jnp.float32),
            pltpu.SemaphoreType.DMA((len(loaded),)),
            pltpu.SemaphoreType.DMA((1,)),
        ]
        + [pltpu.SemaphoreType.DMA((2, chunks))] * 4,
        compiler_params=pltpu.CompilerParams(
            collective_id=cid, has_side_effects=True, vmem_limit_bytes=61 << 20
        ),
        name="attend_back",
    )(x, k, v, norm, own_ids, all_ids, cos_tab, sin_tab, *loaded)


def shards(
    block_input,
    image_starts,
    norm_gain,
    q_down,
    q_gain,
    q_up,
    k_proj,
    v_proj,
    out_proj,
    mlp_gain,
    w_gate,
    w_up,
    w_down,
    d_output,
):
    row_count, model_width = block_input.shape
    dp_count = lax.axis_size("dp")
    tp_count = lax.axis_size("tensor")
    tp_index = lax.axis_index("tensor")

    def own_part(values, axis):
        split = values.shape[axis] // (dp_count * tp_count)
        shape = values.shape[:axis] + (dp_count, tp_count, split) + values.shape[axis + 1 :]
        picked = lax.dynamic_index_in_dim(values.reshape(shape), tp_index, axis + 1, keepdims=False)
        return picked

    seq_count = image_starts.shape[0]
    seq_len = row_count // seq_count
    head_dim = k_proj.shape[1]
    positions = jnp.arange(seq_len, dtype=jnp.float32)
    inv_freq = 10000.0 ** (-(jnp.arange(head_dim // 2, dtype=jnp.float32) * 2.0) / head_dim)
    angles = positions[:, None] * inv_freq[None, :]
    cos_all = jnp.tile(jnp.cos(angles), (seq_count, 1))
    sin_all = jnp.tile(jnp.sin(angles), (seq_count, 1))
    pos_int = jnp.arange(seq_len, dtype=jnp.int32)
    inside = (pos_int[None, :, None] >= image_starts[:, None, :]) & (
        pos_int[None, :, None] < image_starts[:, None, :] + PIECE
    )
    labels = jnp.arange(1, image_starts.shape[1] + 1, dtype=jnp.int32)
    piece_ids = jnp.sum(jnp.where(inside, labels, 0), axis=2)

    own_ids = jnp.where(piece_ids > 0, piece_ids, -1).reshape(row_count, 1)
    all_ids = piece_ids.reshape(1, row_count)
    input_f32 = block_input.astype(jnp.float32)
    gain_attn = norm_gain.astype(jnp.float32)
    gain_query = q_gain.astype(jnp.float32)
    gain_mlp = mlp_gain.astype(jnp.float32)
    cotan_f32 = d_output.astype(jnp.float32)
    normed_one, scale_one = normalize(input_f32)
    normed_in = (normed_one * gain_attn).astype(jnp.bfloat16)
    q_latent = jnp.dot(normed_in, q_down, preferred_element_type=jnp.float32)
    q_latent = lax.optimization_barrier(q_latent)
    q_unit, q_scale = normalize(q_latent)
    q_normed = (q_unit * gain_query).astype(jnp.bfloat16)
    q_raw = jnp.dot(q_normed, q_up, preferred_element_type=jnp.float32)
    key_rows = rotate(
        jnp.dot(normed_in, k_proj, preferred_element_type=jnp.float32), cos_all, sin_all
    ).astype(jnp.bfloat16)
    val_rows = jnp.dot(normed_in, v_proj, preferred_element_type=jnp.float32).astype(jnp.bfloat16)
    hidden_in, queries, mixed_heads, log_norm, normed_mid, scale_two, d_act = attend(
        q_raw,
        key_rows,
        val_rows,
        own_ids,
        all_ids,
        cos_all,
        sin_all,
        gain_mlp.reshape(1, -1),
        out_proj,
        w_down,
        block_input,
        d_output,
        "tensor",
        tp_count,
        seq_len,
        5,
    )
    gate_pre = jnp.dot(normed_mid, w_gate, preferred_element_type=jnp.float32)
    up_pre = jnp.dot(normed_mid, w_up, preferred_element_type=jnp.float32)
    gate_sig = jax.nn.sigmoid(gate_pre)
    hidden_act = (gate_pre * gate_sig * up_pre).astype(jnp.bfloat16)
    d_gate = (d_act * up_pre * gate_sig * (1.0 + gate_pre * (1.0 - gate_sig))).astype(jnp.bfloat16)
    d_up = (d_act * gate_pre * gate_sig).astype(jnp.bfloat16)
    d_hidden, d_hidden_low, acc_two, grad_wide, grad_down, out_part_one, out_part_two = mid_sum(
        scale_two,
        gain_mlp.reshape(1, -1),
        d_gate,
        d_up,
        w_gate,
        w_up,
        hidden_act,
        d_output,
        w_down,
        normed_mid,
        hidden_in,
        "tensor",
        tp_count,
        dp_count,
        1,
    )
    grad_wide = lax.psum_scatter(grad_wide, "dp", scatter_dimension=0, tiled=True)
    grad_down = lax.psum_scatter(grad_down, "dp", scatter_dimension=1, tiled=True)
    grad_gate = grad_wide[: grad_wide.shape[0] // 2]
    grad_up = grad_wide[grad_wide.shape[0] // 2 :]
    output_one, d_q_raw, query_key_val, grad_out = attend_back(
        out_part_one,
        key_rows,
        val_rows,
        log_norm,
        own_ids,
        all_ids,
        cos_all,
        sin_all,
        queries,
        d_hidden_low,
        out_proj,
        q_up,
        mixed_heads,
        "tensor",
        tp_count,
        seq_len,
        3,
    )
    grad_out = lax.psum_scatter(grad_out, "dp", scatter_dimension=1, tiled=True)
    own_width = model_width // (dp_count * tp_count)
    own_at = jnp.arange(model_width // tp_count)
    own_at = (own_at // own_width * tp_count + tp_index) * own_width + own_at % own_width
    pick = (jnp.arange(model_width)[:, None] == own_at[None, :]).astype(jnp.bfloat16)
    grad_input, own_grads, acc_one, acc_mid = tail_sum(
        query_key_val,
        scale_one,
        q_scale,
        cos_all,
        sin_all,
        gain_attn.reshape(1, -1),
        gain_query.reshape(1, -1),
        q_unit,
        q_down,
        k_proj,
        v_proj,
        pick,
        q_normed,
        d_q_raw,
        block_input,
        d_hidden,
        "tensor",
        tp_count,
        dp_count,
        2,
    )
    gains = jnp.concatenate(
        [
            own_part(jnp.sum(acc_one, axis=0), 0),
            own_part(jnp.sum(acc_two, axis=0), 0),
            own_part(jnp.sum(acc_mid, axis=0), 0),
        ],
        axis=1,
    )
    kept = own_width
    group_rows = -(-kept // 8) * 8 + 8
    gain_row = group_rows - 8
    own_grads = lax.dynamic_update_slice(own_grads, gains[:, None, :], (0, gain_row, 0))
    group = own_grads.shape[2]
    own_grads = own_grads.reshape(-1, group)
    own_sum = lax.psum_scatter(own_grads, "dp", scatter_dimension=0, tiled=True)
    rank = q_down.shape[1]
    own_mid = rank // (dp_count * tp_count)
    own_groups = (rank + 2 * head_dim) // group
    own_rows = jnp.concatenate(
        [own_sum[g * group_rows : g * group_rows + kept] for g in range(own_groups)], axis=1
    )
    up_rows = rank // dp_count
    grad_query_up = jnp.concatenate(
        [own_sum[at : at + up_rows] for at in range(own_groups * group_rows, own_sum.shape[0], up_rows)],
        axis=1,
    )
    grad_qd = own_rows[:, :rank]
    grad_key = own_rows[:, rank : rank + head_dim]
    grad_val = own_rows[:, rank + head_dim :]
    grad_g1 = own_sum[gain_row, :kept]
    grad_g2 = own_sum[gain_row, kept : 2 * kept]
    grad_gq = own_sum[gain_row, 2 * kept : 2 * kept + own_mid]
    output_two = line_sum(out_part_two, "tensor", tp_count, 4)
    block_output = jnp.concatenate([output_one, output_two], axis=0)
    return (
        block_output,
        grad_input,
        grad_g1,
        grad_qd,
        grad_gq,
        grad_query_up,
        grad_key,
        grad_val,
        grad_out,
        grad_g2,
        grad_gate,
        grad_up,
        grad_down,
    )


def solution(mesh):
    placed = (
        P("dp", None),
        P("dp", None),
        P(),
        P(),
        P(),
        P(None, "tensor"),
        P(),
        P(),
        P("tensor", None),
        P(),
        P(None, "tensor"),
        P(None, "tensor"),
        P("tensor", None),
        P("dp", None),
    )

    return jax.shard_map(
        shards,
        mesh=mesh,
        in_specs=placed,
        out_specs=(
            P("dp", None),
            P("dp", None),
            P(("dp", "tensor")),
            P(("dp", "tensor"), None),
            P(("dp", "tensor")),
            P("dp", "tensor"),
            P(("dp", "tensor"), None),
            P(("dp", "tensor"), None),
            P("tensor", "dp"),
            P(("dp", "tensor")),
            P("dp", "tensor"),
            P("dp", "tensor"),
            P("tensor", "dp"),
        ),
        check_vma=False,
    )
```
